256 devices in a mesh: members: 4 (over y, x), zonal: 32 (over z), merid: 2 (over core).
Axes of the slice: x: 2, y: 2, z: 32, core: 2. Of those that a mesh axis runs over, the one named last changes fastest.
The devices are a block of a 4x8x32 slice.
Arguments:
- height: float32 [2048, 1024], P(('members', 'zonal'), 'merid'), parts along dimension 0, may hold values from -6 to 6
- transport_u: float32 [2048, 1024], P(('members', 'zonal'), 'merid'), parts along dimension 0, may hold values from -4 to 4
- transport_v: float32 [2048, 1024], P(('members', 'zonal'), 'merid'), parts along dimension 0, may hold values from -4 to 4
- thickness: float32 [14, 2048, 1024], P(None, ('members', 'zonal'), 'merid'), parts along dimension 1, may hold values from 0.5 to 2
- velocity_u: float32 [14, 2048, 1024], P(None, ('members', 'zonal'), 'merid'), parts along dimension 1, may hold values from -3 to 3
- velocity_v: float32 [14, 2048, 1024], P(None, ('members', 'zonal'), 'merid'), parts along dimension 1, may hold values from -3 to 3
- sea_faces: int32 [2, 512, 1024], P(None, 'zonal', 'merid'), may hold values 0 or 1
- wind_seeds: int32 [16, 2], P('members'), parts along dimension 0, may hold values from 1 to 96
- wind_scale: float32 [16], P('members'), parts along dimension 0, may hold values from 0.5 to 2
- wind_base: float32 [2, 512, 1024], P(None, 'zonal', 'merid'), may hold values from -6 to 6
Outputs:
- final_height: float32 [2048, 1024], P(('members', 'zonal'), 'merid'), parts along dimension 0
- final_transport_u: float32 [2048, 1024], P(('members', 'zonal'), 'merid'), parts along dimension 0
- final_transport_v: float32 [2048, 1024], P(('members', 'zonal'), 'merid'), parts along dimension 0
- final_thickness: float32 [14, 2048, 1024], P(None, ('members', 'zonal'), 'merid'), parts along dimension 1
- final_velocity_u: float32 [14, 2048, 1024], P(None, ('members', 'zonal'), 'merid'), parts along dimension 1
- final_velocity_v: float32 [14, 2048, 1024], P(None, ('members', 'zonal'), 'merid'), parts along dimension 1
The draws below stay inside these ranges and needn't reach their ends.
There are 4 independent parts, one for each index of `members`. The reference program is written for one: setup_inputs(seed, part) draws one part's arguments, and reference() takes and returns one part's arrays. A program takes and returns all parts, laid end to end along the dimension named above; an argument that names none is the same for every part. Nothing has to cross between parts.
All inputs are finite; a program needn't handle non-finite values. No bound on the sum of `sea_faces` on one device may be relied on, other than what follows from the above.
Results may differ from the reference program's by a relative error of at most 0.0001.
Values sent between devices are 32-bit elements; how exact they have to be, the bound alone decides.
A program may use at most 64 MiB of HBM per device.

```python
import math
import jax
import jax.numpy as jnp

LAYERS = 14
NSUB = 6
STEPS = 2
MODES = 4
NX = 512
NY = 1024


def plant(result, stream_key, least, top_value):
    spot = [jax.random.randint(jax.random.fold_in(stream_key, axis), (), 0, length) for axis, length in enumerate(result.shape)]
    widest = result.shape.index(max(result.shape))
    beside = spot[:widest] + [(spot[widest] + 1) % result.shape[widest]] + spot[widest + 1:]
    return result.at[tuple(spot)].set(least).at[tuple(beside)].set(top_value)


def block_scale(own_key, extent, shards, least, largest):
    def one(dim, blocks):
        heights = jax.random.uniform(jax.random.fold_in(jax.random.fold_in(own_key, 6), dim), (blocks,), jnp.float32, least / len(shards), largest / len(shards))
        return jnp.repeat(jnp.exp(heights), extent[dim] // blocks).reshape((-1,) + (1,) * (len(extent) - dim - 1))

    gain = one(*shards[0])
    for cut in shards[1:]:
        gain = gain * one(*cut)
    return gain


def noise(rng, shape, deviation, limit, split=(), kind=jnp.bfloat16):
    gain = block_scale(rng, shape, split, -0.22, 0.18) if split else 1.0
    entries = jax.random.normal(rng, shape, jnp.float32) * deviation * gain
    return jnp.minimum(jnp.maximum(entries, -limit), limit).astype(kind)


def setup_inputs(seed: int = 0, part: int = 0) -> dict:
    splits = jax.random.split(jax.random.key(seed), 11)
    part_splits = jax.random.split(jax.random.fold_in(splits[10], part), 11)
    return {
        "height": noise(part_splits[0], (NX, NY), 1.0, 6.0, ((0, 32), (1, 2)), jnp.float32),
        "transport_u": noise(part_splits[1], (NX, NY), 0.5, 4.0, ((0, 32), (1, 2)), jnp.float32),
        "transport_v": noise(part_splits[2], (NX, NY), 0.5, 4.0, ((0, 32), (1, 2)), jnp.float32),
        "thickness": jnp.clip(jnp.exp(math.log(2.0) - 1.3862944 * jax.random.uniform(part_splits[3], (LAYERS, NX, NY), jnp.float32) ** block_scale(part_splits[3], (LAYERS, NX, NY), ((1, 32), (2, 2)), -0.2, 0.2)), 0.5, 2.0),
        "velocity_u": noise(part_splits[4], (LAYERS, NX, NY), 0.5, 3.0, ((1, 32), (2, 2)), jnp.float32),
        "velocity_v": noise(part_splits[5], (LAYERS, NX, NY), 0.5, 3.0, ((1, 32), (2, 2)), jnp.float32),
        "sea_faces": plant((jax.random.randint(splits[6], (2, NX, NY), 0, 8) < 7).astype(jnp.int32), jax.random.fold_in(splits[6], 1), 0, 1),
        "wind_seeds": plant(jax.random.randint(part_splits[7], (MODES, 2), 1, 97), jax.random.fold_in(part_splits[7], 1), 1, 96).astype(jnp.int32),
        "wind_scale": jnp.clip(jnp.exp(jax.random.uniform(part_splits[8], (MODES,), jnp.float32, math.log(0.5), math.log(2.0))), 0.5, 2.0),
        "wind_base": noise(splits[9], (2, NX, NY), 1.0, 6.0, ((1, 32), (2, 2)), jnp.float32),
    }


WAVE_LIMIT = 0.225
STRESS_SCALE = 0.1
FLUX_STEP = 0.05
PRESS_COEF = 0.05


def east(field):
    return jnp.roll(field, -1, axis=-2)


def west(field):
    return jnp.roll(field, 1, axis=-2)


def north(field):
    folded = jnp.flip(field[..., -1], axis=-1)
    return jnp.concatenate([field[..., 1:], folded[..., None]], axis=-1)


def south(field):
    return jnp.concatenate([jnp.zeros_like(field[..., :1]), field[..., :-1]], axis=-1)


def reference(height, transport_u, transport_v, thickness, velocity_u, velocity_v, sea_faces, wind_seeds, wind_scale, wind_base):
    total_x = height.shape[0]
    total_y = height.shape[1]
    mask_u = sea_faces[0].astype(jnp.float32)
    mask_v = sea_faces[1].astype(jnp.float32)
    columns = jnp.arange(total_x, dtype=jnp.int32)
    rows_idx = jnp.arange(total_y, dtype=jnp.int32)
    wave_x = wind_seeds[:, 0].astype(jnp.int32)
    wave_y = wind_seeds[:, 1].astype(jnp.int32)
    phase = ((wave_x[:, None, None] * columns[None, :, None]) % total_x).astype(jnp.float32) / total_x
    phase = phase + ((wave_y[:, None, None] * rows_idx[None, None, :]) % total_y).astype(jnp.float32) / total_y
    angle = (2.0 * math.pi) * phase
    amplitude = wind_scale[:, None, None]
    stress_x = STRESS_SCALE * (wind_base[0] + jnp.sum(amplitude * jnp.cos(angle), axis=0))
    stress_y = STRESS_SCALE * (wind_base[1] + jnp.sum(amplitude * jnp.sin(angle), axis=0))
    layers = thickness.shape[0]
    wave = (WAVE_LIMIT / layers) * jnp.sum(thickness, axis=0)
    depth_u = jnp.sum((thickness + east(thickness)) * 0.5, axis=0)
    depth_v = jnp.sum((thickness + north(thickness)) * 0.5, axis=0)
    surface, flow_u, flow_v = height, transport_u, transport_v
    thick, speed_u, speed_v = thickness, velocity_u, velocity_v
    for outer in range(STEPS):
        mean_u = jnp.zeros_like(surface)
        mean_v = jnp.zeros_like(surface)
        for inner in range(NSUB):
            surface = surface - (flow_u - west(flow_u) + flow_v - south(flow_v))
            flow_u = mask_u * (flow_u - wave * (east(surface) - surface) + stress_x)
            flow_v = mask_v * (flow_v - wave * (north(surface) - surface) + stress_y)
            mean_u = mean_u + flow_u
            mean_v = mean_v + flow_v
        mean_u = mean_u / NSUB
        mean_v = mean_v / NSUB
        thick_u = (thick + east(thick)) * 0.5
        thick_v = (thick + north(thick)) * 0.5
        flux_u = speed_u * thick_u
        flux_v = speed_v * thick_v
        pressure = jnp.cumsum(thick, axis=0)
        trial_u = speed_u - PRESS_COEF * (east(pressure) - pressure)
        trial_v = speed_v - PRESS_COEF * (north(pressure) - pressure)
        speed_u = mask_u * (trial_u + (mean_u - jnp.sum(thick_u * trial_u, axis=0)) / depth_u)
        speed_v = mask_v * (trial_v + (mean_v - jnp.sum(thick_v * trial_v, axis=0)) / depth_v)
        thick = thick - FLUX_STEP * (flux_u - west(flux_u) + flux_v - south(flux_v))
    return surface, flow_u, flow_v, thick, speed_u, speed_v
```

```python
import functools
import math

import jax
import jax.numpy as jnp
from jax import lax
from jax.experimental import pallas as pl
from jax.experimental.pallas import tpu as pltpu
from jax.sharding import PartitionSpec as P

NSUB = 6
STEPS = 2
WAVE_LIMIT = 0.225
STRESS_SCALE = 0.1
FLUX_STEP = 0.05
PRESS_COEF = 0.05

MESH = pl.DeviceIdType.MESH
F32 = jnp.float32
OWN, EAST, WEST = 0, 1, 2
LANES = 128
STRIP = 16


def lane_iota(shape):
    return lax.broadcasted_iota(jnp.int32, shape, len(shape) - 1)


def modulo(value, size):
    return value & (size - 1) if size & (size - 1) == 0 else lax.rem(value, size)


def exchange(
    sizes,
    eta_ref, bu_ref, bv_ref, h_ref, u_ref, v_ref, faces_ref, base_ref, seeds_ref, scale_ref,
    own_ref, east_ref, west_ref, least_ref, lwest_ref, north_ref, south_ref,
    goeast, gowest, top, bottom, send, recv,
):
    devices = sizes
    z = lax.axis_index("zonal")
    c = lax.axis_index("merid")
    e = lax.rem(z + 1, devices)
    w = lax.rem(z + devices - 1, devices)
    other = 1 - c
    far = [lax.rem(2 * devices - 1 - z + d, devices) for d in (0, -1, 1)]

    barrier = pltpu.get_barrier_semaphore()

    def greet(zonal, merid):
        pl.semaphore_signal(
            barrier, inc=1, device_id={"zonal": zonal, "merid": merid}, device_id_type=MESH
        )

    greet(e, c)
    greet(w, c)
    for target in (z, e, w):
        greet(target, other)
    for target in far:
        @pl.when(jnp.logical_and(c == 1, target != z))
        def _(target=target):
            greet(target, c)

    layers, cells, rows = h_ref.shape
    total_x = cells * devices
    total_y = rows * 2
    h_sum = h_ref[0]
    for l in range(1, layers):
        h_sum = h_sum + h_ref[l]
    wave = (WAVE_LIMIT / layers) * h_sum
    mask_u = faces_ref[0].astype(F32)
    mask_v = faces_ref[1].astype(F32)
    cols = lax.broadcasted_iota(jnp.int32, (cells, LANES), 0) + z * cells
    rws = lax.broadcasted_iota(jnp.int32, (8, rows), 1) + c * rows
    sum_cos = jnp.zeros((cells, rows), F32)
    sum_sin = jnp.zeros((cells, rows), F32)
    for m in range(seeds_ref.shape[0]):
        ax = (2.0 * math.pi / total_x) * modulo(seeds_ref[m, 0] * cols, total_x).astype(F32)
        ay = (2.0 * math.pi / total_y) * modulo(seeds_ref[m, 1] * rws, total_y).astype(F32)
        amp = scale_ref[m]
        cx = jnp.concatenate([amp * jnp.cos(ax)] * (rows // LANES), 1)
        sx = jnp.concatenate([amp * jnp.sin(ax)] * (rows // LANES), 1)
        cy = jnp.concatenate([jnp.cos(ay)] * (cells // 8), 0)
        sy = jnp.concatenate([jnp.sin(ay)] * (cells // 8), 0)
        sum_cos = sum_cos + (cx * cy - sx * sy)
        sum_sin = sum_sin + (sx * cy + cx * sy)
    own_ref[0] = mask_u * wave
    own_ref[1] = mask_v * wave
    own_ref[2] = mask_u * (STRESS_SCALE * (base_ref[0] + sum_cos))
    own_ref[3] = mask_v * (STRESS_SCALE * (base_ref[1] + sum_sin))
    own_ref[4] = eta_ref[...]
    own_ref[5] = bu_ref[...]
    own_ref[6] = bv_ref[...]
    pad = jnp.zeros((16 - layers, rows), F32)
    last = cells - 1
    for k, (ref, col) in enumerate(((h_ref, last), (h_ref, last - 1), (u_ref, last), (u_ref, last - 1), (v_ref, last))):
        goeast[k] = jnp.concatenate([ref[:, col, :], pad], 0)
    for k, (ref, col) in enumerate(((h_ref, 0), (h_ref, 1), (u_ref, 0), (v_ref, 0))):
        gowest[k] = jnp.concatenate([ref[:, col, :], pad], 0)
    lane = lane_iota((cells, LANES))
    hi = rows - LANES
    base_t = jnp.zeros((cells, LANES), F32)
    base_b = jnp.zeros((cells, LANES), F32)
    for f in range(7):
        here = lane // STRIP == f
        base_t = jnp.where(here, pltpu.roll(own_ref[f, :, hi:], (f * STRIP + STRIP) % LANES, 1), base_t)
        low = own_ref[f, :, :LANES]
        base_b = jnp.where(here, pltpu.roll(low, f * STRIP, 1) if f else low, base_b)
    lay_t = jnp.zeros((cells, LANES), F32)
    lay_b = jnp.zeros((cells, LANES), F32)
    for start, width, ref in ((0, 2, h_ref), (2 * layers, 2, v_ref), (4 * layers, 1, u_ref)):
        for l in range(layers):
            spot = start + width * l
            here = jnp.logical_and(lane >= spot, lane < spot + width)
            lay_t = jnp.where(here, pltpu.roll(ref[l, :, hi:], (spot + width) % LANES, 1), lay_t)
            low = ref[l, :, :LANES]
            lay_b = jnp.where(here, pltpu.roll(low, spot, 1) if spot else low, lay_b)
    bottom[:, :LANES] = base_b
    bottom[:, LANES:] = lay_b
    r2 = lax.broadcasted_iota(jnp.int32, (LANES, LANES), 0)
    c2 = lax.broadcasted_iota(jnp.int32, (LANES, LANES), 1)
    perm_b = jnp.where(r2 == (c2 ^ (STRIP - 1)), 1.0, 0.0).astype(F32)
    perm_l = jnp.where(r2 == jnp.where(c2 < 4 * layers, c2 ^ 1, c2), 1.0, 0.0).astype(F32)
    r1 = lax.broadcasted_iota(jnp.int32, (cells, cells), 0)
    c1 = lax.broadcasted_iota(jnp.int32, (cells, cells), 1)
    mirror = jnp.where(r1 + c1 == cells - 1, 1.0, 0.0).astype(F32)
    dot = functools.partial(
        jnp.dot, preferred_element_type=F32, precision=lax.Precision.HIGHEST
    )
    north_edge = c == 1
    top[:, :LANES] = jnp.where(north_edge, dot(mirror, dot(base_t, perm_b)), base_t)
    top[:, LANES:] = jnp.where(north_edge, dot(mirror, dot(lay_t, perm_l)), lay_t)

    @pl.when(c == 0)
    def _():
        south_ref[...] = jnp.zeros_like(south_ref)

    for target, slot in zip(far, (OWN, EAST, WEST)):
        @pl.when(jnp.logical_and(c == 1, target == z))
        def _(slot=slot):
            north_ref[slot] = top[...]

    alone = sum(jnp.where(target == z, 1, 0) for target in far)
    pl.semaphore_wait(barrier, 5 + c * (3 - alone))

    def copy(src, dst, k, zonal, merid):
        return pltpu.make_async_remote_copy(
            src_ref=src, dst_ref=dst, send_sem=send.at[k], recv_sem=recv.at[k],
            device_id={"zonal": zonal, "merid": merid}, device_id_type=MESH,
        )

    far_copies = [
        copy(top, north_ref.at[slot], 4 + slot, target, c)
        for target, slot in zip(far, (OWN, EAST, WEST))
    ]
    up_copies = [
        copy(top, south_ref.at[slot], 7 + slot, target, other)
        for target, slot in zip((z, w, e), (OWN, EAST, WEST))
    ]
    down_copies = [
        copy(bottom, north_ref.at[slot], 10 + slot, target, other)
        for target, slot in zip((z, w, e), (OWN, EAST, WEST))
    ]
    side_copies = [
        copy(goeast, lwest_ref, 0, e, c),
        copy(gowest, least_ref, 1, w, c),
        copy(own_ref, west_ref, 2, e, c),
        copy(own_ref, east_ref, 3, w, c),
    ]
    for target, cp in zip(far, far_copies):
        @pl.when(jnp.logical_and(c == 1, target != z))
        def _(cp=cp):
            cp.start()

    @pl.when(c == 0)
    def _():
        for cp in up_copies:
            cp.start()

    @pl.when(c == 1)
    def _():
        for cp in down_copies:
            cp.start()

    for cp in side_copies:
        cp.start()
    for cp in side_copies:
        cp.wait()

    @pl.when(c == 0)
    def _():
        for cp in up_copies:
            cp.wait_send()
        for cp in down_copies:
            cp.wait_recv()

    @pl.when(c == 1)
    def _():
        for cp in down_copies:
            cp.wait_send()
        for cp in up_copies:
            cp.wait_recv()

    for target, cp in zip(far, far_copies):
        @pl.when(jnp.logical_and(c == 1, target != z))
        def _(cp=cp):
            cp.wait()


def advance(
    h_ref, u_ref, v_ref, own_ref, east_ref, west_ref, least_ref, lwest_ref, north_ref, south_ref,
    eta_out, bu_out, bv_out, h_out, u_out, v_out,
    base, lay, trial,
):
    layers, cells, rows = h_ref.shape
    wide = rows + LANES
    lane = lane_iota((cells, LANES))
    first = lane < LANES // 2
    fold1 = jnp.logical_and(lane_iota((8, LANES)) < LANES // 2, lax.axis_index("merid") == 1)

    def rolled(x, shift, axis):
        shift = shift % x.shape[axis]
        return pltpu.roll(x, shift, axis) if shift else x

    def fold_of(x):
        return jnp.concatenate([fold1] * (x.shape[0] // 8), 0)

    def merge(main, alt):
        halo = jnp.where(fold_of(alt), alt, main[:, rows:])
        return jnp.concatenate([main[:, :rows], halo], 1)

    def at_west(x):
        return merge(rolled(x, 1, 0), rolled(x[:, rows:], -1, 0))

    def at_east(x):
        return merge(rolled(x, -1, 0), rolled(x[:, rows:], 1, 0))

    def at_south(x):
        return merge(rolled(x, 1, 1), rolled(x[:, rows:], -1, 1))

    def at_north(x):
        return merge(rolled(x, -1, 1), rolled(x[:, rows - LANES:], 1, 1)[:, LANES:])

    for f in range(7):
        for slot, ref in ((OWN, own_ref), (EAST, east_ref), (WEST, west_ref)):
            place = slice(slot * cells, (slot + 1) * cells)
            base[f, place, :rows] = ref[f]
            base[f, place, rows:] = jnp.where(
                first,
                rolled(north_ref[slot, :, :LANES], -STRIP * f, 1),
                rolled(south_ref[slot, :, :LANES], LANES - STRIP - STRIP * f, 1),
            )
    near = lax.broadcasted_iota(jnp.int32, (8, LANES), 0) < 4

    def around(x):
        return jnp.concatenate([x[OWN], jnp.where(near, x[EAST][:8], x[WEST][cells - 8:])], 0)

    north = around([north_ref[s, :, LANES:] for s in range(3)])
    south = around([south_ref[s, :, LANES:] for s in range(3)])
    first24 = lane_iota(north.shape) < LANES // 2
    ext = cells + 8
    H, U, V = 0, 1, 2
    for kind, ref, start, width, east_cols, west_cols in (
        (H, h_ref, 0, 2, (0, 1), (0, 1)),
        (U, u_ref, 4 * layers, 1, (2,), (2, 3)),
        (V, v_ref, 2 * layers, 2, (3,), (4,)),
    ):
        for l in range(layers):
            spot = start + width * l
            lay[kind, l, :cells, :rows] = ref[l]
            lay[kind, l, cells:, :rows] = jnp.zeros((8, rows), F32)
            lay[kind, l, :, rows:] = jnp.where(
                first24, rolled(north, -spot, 1), rolled(south, LANES - width - spot, 1)
            )
            for k, src in enumerate(east_cols):
                lay[kind, l, cells + k: cells + k + 1, :rows] = least_ref[src, l: l + 1, :]
            for k, src in enumerate(west_cols):
                lay[kind, l, ext - 1 - k: ext - k, :rows] = lwest_ref[src, l: l + 1, :]

    def trimmed(x):
        wide_near = lax.broadcasted_iota(jnp.int32, (8, wide), 0) < 4
        return jnp.concatenate([x[:cells], jnp.where(wide_near, x[cells: cells + 8], x[3 * cells - 8:])], 0)

    mask_u = trimmed(base[0]) != 0.0
    mask_v = trimmed(base[1]) != 0.0
    depth_u = None
    depth_v = None
    for outer in range(STEPS):
        def substep(_, sums):
            sum_u, sum_v = sums
            bu = base[5]
            bv = base[6]
            eta = base[4] - (bu - at_west(bu) + bv - at_south(bv))
            base[4] = eta
            au = base[0]
            bu = jnp.where(au != 0.0, bu - au * (at_east(eta) - eta) + base[2], 0.0)
            base[5] = bu
            av = base[1]
            bv = jnp.where(av != 0.0, bv - av * (at_north(eta) - eta) + base[3], 0.0)
            base[6] = bv
            return sum_u + trimmed(bu), sum_v + trimmed(bv)

        zero = jnp.zeros((ext, wide), F32)
        sum_u, sum_v = lax.fori_loop(0, NSUB, substep, (zero, zero))
        press_u = zero
        press_v = zero
        deep_u = zero
        deep_v = zero
        total_u = zero
        total_v = zero
        for l in range(layers):
            h = lay[H, l]
            u = lay[U, l]
            v = lay[V, l]
            diff_u = at_east(h) - h
            diff_v = at_north(h) - h
            press_u = press_u + diff_u
            press_v = press_v + diff_v
            hu = h + 0.5 * diff_u
            hv = h + 0.5 * diff_v
            flux_u = u * hu
            flux_v = v * hv
            new = h - FLUX_STEP * (flux_u - at_west(flux_u) + flux_v - at_south(flux_v))
            if outer == STEPS - 1:
                h_out[l] = new[:cells, :rows]
            else:
                lay[H, l] = new
            ut = u - PRESS_COEF * press_u
            vt = v - PRESS_COEF * press_v
            trial[0, l] = ut
            trial[1, l] = vt
            total_u = total_u + hu * ut
            total_v = total_v + hv * vt
            if outer == 0:
                deep_u = deep_u + hu
                deep_v = deep_v + hv
        if outer == 0:
            depth_u, depth_v = deep_u, deep_v
        fix_u = (sum_u * (1.0 / NSUB) - total_u) / depth_u
        fix_v = (sum_v * (1.0 / NSUB) - total_v) / depth_v
        for l in range(layers):
            u = jnp.where(mask_u, trial[0, l] + fix_u, 0.0)
            v = jnp.where(mask_v, trial[1, l] + fix_v, 0.0)
            if outer == STEPS - 1:
                u_out[l] = u[:cells, :rows]
                v_out[l] = v[:cells, :rows]
            else:
                lay[U, l] = u
                lay[V, l] = v
    eta_out[...] = base[4, :cells, :rows]
    bu_out[...] = base[5, :cells, :rows]
    bv_out[...] = base[6, :cells, :rows]


def body(
    devices, height, transport_u, transport_v, thickness, velocity_u, velocity_v,
    sea_faces, wind_seeds, wind_scale, wind_base,
):
    layers, cells, rows = thickness.shape
    vmem = pl.BlockSpec(memory_space=pltpu.VMEM)
    smem = pl.BlockSpec(memory_space=pltpu.SMEM)

    def shape(*dims):
        return jax.ShapeDtypeStruct(dims, F32)

    halos = pl.pallas_call(
        functools.partial(exchange, devices),
        out_shape=[
            shape(7, cells, rows), shape(7, cells, rows), shape(7, cells, rows),
            shape(4, 16, rows), shape(5, 16, rows),
            shape(3, cells, 2 * LANES), shape(3, cells, 2 * LANES),
        ],
        in_specs=[vmem] * 8 + [smem] * 2,
        out_specs=[vmem] * 7,
        scratch_shapes=[
            pltpu.VMEM((5, 16, rows), F32),
            pltpu.VMEM((4, 16, rows), F32),
            pltpu.VMEM((cells, 2 * LANES), F32),
            pltpu.VMEM((cells, 2 * LANES), F32),
            pltpu.SemaphoreType.DMA((13,)),
            pltpu.SemaphoreType.DMA((13,)),
        ],
        compiler_params=pltpu.CompilerParams(collective_id=0, has_side_effects=True),
        name="exchange",
    )(
        height, transport_u, transport_v, thickness, velocity_u, velocity_v,
        sea_faces, wind_base, wind_seeds, wind_scale,
    )
    return pl.pallas_call(
        advance,
        out_shape=[shape(cells, rows)] * 3 + [shape(layers, cells, rows)] * 3,
        in_specs=[vmem] * 10,
        out_specs=[vmem] * 6,
        scratch_shapes=[
            pltpu.VMEM((7, 3 * cells, rows + LANES), F32),
            pltpu.VMEM((3, layers, cells + 8, rows + LANES), F32),
            pltpu.VMEM((2, layers, cells + 8, rows + LANES), F32),
        ],
        name="advance",
    )(thickness, velocity_u, velocity_v, *halos)


def solution(mesh):
    flat = P(("members", "zonal"), "merid")
    deep = P(None, ("members", "zonal"), "merid")
    fixed = P(None, "zonal", "merid")
    return jax.shard_map(
        functools.partial(body, mesh.shape["zonal"]),
        mesh=mesh,
        in_specs=(flat, flat, flat, deep, deep, deep, fixed, P("members", None), P("members"), fixed),
        out_specs=(flat, flat, flat, deep, deep, deep),
        check_vma=False,
    )
```

```python
import functools
import math

import jax
import jax.numpy as jnp
from jax import lax
from jax.experimental import pallas as pl
from jax.experimental.pallas import tpu as pltpu
from jax.sharding import PartitionSpec as P

NSUB = 6
STEPS = 2
WAVE_LIMIT = 0.225
STRESS_SCALE = 0.1
FLUX_STEP = 0.05
PRESS_COEF = 0.05

MESH = pl.DeviceIdType.MESH
F32 = jnp.float32
OWN, EAST, WEST = 0, 1, 2
LANES = 128
STRIP = 16


def lane_iota(shape):
    return lax.broadcasted_iota(jnp.int32, shape, len(shape) - 1)


def modulo(value, size):
    return value & (size - 1) if size & (size - 1) == 0 else lax.rem(value, size)


def rolled(x, shift, axis):
    shift = shift % x.shape[axis]
    return pltpu.roll(x, shift, axis) if shift else x


def neighbours(rows):
    fold1 = jnp.logical_and(lane_iota((8, LANES)) < LANES // 2, lax.axis_index("merid") == 1)

    def merge(main, alt):
        fold = jnp.concatenate([fold1] * (alt.shape[0] // 8), 0)
        halo = jnp.where(fold, alt, main[:, rows:])
        return jnp.concatenate([main[:, :rows], halo], 1)

    def at_west(x):
        return merge(rolled(x, 1, 0), rolled(x[:, rows:], -1, 0))

    def at_east(x):
        return merge(rolled(x, -1, 0), rolled(x[:, rows:], 1, 0))

    def at_south(x):
        return merge(rolled(x, 1, 1), rolled(x[:, rows:], -1, 1))

    def at_north(x):
        return merge(rolled(x, -1, 1), rolled(x[:, rows - LANES:], 1, 1)[:, LANES:])

    return at_east, at_west, at_south, at_north


def exchange(
    devices,
    eta_ref, bu_ref, bv_ref, h_ref, u_ref, v_ref, faces_ref, base_ref, seeds_ref, scale_ref,
    lay, means, faces_out, state_out,
    base, faces, winds, seeds, scale, goeast, gowest, least, lwest, outw, oute, inw, ine,
    top, bottom, north_ref, south_ref,
    load, send, recv, near_ok, far_ok,
):
    z = lax.axis_index("zonal")
    c = lax.axis_index("merid")
    e = lax.rem(z + 1, devices)
    w = lax.rem(z + devices - 1, devices)
    other = 1 - c
    far = [lax.rem(2 * devices - 1 - z + d, devices) for d in (0, -1, 1)]
    layers, cells, rows = h_ref.shape
    wide = rows + LANES
    ext = cells + 8
    H, U, V = 0, 1, 2

    barrier = pltpu.get_barrier_semaphore()

    def greet(zonal, merid):
        pl.semaphore_signal(
            barrier, inc=1, device_id={"zonal": zonal, "merid": merid}, device_id_type=MESH
        )

    greet(e, 1)
    greet(w, 1)

    @pl.when(c == 0)
    def _():
        greet(z, 1)

    @pl.when(c == 1)
    def _():
        for target in far:
            greet(target, 0)

    fetches = [
        pltpu.make_async_copy(src, dst, load.at[k])
        for k, (src, dst) in enumerate((
            (h_ref, lay.at[H, :, pl.ds(0, cells), pl.ds(0, rows)]),
            (seeds_ref, seeds),
            (scale_ref, scale),
            (faces_ref, faces),
            (base_ref, winds),
            (eta_ref, base.at[4, pl.ds(0, cells), pl.ds(0, rows)]),
            (bu_ref, base.at[5, pl.ds(0, cells), pl.ds(0, rows)]),
            (bv_ref, base.at[6, pl.ds(0, cells), pl.ds(0, rows)]),
            (u_ref, lay.at[U, :, pl.ds(0, cells), pl.ds(0, rows)]),
            (v_ref, lay.at[V, :, pl.ds(0, cells), pl.ds(0, rows)]),
        ))
    ]
    for cp in fetches:
        cp.start()
    for cp in fetches[1:5]:
        cp.wait()
    total_x = cells * devices
    total_y = rows * 2
    cols = lax.broadcasted_iota(jnp.int32, (cells, LANES), 0) + z * cells
    rws = lax.broadcasted_iota(jnp.int32, (8, rows), 1) + c * rows
    sum_cos = jnp.zeros((cells, rows), F32)
    sum_sin = jnp.zeros((cells, rows), F32)
    for m in range(seeds.shape[1]):
        ax = (2.0 * math.pi / total_x) * modulo(seeds[0, m] * cols, total_x).astype(F32)
        ay = (2.0 * math.pi / total_y) * modulo(seeds[1, m] * rws, total_y).astype(F32)
        amp = scale[m]
        cx = jnp.concatenate([amp * jnp.cos(ax)] * (rows // LANES), 1)
        sx = jnp.concatenate([amp * jnp.sin(ax)] * (rows // LANES), 1)
        cy = jnp.concatenate([jnp.cos(ay)] * (cells // 8), 0)
        sy = jnp.concatenate([jnp.sin(ay)] * (cells // 8), 0)
        sum_cos = sum_cos + (cx * cy - sx * sy)
        sum_sin = sum_sin + (sx * cy + cx * sy)
    mask_u = faces[0].astype(F32)
    mask_v = faces[1].astype(F32)
    base[2, :cells, :rows] = mask_u * (STRESS_SCALE * (winds[0] + sum_cos))
    base[3, :cells, :rows] = mask_v * (STRESS_SCALE * (winds[1] + sum_sin))
    fetches[0].wait()
    h_sum = lay[H, 0, :cells, :rows]
    for l in range(1, layers):
        h_sum = h_sum + lay[H, l, :cells, :rows]
    wave = (WAVE_LIMIT / layers) * h_sum
    base[0, :cells, :rows] = mask_u * wave
    base[1, :cells, :rows] = mask_v * wave
    for cp in fetches[5:]:
        cp.wait()
    low4 = lax.broadcasted_iota(jnp.int32, (8, rows), 0) < 4
    for k in range(4):
        a = base[2 * k, 0:8, :rows]
        b = base[2 * k, 8:16, :rows]
        if 2 * k + 1 < 7:
            a = jnp.where(low4, pltpu.roll(base[2 * k + 1, 0:8, :rows], 4, 0), a)
            b = jnp.where(low4, b, pltpu.roll(base[2 * k + 1, 8:16, :rows], 4, 0))
        oute[k] = a
        outw[k] = b
    last = cells - 1
    for k, (kind, col) in enumerate(((H, last), (H, last - 1), (U, last), (U, last - 1), (V, last))):
        goeast[k * layers: (k + 1) * layers] = lay[kind, :, col, :rows]
    for k, (kind, col) in enumerate(((H, 0), (H, 1), (U, 0), (V, 0))):
        gowest[k * layers: (k + 1) * layers] = lay[kind, :, col, :rows]

    def copy(src, dst, k, zonal, merid):
        return pltpu.make_async_remote_copy(
            src_ref=src, dst_ref=dst, send_sem=send.at[k], recv_sem=recv.at[k],
            device_id={"zonal": zonal, "merid": merid}, device_id_type=MESH,
        )

    lanes = pl.ds(0, rows)
    side_copies = [
        copy(base.at[:, pl.ds(8, 8), lanes], base.at[:, pl.ds(32, 8), lanes], 0, e, c),
        copy(base.at[:, pl.ds(0, 8), lanes], base.at[:, pl.ds(16, 8), lanes], 1, w, c),
        copy(oute, inw, 2, e, c),
        copy(outw, ine, 3, w, c),
    ]
    column_copies = [
        copy(goeast, lwest, 13, e, c),
        copy(gowest, least, 14, w, c),
    ]

    @pl.when(c == 1)
    def _():
        pl.semaphore_wait(barrier, 5)
        pl.semaphore_signal(
            near_ok, inc=1, device_id={"zonal": z, "merid": other}, device_id_type=MESH
        )

    @pl.when(c == 0)
    def _():
        pl.semaphore_wait(near_ok, 1)

    for cp in side_copies:
        cp.start()
    lane = lane_iota((cells, LANES))
    hi = rows - LANES
    base_t = jnp.zeros((cells, LANES), F32)
    base_b = jnp.zeros((cells, LANES), F32)
    for f in range(7):
        here = lane // STRIP == f
        base_t = jnp.where(here, rolled(base[f, :cells, hi:rows], f * STRIP + STRIP, 1), base_t)
        base_b = jnp.where(here, rolled(base[f, :cells, :LANES], f * STRIP, 1), base_b)
    lay_t = jnp.zeros((cells, LANES), F32)
    lay_b = jnp.zeros((cells, LANES), F32)
    for start, width, kind in ((0, 2, H), (2 * layers, 2, V), (4 * layers, 1, U)):
        for l in range(layers):
            spot = start + width * l
            here = jnp.logical_and(lane >= spot, lane < spot + width)
            lay_t = jnp.where(here, rolled(lay[kind, l, :cells, hi:rows], spot + width, 1), lay_t)
            lay_b = jnp.where(here, rolled(lay[kind, l, :cells, :LANES], spot, 1), lay_b)
    bottom[:, :LANES] = base_b
    bottom[:, LANES:] = lay_b
    r2 = lax.broadcasted_iota(jnp.int32, (LANES, LANES), 0)
    c2 = lax.broadcasted_iota(jnp.int32, (LANES, LANES), 1)
    perm_b = jnp.where(r2 == (c2 ^ (STRIP - 1)), 1.0, 0.0).astype(F32)
    perm_l = jnp.where(r2 == jnp.where(c2 < 4 * layers, c2 ^ 1, c2), 1.0, 0.0).astype(F32)
    r1 = lax.broadcasted_iota(jnp.int32, (cells, cells), 0)
    c1 = lax.broadcasted_iota(jnp.int32, (cells, cells), 1)
    mirror = jnp.where(r1 + c1 == cells - 1, 1.0, 0.0).astype(F32)
    dot = functools.partial(
        jnp.dot, preferred_element_type=F32, precision=lax.Precision.HIGHEST
    )
    north_edge = c == 1
    top[:, :LANES] = jnp.where(north_edge, dot(mirror, dot(base_t, perm_b)), base_t)
    top[:, LANES:] = jnp.where(north_edge, dot(mirror, dot(lay_t, perm_l)), lay_t)

    far_copies = [
        copy(top, north_ref.at[slot], 4 + slot, target, c)
        for target, slot in zip(far, (OWN, EAST, WEST))
    ]
    up_copies = [
        copy(top, south_ref.at[slot], 7 + slot, target, other)
        for target, slot in zip((z, w, e), (OWN, EAST, WEST))
    ]
    down_copies = [
        copy(bottom, north_ref.at[slot], 10 + slot, target, other)
        for target, slot in zip((z, w, e), (OWN, EAST, WEST))
    ]

    @pl.when(c == 0)
    def _():
        for cp in up_copies:
            cp.start()

    @pl.when(c == 1)
    def _():
        for cp in down_copies:
            cp.start()

    for cp in column_copies:
        cp.start()

    @pl.when(c == 0)
    def _():
        south_ref[...] = jnp.zeros_like(south_ref)
        pl.semaphore_wait(barrier, 3)
        pl.semaphore_signal(
            far_ok, inc=1, device_id={"zonal": z, "merid": other}, device_id_type=MESH
        )

    @pl.when(c == 1)
    def _():
        pl.semaphore_wait(far_ok, 1)

    for target, cp, slot in zip(far, far_copies, (OWN, EAST, WEST)):
        @pl.when(jnp.logical_and(c == 1, target != z))
        def _(cp=cp):
            cp.start()

        @pl.when(jnp.logical_and(c == 1, target == z))
        def _(slot=slot):
            north_ref[slot] = top[...]

    for kind in (H, U, V):
        for l in range(layers):
            lay[kind, l, cells:, :rows] = jnp.zeros((8, rows), F32)

    for cp in side_copies:
        cp.wait()

    @pl.when(c == 0)
    def _():
        for cp in up_copies:
            cp.wait_send()
        for cp in down_copies:
            cp.wait_recv()

    @pl.when(c == 1)
    def _():
        for cp in down_copies:
            cp.wait_send()
        for cp in up_copies:
            cp.wait_recv()

    for target, cp in zip(far, far_copies):
        @pl.when(jnp.logical_and(c == 1, target != z))
        def _(cp=cp):
            cp.wait()

    for k in range(4):
        from_w = inw[k]
        from_e = ine[k]
        base[2 * k, 24:32, :rows] = jnp.where(low4, from_e, from_w)
        if 2 * k + 1 < 7:
            base[2 * k + 1, 24:32, :rows] = pltpu.roll(jnp.where(low4, from_w, from_e), 4, 0)
    first8 = lane_iota((8, LANES)) < LANES // 2
    far_rows = lax.broadcasted_iota(jnp.int32, (8, LANES), 0) < 4
    norths = [north_ref[s, :, :LANES] for s in range(3)]
    souths = [south_ref[s, :, :LANES] for s in range(3)]

    def ring(x):
        outer = jnp.where(far_rows, x[EAST][8:], x[WEST][:8])
        return (x[OWN][:8], x[OWN][8:], x[EAST][:8], outer, x[WEST][8:])

    for k, (n, s) in enumerate(zip(ring(norths), ring(souths))):
        for f in range(7):
            base[f, 8 * k: 8 * k + 8, rows:] = jnp.where(
                first8, rolled(n, -STRIP * f, 1), rolled(s, LANES - STRIP - STRIP * f, 1)
            )
    at_east, at_west, at_south, at_north = neighbours(rows)
    near = lax.broadcasted_iota(jnp.int32, (8, wide), 0) < 4

    def trimmed(x):
        size = x.shape[0]
        return jnp.concatenate([x[:cells], jnp.where(near, x[cells: cells + 8], x[size - 8:])], 0)

    faces_out[0] = trimmed(base[0])
    faces_out[1] = trimmed(base[1])

    def substep(narrow):
        def get(f):
            if narrow:
                return jnp.concatenate([base[f, :cells + 8], base[f, cells + 16:]], 0)
            return base[f]

        def put(f, x):
            if narrow:
                base[f, :cells + 8] = x[:cells + 8]
                base[f, cells + 16:] = x[cells + 8:]
            else:
                base[f] = x

        def run(_, sums):
            sum_u, sum_v = sums
            bu = get(5)
            bv = get(6)
            eta = get(4) - (bu - at_west(bu) + bv - at_south(bv))
            put(4, eta)
            au = get(0)
            bu = jnp.where(au != 0.0, bu - au * (at_east(eta) - eta) + get(2), 0.0)
            put(5, bu)
            av = get(1)
            bv = jnp.where(av != 0.0, bv - av * (at_north(eta) - eta) + get(3), 0.0)
            put(6, bv)
            return sum_u + trimmed(bu), sum_v + trimmed(bv)

        return run

    outer_steps = 2 * NSUB - 8
    zero = jnp.zeros((ext, wide), F32)
    for step in range(STEPS):
        sums = (zero, zero)
        if step == 0:
            sums = lax.fori_loop(0, outer_steps, substep(False), sums)
            sums = lax.fori_loop(outer_steps, NSUB, substep(True), sums)
        else:
            sums = lax.fori_loop(0, NSUB, substep(True), sums)
        means[step, 0] = sums[0] * (1.0 / NSUB)
        means[step, 1] = sums[1] * (1.0 / NSUB)
    for k in range(3):
        state_out[k] = base[4 + k, :cells, :rows]

    def around(x):
        return jnp.concatenate([x[OWN], jnp.where(far_rows, x[EAST][:8], x[WEST][cells - 8:])], 0)

    north = around([north_ref[s, :, LANES:] for s in range(3)])
    south = around([south_ref[s, :, LANES:] for s in range(3)])
    first24 = lane_iota(north.shape) < LANES // 2
    for kind, start, width in ((H, 0, 2), (U, 4 * layers, 1), (V, 2 * layers, 2)):
        for l in range(layers):
            spot = start + width * l
            lay[kind, l, :, rows:] = jnp.where(
                first24, rolled(north, -spot, 1), rolled(south, LANES - width - spot, 1)
            )
    for cp in column_copies:
        cp.wait()
    for kind, east_cols, west_cols in ((H, (0, 1), (0, 1)), (U, (2,), (2, 3)), (V, (3,), (4,))):
        for l in range(layers):
            for k, src in enumerate(east_cols):
                lay[kind, l, cells + k: cells + k + 1, :rows] = least[src * layers + l: src * layers + l + 1, :]
            for k, src in enumerate(west_cols):
                lay[kind, l, ext - 1 - k: ext - k, :rows] = lwest[src * layers + l: src * layers + l + 1, :]


def advance(
    lay_in, means, faces, state, eta_out, bu_out, bv_out, h_out, u_out, v_out,
    lay, trial, results, done,
):
    layers, cells, rows = h_out.shape
    wide = rows + LANES
    ext = cells + 8
    H, U, V = 0, 1, 2
    at_east, at_west, at_south, at_north = neighbours(rows)
    stores = [
        pltpu.make_async_copy(state.at[k], out, done.at[k])
        for k, out in enumerate((eta_out, bu_out, bv_out))
    ] + [
        pltpu.make_async_copy(results.at[k], out, done.at[3 + k])
        for k, out in enumerate((h_out, u_out, v_out))
    ]
    for cp in stores[:3]:
        cp.start()
    zero = jnp.zeros((ext, wide), F32)
    depth_u = None
    depth_v = None
    for outer in range(STEPS):
        source = lay_in if outer == 0 else lay
        press_u = zero
        press_v = zero
        deep_u = zero
        deep_v = zero
        total_u = zero
        total_v = zero
        for l in range(layers):
            h = source[H, l]
            u = source[U, l]
            v = source[V, l]
            diff_u = at_east(h) - h
            diff_v = at_north(h) - h
            press_u = press_u + diff_u
            press_v = press_v + diff_v
            hu = h + 0.5 * diff_u
            hv = h + 0.5 * diff_v
            flux_u = u * hu
            flux_v = v * hv
            new = h - FLUX_STEP * (flux_u - at_west(flux_u) + flux_v - at_south(flux_v))
            if outer == STEPS - 1:
                results[0, l] = new[:cells, :rows]
            else:
                lay[H, l] = new
            ut = u - PRESS_COEF * press_u
            vt = v - PRESS_COEF * press_v
            trial[0, l] = ut
            trial[1, l] = vt
            total_u = total_u + hu * ut
            total_v = total_v + hv * vt
            if outer == 0:
                deep_u = deep_u + hu
                deep_v = deep_v + hv
        if outer == 0:
            depth_u, depth_v = deep_u, deep_v
        if outer == STEPS - 1:
            stores[3].start()
        fix_u = (means[outer, 0] - total_u) / depth_u
        fix_v = (means[outer, 1] - total_v) / depth_v
        for k, fix in ((U, fix_u), (V, fix_v)):
            open_face = faces[k - 1] != 0.0
            for l in range(layers):
                new = jnp.where(open_face, trial[k - 1, l] + fix, 0.0)
                if outer == STEPS - 1:
                    results[k, l] = new[:cells, :rows]
                else:
                    lay[k, l] = new
            if outer == STEPS - 1:
                stores[3 + k].start()
    for cp in stores:
        cp.wait()


def body(
    devices, height, transport_u, transport_v, thickness, velocity_u, velocity_v,
    sea_faces, wind_seeds, wind_scale, wind_base,
):
    layers, cells, rows = thickness.shape
    wide = rows + LANES
    ext = cells + 8
    anywhere = pl.BlockSpec(memory_space=pl.ANY)
    vmem = pl.BlockSpec(memory_space=pltpu.VMEM)

    def shape(*dims):
        return jax.ShapeDtypeStruct(dims, F32)

    def inner(*dims):
        return pltpu.VMEM(dims, F32)

    mid = pl.pallas_call(
        functools.partial(exchange, devices),
        out_shape=[
            inner(3, layers, ext, wide), inner(STEPS, 2, ext, wide), inner(2, ext, wide),
            inner(3, cells, rows),
        ],
        in_specs=[anywhere] * 10,
        out_specs=[vmem] * 4,
        scratch_shapes=[
            inner(7, cells + 24, wide),
            pltpu.VMEM(sea_faces.shape, sea_faces.dtype),
            inner(*wind_base.shape),
            pltpu.SMEM(wind_seeds.shape[::-1], wind_seeds.dtype),
            pltpu.SMEM(wind_scale.shape, F32),
            inner(72, rows), inner(56, rows), inner(56, rows), inner(72, rows),
            inner(4, 8, rows), inner(4, 8, rows), inner(4, 8, rows), inner(4, 8, rows),
            inner(cells, 2 * LANES), inner(cells, 2 * LANES),
            inner(3, cells, 2 * LANES), inner(3, cells, 2 * LANES),
            pltpu.SemaphoreType.DMA((10,)),
            pltpu.SemaphoreType.DMA((15,)),
            pltpu.SemaphoreType.DMA((15,)),
            pltpu.SemaphoreType.REGULAR,
            pltpu.SemaphoreType.REGULAR,
        ],
        compiler_params=pltpu.CompilerParams(collective_id=0, has_side_effects=True),
        name="exchange",
    )(
        height, transport_u, transport_v, thickness, velocity_u, velocity_v,
        sea_faces, wind_base, wind_seeds.T, wind_scale,
    )
    return pl.pallas_call(
        advance,
        out_shape=[shape(cells, rows)] * 3 + [shape(layers, cells, rows)] * 3,
        in_specs=[vmem] * 4,
        out_specs=[anywhere] * 6,
        scratch_shapes=[
            inner(3, layers, ext, wide),
            inner(2, layers, ext, wide),
            inner(3, layers, cells, rows),
            pltpu.SemaphoreType.DMA((6,)),
        ],
        name="advance",
    )(*[pltpu.with_memory_space_constraint(x, pltpu.VMEM) for x in mid])


def solution(mesh):
    flat = P(("members", "zonal"), "merid")
    deep = P(None, ("members", "zonal"), "merid")
    fixed = P(None, "zonal", "merid")
    return jax.shard_map(
        functools.partial(body, mesh.shape["zonal"]),
        mesh=mesh,
        in_specs=(flat, flat, flat, deep, deep, deep, fixed, P("members", None), P("members"), fixed),
        out_specs=(flat, flat, flat, deep, deep, deep),
        check_vma=False,
    )
```

```python
import functools
import math

import jax
import jax.numpy as jnp
from jax import lax
from jax.experimental import pallas as pl
from jax.experimental.pallas import tpu as pltpu
from jax.sharding import PartitionSpec as P

NSUB = 6
STEPS = 2
WAVE_LIMIT = 0.225
STRESS_SCALE = 0.1
FLUX_STEP = 0.05
PRESS_COEF = 0.05

MESH = pl.DeviceIdType.MESH
F32 = jnp.float32
OWN, EAST, WEST = 0, 1, 2
LANES = 128
STRIP = 16


def lane_iota(shape):
    return lax.broadcasted_iota(jnp.int32, shape, len(shape) - 1)


def modulo(value, size):
    return value & (size - 1) if size & (size - 1) == 0 else lax.rem(value, size)


def rolled(x, shift, axis):
    shift = shift % x.shape[axis]
    return pltpu.roll(x, shift, axis) if shift else x


def neighbours(rows):
    fold1 = jnp.logical_and(lane_iota((8, LANES)) < LANES // 2, lax.axis_index("merid") == 1)

    def merge(main, alt):
        fold = jnp.concatenate([fold1] * (alt.shape[0] // 8), 0)
        halo = jnp.where(fold, alt, main[:, rows:])
        return jnp.concatenate([main[:, :rows], halo], 1)

    def at_west(x):
        return merge(rolled(x, 1, 0), rolled(x[:, rows:], -1, 0))

    def at_east(x):
        return merge(rolled(x, -1, 0), rolled(x[:, rows:], 1, 0))

    def at_south(x):
        return merge(rolled(x, 1, 1), rolled(x[:, rows:], -1, 1))

    def at_north(x):
        return merge(rolled(x, -1, 1), rolled(x[:, rows - LANES:], 1, 1)[:, LANES:])

    return at_east, at_west, at_south, at_north


def exchange(
    devices,
    eta_ref, bu_ref, bv_ref, h_ref, u_ref, v_ref, faces_ref, base_ref, seeds_ref, scale_ref,
    lay, means, faces_out, state_out,
    base, faces, winds, seeds, scale, goeast, gowest, least, lwest, outw, oute, inw, ine,
    top, bottom, top_side, bottom_side, north_ref, south_ref, north_side, south_side,
    load, send, recv, near_ok, west_ok, far_ok,
):
    z = lax.axis_index("zonal")
    c = lax.axis_index("merid")
    e = lax.rem(z + 1, devices)
    w = lax.rem(z + devices - 1, devices)
    other = 1 - c
    far = [lax.rem(2 * devices - 1 - z + d, devices) for d in (0, -1, 1)]
    layers, cells, rows = h_ref.shape
    wide = rows + LANES
    ext = cells + 8
    H, U, V = 0, 1, 2

    fetches = [
        pltpu.make_async_copy(src, dst, load.at[k])
        for k, (src, dst) in enumerate((
            (eta_ref, base.at[4, pl.ds(0, cells), pl.ds(0, rows)]),
            (bu_ref, base.at[5, pl.ds(0, cells), pl.ds(0, rows)]),
            (bv_ref, base.at[6, pl.ds(0, cells), pl.ds(0, rows)]),
            (seeds_ref, seeds),
            (scale_ref, scale),
            (faces_ref, faces),
            (base_ref, winds),
            (h_ref, lay.at[H, :, pl.ds(0, cells), pl.ds(0, rows)]),
            (u_ref, lay.at[U, :, pl.ds(0, cells), pl.ds(0, rows)]),
            (v_ref, lay.at[V, :, pl.ds(0, cells), pl.ds(0, rows)]),
        ))
    ]
    for cp in fetches:
        cp.start()
    barrier = pltpu.get_barrier_semaphore()

    def greet(zonal, merid):
        pl.semaphore_signal(
            barrier, inc=1, device_id={"zonal": zonal, "merid": merid}, device_id_type=MESH
        )

    greet(w, 1)

    @pl.when(c == 0)
    def _():
        greet(z, 1)

    @pl.when(c == 1)
    def _():
        for target in far:
            greet(target, 0)

    def copy(src, dst, k, zonal, merid):
        return pltpu.make_async_remote_copy(
            src_ref=src, dst_ref=dst, send_sem=send.at[k], recv_sem=recv.at[k],
            device_id={"zonal": zonal, "merid": merid}, device_id_type=MESH,
        )

    lanes = pl.ds(0, rows)

    def to_sides(fields, k):
        return [
            copy(base.at[fields, pl.ds(8, 8), lanes], base.at[fields, pl.ds(32, 8), lanes], k, e, c),
            copy(base.at[fields, pl.ds(0, 8), lanes], base.at[fields, pl.ds(16, 8), lanes], k + 1, w, c),
        ]

    state_copies = to_sides(pl.ds(4, 3), 15)
    side_copies = to_sides(pl.ds(0, 4), 0) + [
        copy(oute, inw, 2, e, c),
        copy(outw, ine, 3, w, c),
    ]
    column_copies = [
        copy(goeast, lwest, 13, e, c),
        copy(gowest, least, 14, w, c),
    ]

    for cp in fetches[:3]:
        cp.wait()

    def tell(semaphore, zonal, merid):
        pl.semaphore_signal(
            semaphore, inc=1, device_id={"zonal": zonal, "merid": merid}, device_id_type=MESH
        )

    @pl.when(c == 1)
    def _():
        pl.semaphore_wait(barrier, 3)
        tell(near_ok, z, other)
        tell(west_ok, e, 1)
        tell(west_ok, e, 0)

    @pl.when(c == 0)
    def _():
        pl.semaphore_wait(near_ok, 1)

    state_copies[0].start()
    for cp in fetches[3:7]:
        cp.wait()
    total_x = cells * devices
    total_y = rows * 2
    cols = lax.broadcasted_iota(jnp.int32, (cells, LANES), 0) + z * cells
    rws = lax.broadcasted_iota(jnp.int32, (8, rows), 1) + c * rows
    sum_cos = jnp.zeros((cells, rows), F32)
    sum_sin = jnp.zeros((cells, rows), F32)
    for m in range(seeds.shape[1]):
        ax = (2.0 * math.pi / total_x) * modulo(seeds[0, m] * cols, total_x).astype(F32)
        ay = (2.0 * math.pi / total_y) * modulo(seeds[1, m] * rws, total_y).astype(F32)
        amp = scale[m]
        cx = jnp.concatenate([amp * jnp.cos(ax)] * (rows // LANES), 1)
        sx = jnp.concatenate([amp * jnp.sin(ax)] * (rows // LANES), 1)
        cy = jnp.concatenate([jnp.cos(ay)] * (cells // 8), 0)
        sy = jnp.concatenate([jnp.sin(ay)] * (cells // 8), 0)
        sum_cos = sum_cos + (cx * cy - sx * sy)
        sum_sin = sum_sin + (sx * cy + cx * sy)
    mask_u = faces[0].astype(F32)
    mask_v = faces[1].astype(F32)
    base[2, :cells, :rows] = mask_u * (STRESS_SCALE * (winds[0] + sum_cos))
    base[3, :cells, :rows] = mask_v * (STRESS_SCALE * (winds[1] + sum_sin))
    fetches[7].wait()
    h_sum = lay[H, 0, :cells, :rows]
    for l in range(1, layers):
        h_sum = h_sum + lay[H, l, :cells, :rows]
    wave = (WAVE_LIMIT / layers) * h_sum
    base[0, :cells, :rows] = mask_u * wave
    base[1, :cells, :rows] = mask_v * wave
    for cp in fetches[8:]:
        cp.wait()
    low4 = lax.broadcasted_iota(jnp.int32, (8, rows), 0) < 4
    for k in range(4):
        a = base[2 * k, 0:8, :rows]
        b = base[2 * k, 8:16, :rows]
        if 2 * k + 1 < 7:
            a = jnp.where(low4, pltpu.roll(base[2 * k + 1, 0:8, :rows], 4, 0), a)
            b = jnp.where(low4, b, pltpu.roll(base[2 * k + 1, 8:16, :rows], 4, 0))
        oute[k] = a
        outw[k] = b
    last = cells - 1
    h_last = lay[H, :, last, :rows]
    u_last = lay[U, :, last, :rows]
    flux_in = lay[U, :, last - 1, :rows] * (0.5 * (lay[H, :, last - 1, :rows] + h_last))
    for k, x in enumerate((h_last, u_last, flux_in, lay[V, :, last, :rows])):
        goeast[k * layers: (k + 1) * layers] = x
    h_first = lay[H, :, 0, :rows]
    flux_out = lay[U, :, 0, :rows] * (0.5 * (h_first + lay[H, :, 1, :rows]))
    for k, x in enumerate((h_first, flux_out, lay[V, :, 0, :rows])):
        gowest[k * layers: (k + 1) * layers] = x

    side_copies[0].start()
    side_copies[2].start()
    lane = lane_iota((cells, LANES))
    hi = rows - LANES
    base_t = jnp.zeros((cells, LANES), F32)
    base_b = jnp.zeros((cells, LANES), F32)
    for f in range(7):
        here = lane // STRIP == f
        base_t = jnp.where(here, rolled(base[f, :cells, hi:rows], f * STRIP + STRIP, 1), base_t)
        base_b = jnp.where(here, rolled(base[f, :cells, :LANES], f * STRIP, 1), base_b)
    lay_t = jnp.zeros((cells, LANES), F32)
    lay_b = jnp.zeros((cells, LANES), F32)
    for start, width, kind in ((0, 2, H), (2 * layers, 2, V), (4 * layers, 1, U)):
        for l in range(layers):
            spot = start + width * l
            here = jnp.logical_and(lane >= spot, lane < spot + width)
            lay_t = jnp.where(here, rolled(lay[kind, l, :cells, hi:rows], spot + width, 1), lay_t)
            lay_b = jnp.where(here, rolled(lay[kind, l, :cells, :LANES], spot, 1), lay_b)
    r2 = lax.broadcasted_iota(jnp.int32, (LANES, LANES), 0)
    c2 = lax.broadcasted_iota(jnp.int32, (LANES, LANES), 1)
    perm_b = jnp.where(r2 == (c2 ^ (STRIP - 1)), 1.0, 0.0).astype(F32)
    perm_l = jnp.where(r2 == jnp.where(c2 < 4 * layers, c2 ^ 1, c2), 1.0, 0.0).astype(F32)
    r1 = lax.broadcasted_iota(jnp.int32, (cells, cells), 0)
    c1 = lax.broadcasted_iota(jnp.int32, (cells, cells), 1)
    mirror = jnp.where(r1 + c1 == cells - 1, 1.0, 0.0).astype(F32)
    dot = functools.partial(
        jnp.dot, preferred_element_type=F32, precision=lax.Precision.HIGHEST
    )
    north_edge = c == 1
    base_t = jnp.where(north_edge, dot(mirror, dot(base_t, perm_b)), base_t)
    lay_t = jnp.where(north_edge, dot(mirror, dot(lay_t, perm_l)), lay_t)
    sub = lax.broadcasted_iota(jnp.int32, (8, LANES), 0)
    for whole, side, fields, columns in ((top, top_side, base_t, lay_t), (bottom, bottom_side, base_b, lay_b)):
        whole[:, :LANES] = fields
        whole[:, LANES:] = columns
        side[0, 0:8] = jnp.where(sub < 2, pltpu.roll(columns[8:], 2, 0), fields[:8])
        side[0, 8:16] = fields[8:]
        side[1, 0:8] = fields[:8]
        side[1, 8:16] = jnp.where(sub >= 6, pltpu.roll(columns[:8], 6, 0), fields[8:])

    def strips(whole, side, into, into_side, k, own, to_west_slot, to_east_slot, merid):
        return [
            copy(whole, into, k, own, merid),
            copy(side.at[0], into_side.at[0], k + 1, to_west_slot, merid),
            copy(side.at[1], into_side.at[1], k + 2, to_east_slot, merid),
        ]

    far_targets = (far[0], far[2], far[1])
    far_copies = strips(top, top_side, north_ref, north_side, 4, *far_targets, c)
    up_copies = strips(top, top_side, south_ref, south_side, 7, z, e, w, other)
    down_copies = strips(bottom, bottom_side, north_ref, north_side, 10, z, e, w, other)

    @pl.when(c == 0)
    def _():
        up_copies[0].start()
        up_copies[1].start()

    @pl.when(c == 1)
    def _():
        down_copies[0].start()
        down_copies[1].start()

    def send_far():
        @pl.when(c == 0)
        def _():
            pl.semaphore_wait(barrier, 3)
            pl.semaphore_signal(
                far_ok, inc=1, device_id={"zonal": z, "merid": other}, device_id_type=MESH
            )

        @pl.when(c == 1)
        def _():
            pl.semaphore_wait(far_ok, 1)
            for target, cp in zip(far_targets, far_copies):
                @pl.when(target != z)
                def _(cp=cp):
                    cp.start()

    late = 2 * z >= devices

    @pl.when(late)
    def _():
        send_far()

    column_copies[0].start()

    pl.semaphore_wait(west_ok, 1)
    state_copies[1].start()
    side_copies[1].start()
    side_copies[3].start()

    @pl.when(c == 0)
    def _():
        up_copies[2].start()

    @pl.when(c == 1)
    def _():
        down_copies[2].start()

    column_copies[1].start()

    @pl.when(jnp.logical_not(late))
    def _():
        send_far()

    @pl.when(c == 0)
    def _():
        south_ref[...] = jnp.zeros_like(south_ref)
        south_side[...] = jnp.zeros_like(south_side)

    for target, dst, src in (
        (far_targets[0], north_ref, top),
        (far_targets[1], north_side.at[0], top_side.at[0]),
        (far_targets[2], north_side.at[1], top_side.at[1]),
    ):
        @pl.when(jnp.logical_and(c == 1, target == z))
        def _(dst=dst, src=src):
            dst[...] = src[...]

    for kind in (H, U, V):
        for l in range(layers):
            lay[kind, l, cells:, :rows] = jnp.zeros((8, rows), F32)

    for cp in state_copies + side_copies:
        cp.wait()

    @pl.when(c == 0)
    def _():
        for cp in up_copies:
            cp.wait_send()
        for cp in down_copies:
            cp.wait_recv()

    @pl.when(c == 1)
    def _():
        for cp in down_copies:
            cp.wait_send()
        for cp in up_copies:
            cp.wait_recv()

    for target, cp in zip(far_targets, far_copies):
        @pl.when(jnp.logical_and(c == 1, target != z))
        def _(cp=cp):
            cp.wait()

    for k in range(4):
        from_w = inw[k]
        from_e = ine[k]
        base[2 * k, 24:32, :rows] = jnp.where(low4, from_e, from_w)
        if 2 * k + 1 < 7:
            base[2 * k + 1, 24:32, :rows] = pltpu.roll(jnp.where(low4, from_w, from_e), 4, 0)
    first8 = lane_iota((8, LANES)) < LANES // 2
    far_rows = lax.broadcasted_iota(jnp.int32, (8, LANES), 0) < 4
    norths = [north_ref[:, :LANES], north_side[1], north_side[0]]
    souths = [south_ref[:, :LANES], south_side[1], south_side[0]]

    def ring(x):
        outer = jnp.where(far_rows, x[EAST][8:], x[WEST][:8])
        return (x[OWN][:8], x[OWN][8:], x[EAST][:8], outer, x[WEST][8:])

    for k, (n, s) in enumerate(zip(ring(norths), ring(souths))):
        for f in range(7):
            base[f, 8 * k: 8 * k + 8, rows:] = jnp.where(
                first8, rolled(n, -STRIP * f, 1), rolled(s, LANES - STRIP - STRIP * f, 1)
            )
    at_east, at_west, at_south, at_north = neighbours(rows)
    near = lax.broadcasted_iota(jnp.int32, (8, wide), 0) < 4

    def trimmed(x):
        size = x.shape[0]
        return jnp.concatenate([x[:cells], jnp.where(near, x[cells: cells + 8], x[size - 8:])], 0)

    faces_out[0] = trimmed(base[0])
    faces_out[1] = trimmed(base[1])

    def substep(narrow):
        def get(f):
            if narrow:
                return jnp.concatenate([base[f, :cells + 8], base[f, cells + 16:]], 0)
            return base[f]

        def put(f, x):
            if narrow:
                base[f, :cells + 8] = x[:cells + 8]
                base[f, cells + 16:] = x[cells + 8:]
            else:
                base[f] = x

        def run(_, sums):
            sum_u, sum_v = sums
            bu = get(5)
            bv = get(6)
            eta = get(4) - (bu - at_west(bu) + bv - at_south(bv))
            put(4, eta)
            au = get(0)
            bu = jnp.where(au != 0.0, bu - au * (at_east(eta) - eta) + get(2), 0.0)
            put(5, bu)
            av = get(1)
            bv = jnp.where(av != 0.0, bv - av * (at_north(eta) - eta) + get(3), 0.0)
            put(6, bv)
            return sum_u + trimmed(bu), sum_v + trimmed(bv)

        return run

    outer_steps = 2 * NSUB - 8
    zero = jnp.zeros((ext, wide), F32)
    for step in range(STEPS):
        sums = (zero, zero)
        if step == 0:
            sums = lax.fori_loop(0, outer_steps, substep(False), sums)
            sums = lax.fori_loop(outer_steps, NSUB, substep(True), sums)
        else:
            sums = lax.fori_loop(0, NSUB, substep(True), sums)
        means[step, 0] = sums[0] * (1.0 / NSUB)
        means[step, 1] = sums[1] * (1.0 / NSUB)
    for k in range(3):
        state_out[k] = base[4 + k, :cells, :rows]

    def around(own, sides):
        halo = jnp.where(far_rows, pltpu.roll(sides[1, 8:], 2, 0), pltpu.roll(sides[0, :8], 6, 0))
        return jnp.concatenate([own[:, LANES:], halo], 0)

    north = around(north_ref, north_side)
    south = around(south_ref, south_side)
    first24 = lane_iota(north.shape) < LANES // 2
    for kind, start, width in ((H, 0, 2), (U, 4 * layers, 1), (V, 2 * layers, 2)):
        for l in range(layers):
            spot = start + width * l
            lay[kind, l, :, rows:] = jnp.where(
                first24, rolled(north, -spot, 1), rolled(south, LANES - width - spot, 1)
            )
    for cp in column_copies:
        cp.wait()
    for l in range(layers):
        def column(ref, k):
            return ref[k * layers + l: k * layers + l + 1, :]

        lay[H, l, cells: cells + 1, :rows] = column(least, 0)
        lay[H, l, cells + 1: cells + 2, :rows] = 2.0 - column(least, 0)
        lay[U, l, cells: cells + 1, :rows] = column(least, 1)
        lay[V, l, cells: cells + 1, :rows] = column(least, 2)
        lay[H, l, ext - 1: ext, :rows] = column(lwest, 0)
        lay[H, l, ext - 2: ext - 1, :rows] = 2.0 - column(lwest, 0)
        lay[U, l, ext - 1: ext, :rows] = column(lwest, 1)
        lay[U, l, ext - 2: ext - 1, :rows] = column(lwest, 2)
        lay[V, l, ext - 1: ext, :rows] = column(lwest, 3)


def advance(
    lay_in, means, faces, state, eta_out, bu_out, bv_out, h_out, u_out, v_out,
    lay, trial, depth, results, done,
):
    layers, cells, rows = h_out.shape
    wide = rows + LANES
    ext = cells + 8
    H, U, V = 0, 1, 2
    at_east, at_west, at_south, at_north = neighbours(rows)
    stores = [
        pltpu.make_async_copy(state.at[k], out, done.at[k])
        for k, out in enumerate((eta_out, bu_out, bv_out))
    ] + [
        pltpu.make_async_copy(results.at[k], out, done.at[3 + k])
        for k, out in enumerate((h_out, u_out, v_out))
    ]
    for cp in stores[:3]:
        cp.start()
    for outer in range(STEPS):
        final = outer == STEPS - 1
        source = lay_in if outer == 0 else lay
        size_c, size_r = (cells, rows) if final else (ext, wide)
        press_u = press_v = total_u = total_v = jnp.zeros((size_c, size_r), F32)
        deep_u = deep_v = press_u
        for l in range(layers):
            h = source[H, l]
            u = source[U, l]
            v = source[V, l]
            if final:
                diff_u = rolled(h[:, :rows], -1, 0) - h[:, :rows]
                diff_v = rolled(h[:cells], -1, 1) - h[:cells]
                hu = h[:, :rows] + 0.5 * diff_u
                hv = h[:cells] + 0.5 * diff_v
                flux_u = u[:, :rows] * hu
                flux_v = v[:cells] * hv
                out_u = (flux_u - rolled(flux_u, 1, 0))[:cells]
                out_v = (flux_v - rolled(flux_v, 1, 1))[:, :rows]
                results[0, l] = h[:cells, :rows] - FLUX_STEP * (out_u + out_v)
                diff_u, hu = diff_u[:cells], hu[:cells]
                diff_v, hv = diff_v[:, :rows], hv[:, :rows]
                u, v = u[:cells, :rows], v[:cells, :rows]
            else:
                diff_u = at_east(h) - h
                diff_v = at_north(h) - h
                hu = h + 0.5 * diff_u
                hv = h + 0.5 * diff_v
                flux_u = u * hu
                flux_v = v * hv
                lay[H, l] = h - FLUX_STEP * (flux_u - at_west(flux_u) + flux_v - at_south(flux_v))
            press_u = press_u + diff_u
            press_v = press_v + diff_v
            ut = u - PRESS_COEF * press_u
            vt = v - PRESS_COEF * press_v
            trial[0, l, :size_c, :size_r] = ut
            trial[1, l, :size_c, :size_r] = vt
            total_u = total_u + hu * ut
            total_v = total_v + hv * vt
            if outer == 0:
                deep_u = deep_u + hu
                deep_v = deep_v + hv
        if outer == 0:
            depth[0] = deep_u
            depth[1] = deep_v
        if final:
            stores[3].start()
        for k, total in ((U, total_u), (V, total_v)):
            fix = (means[outer, k - 1, :size_c, :size_r] - total) / depth[k - 1, :size_c, :size_r]
            open_face = faces[k - 1, :size_c, :size_r] != 0.0
            for l in range(layers):
                new = jnp.where(open_face, trial[k - 1, l, :size_c, :size_r] + fix, 0.0)
                if final:
                    results[k, l] = new
                else:
                    lay[k, l] = new
            if final:
                stores[3 + k].start()
    for cp in stores:
        cp.wait()


def body(
    devices, height, transport_u, transport_v, thickness, velocity_u, velocity_v,
    sea_faces, wind_seeds, wind_scale, wind_base,
):
    layers, cells, rows = thickness.shape
    wide = rows + LANES
    ext = cells + 8
    anywhere = pl.BlockSpec(memory_space=pl.ANY)
    vmem = pl.BlockSpec(memory_space=pltpu.VMEM)

    def shape(*dims):
        return jax.ShapeDtypeStruct(dims, F32)

    def inner(*dims):
        return pltpu.VMEM(dims, F32)

    mid = pl.pallas_call(
        functools.partial(exchange, devices),
        out_shape=[
            inner(3, layers, ext, wide), inner(STEPS, 2, ext, wide), inner(2, ext, wide),
            inner(3, cells, rows),
        ],
        in_specs=[anywhere] * 10,
        out_specs=[vmem] * 4,
        scratch_shapes=[
            inner(7, cells + 24, wide),
            pltpu.VMEM(sea_faces.shape, sea_faces.dtype),
            inner(*wind_base.shape),
            pltpu.SMEM(wind_seeds.shape[::-1], wind_seeds.dtype),
            pltpu.SMEM(wind_scale.shape, F32),
            inner(4 * layers, rows), inner(3 * layers, rows), inner(3 * layers, rows), inner(4 * layers, rows),
            inner(4, 8, rows), inner(4, 8, rows), inner(4, 8, rows), inner(4, 8, rows),
            inner(cells, 2 * LANES), inner(cells, 2 * LANES), inner(2, cells, LANES), inner(2, cells, LANES),
            inner(cells, 2 * LANES), inner(cells, 2 * LANES), inner(2, cells, LANES), inner(2, cells, LANES),
            pltpu.SemaphoreType.DMA((10,)),
            pltpu.SemaphoreType.DMA((17,)),
            pltpu.SemaphoreType.DMA((17,)),
            pltpu.SemaphoreType.REGULAR,
            pltpu.SemaphoreType.REGULAR,
            pltpu.SemaphoreType.REGULAR,
        ],
        compiler_params=pltpu.CompilerParams(collective_id=0, has_side_effects=True),
        name="exchange",
    )(
        height, transport_u, transport_v, thickness, velocity_u, velocity_v,
        sea_faces, wind_base, wind_seeds.T, wind_scale,
    )
    return pl.pallas_call(
        advance,
        out_shape=[shape(cells, rows)] * 3 + [shape(layers, cells, rows)] * 3,
        in_specs=[vmem] * 4,
        out_specs=[anywhere] * 6,
        scratch_shapes=[
            inner(3, layers, ext, wide),
            inner(2, layers, ext, wide),
            inner(2, ext, wide),
            inner(3, layers, cells, rows),
            pltpu.SemaphoreType.DMA((6,)),
        ],
        name="advance",
    )(*[pltpu.with_memory_space_constraint(x, pltpu.VMEM) for x in mid])


def solution(mesh):
    flat = P(("members", "zonal"), "merid")
    deep = P(None, ("members", "zonal"), "merid")
    fixed = P(None, "zonal", "merid")
    return jax.shard_map(
        functools.partial(body, mesh.shape["zonal"]),
        mesh=mesh,
        in_specs=(flat, flat, flat, deep, deep, deep, fixed, P("members", None), P("members"), fixed),
        out_specs=(flat, flat, flat, deep, deep, deep),
        check_vma=False,
    )
```

```python
import functools
import math

import jax
import jax.numpy as jnp
from jax import lax
from jax.experimental import pallas as pl
from jax.experimental.pallas import tpu as pltpu
from jax.sharding import PartitionSpec as P

NSUB = 6
STEPS = 2
WAVE_LIMIT = 0.225
STRESS_SCALE = 0.1
FLUX_STEP = 0.05
PRESS_COEF = 0.05

MESH = pl.DeviceIdType.MESH
F32 = jnp.float32
OWN, EAST, WEST = 0, 1, 2
LANES = 128
STRIP = 16


def lane_iota(shape):
    return lax.broadcasted_iota(jnp.int32, shape, len(shape) - 1)


def modulo(value, size):
    return value & (size - 1) if size & (size - 1) == 0 else lax.rem(value, size)


def rolled(x, shift, axis):
    shift = shift % x.shape[axis]
    return pltpu.roll(x, shift, axis) if shift else x


def neighbours(rows):
    fold1 = jnp.logical_and(lane_iota((8, LANES)) < LANES // 2, lax.axis_index("merid") == 1)

    def merge(main, alt):
        fold = jnp.concatenate([fold1] * (alt.shape[0] // 8), 0)
        halo = jnp.where(fold, alt, main[:, rows:])
        return jnp.concatenate([main[:, :rows], halo], 1)

    def at_west(x):
        return merge(rolled(x, 1, 0), rolled(x[:, rows:], -1, 0))

    def at_east(x):
        return merge(rolled(x, -1, 0), rolled(x[:, rows:], 1, 0))

    def at_south(x):
        return merge(rolled(x, 1, 1), rolled(x[:, rows:], -1, 1))

    def at_north(x):
        return merge(rolled(x, -1, 1), rolled(x[:, rows - LANES:], 1, 1)[:, LANES:])

    return at_east, at_west, at_south, at_north


def exchange(
    devices,
    eta_ref, bu_ref, bv_ref, h_ref, u_ref, v_ref, faces_ref, base_ref, seeds_ref, scale_ref,
    h_new, trial, fixes, faces_out, state_out,
    base, lay, halo_trial, depth, faces, winds, seeds, scale, goeast, gowest, least, lwest, late_east, late_west,
    top, bottom, top_side, bottom_side, north_ref, south_ref, north_side, south_side,
    load, send, recv, near_ok, west_ok, far_ok,
):
    z = lax.axis_index("zonal")
    c = lax.axis_index("merid")
    e = lax.rem(z + 1, devices)
    w = lax.rem(z + devices - 1, devices)
    other = 1 - c
    far = [lax.rem(2 * devices - 1 - z + d, devices) for d in (0, -1, 1)]
    layers, cells, rows = h_ref.shape
    wide = rows + LANES
    ext = cells + 8
    H, U, V = 0, 1, 2

    fetches = [
        pltpu.make_async_copy(src, dst, load.at[k])
        for k, (src, dst) in enumerate((
            (eta_ref, base.at[4, pl.ds(0, cells), pl.ds(0, rows)]),
            (bu_ref, base.at[5, pl.ds(0, cells), pl.ds(0, rows)]),
            (bv_ref, base.at[6, pl.ds(0, cells), pl.ds(0, rows)]),
            (seeds_ref, seeds),
            (scale_ref, scale),
            (faces_ref, faces),
            (base_ref, winds),
            (h_ref, lay.at[H, :, pl.ds(0, cells), pl.ds(0, rows)]),
            (u_ref, lay.at[U, :, pl.ds(0, cells), pl.ds(0, rows)]),
            (v_ref, lay.at[V, :, pl.ds(0, cells), pl.ds(0, rows)]),
        ))
    ]
    for cp in fetches:
        cp.start()
    barrier = pltpu.get_barrier_semaphore()

    def greet(zonal, merid):
        pl.semaphore_signal(
            barrier, inc=1, device_id={"zonal": zonal, "merid": merid}, device_id_type=MESH
        )

    greet(w, 1)

    @pl.when(c == 0)
    def _():
        greet(z, 1)

    @pl.when(c == 1)
    def _():
        for target in far:
            greet(target, 0)

    def copy(src, dst, k, zonal, merid):
        return pltpu.make_async_remote_copy(
            src_ref=src, dst_ref=dst, send_sem=send.at[k], recv_sem=recv.at[k],
            device_id={"zonal": zonal, "merid": merid}, device_id_type=MESH,
        )

    lanes = pl.ds(0, rows)

    def to_sides(fields, k):
        return [
            copy(base.at[fields, pl.ds(8, 8), lanes], base.at[fields, pl.ds(24, 8), lanes], k, e, c),
            copy(base.at[fields, pl.ds(0, 8), lanes], base.at[fields, pl.ds(16, 8), lanes], k + 1, w, c),
        ]

    state_copies = to_sides(pl.ds(4, 3), 15)
    side_copies = to_sides(pl.ds(0, 4), 0)
    second_copies = [
        copy(base.at[pl.ds(4, 3), pl.ds(8, 8)], late_west, 2, e, c),
        copy(base.at[pl.ds(4, 3), pl.ds(0, 8)], late_east, 3, w, c),
    ]
    column_copies = [
        copy(goeast, lwest, 13, e, c),
        copy(gowest, least, 14, w, c),
    ]

    for cp in fetches[:3]:
        cp.wait()

    def tell(semaphore, zonal, merid):
        pl.semaphore_signal(
            semaphore, inc=1, device_id={"zonal": zonal, "merid": merid}, device_id_type=MESH
        )

    @pl.when(c == 1)
    def _():
        pl.semaphore_wait(barrier, 3)
        tell(near_ok, z, other)
        tell(west_ok, e, 1)
        tell(west_ok, e, 0)

    @pl.when(c == 0)
    def _():
        pl.semaphore_wait(near_ok, 1)

    state_copies[0].start()
    for cp in fetches[3:7]:
        cp.wait()
    total_x = cells * devices
    total_y = rows * 2
    cols = lax.broadcasted_iota(jnp.int32, (cells, LANES), 0) + z * cells
    rws = lax.broadcasted_iota(jnp.int32, (8, rows), 1) + c * rows
    sum_cos = jnp.zeros((cells, rows), F32)
    sum_sin = jnp.zeros((cells, rows), F32)
    for m in range(seeds.shape[1]):
        ax = (2.0 * math.pi / total_x) * modulo(seeds[0, m] * cols, total_x).astype(F32)
        ay = (2.0 * math.pi / total_y) * modulo(seeds[1, m] * rws, total_y).astype(F32)
        amp = scale[m]
        cx = jnp.concatenate([amp * jnp.cos(ax)] * (rows // LANES), 1)
        sx = jnp.concatenate([amp * jnp.sin(ax)] * (rows // LANES), 1)
        cy = jnp.concatenate([jnp.cos(ay)] * (cells // 8), 0)
        sy = jnp.concatenate([jnp.sin(ay)] * (cells // 8), 0)
        sum_cos = sum_cos + (cx * cy - sx * sy)
        sum_sin = sum_sin + (sx * cy + cx * sy)
    mask_u = faces[0].astype(F32)
    mask_v = faces[1].astype(F32)
    base[2, :cells, :rows] = mask_u * (STRESS_SCALE * (winds[0] + sum_cos))
    base[3, :cells, :rows] = mask_v * (STRESS_SCALE * (winds[1] + sum_sin))
    fetches[7].wait()
    h_sum = lay[H, 0, :cells, :rows]
    for l in range(1, layers):
        h_sum = h_sum + lay[H, l, :cells, :rows]
    wave = (WAVE_LIMIT / layers) * h_sum
    base[0, :cells, :rows] = mask_u * wave
    base[1, :cells, :rows] = mask_v * wave
    for cp in fetches[8:]:
        cp.wait()
    last = cells - 1
    h_last = lay[H, :, last, :rows]
    u_last = lay[U, :, last, :rows]
    flux_in = lay[U, :, last - 1, :rows] * (0.5 * (lay[H, :, last - 1, :rows] + h_last))
    for k, x in enumerate((h_last, u_last, flux_in, lay[V, :, last, :rows])):
        goeast[k * layers: (k + 1) * layers] = x
    h_first = lay[H, :, 0, :rows]
    flux_out = lay[U, :, 0, :rows] * (0.5 * (h_first + lay[H, :, 1, :rows]))
    for k, x in enumerate((h_first, flux_out, lay[V, :, 0, :rows])):
        gowest[k * layers: (k + 1) * layers] = x

    side_copies[0].start()
    lane = lane_iota((cells, LANES))
    hi = rows - LANES
    base_t = jnp.zeros((cells, LANES), F32)
    base_b = jnp.zeros((cells, LANES), F32)
    for f in range(7):
        here = lane // STRIP == f
        base_t = jnp.where(here, rolled(base[f, :cells, hi:rows], f * STRIP + STRIP, 1), base_t)
        base_b = jnp.where(here, rolled(base[f, :cells, :LANES], f * STRIP, 1), base_b)
    lay_t = jnp.zeros((cells, LANES), F32)
    lay_b = jnp.zeros((cells, LANES), F32)
    for start, width, kind in ((0, 2, H), (2 * layers, 2, V), (4 * layers, 1, U)):
        for l in range(layers):
            spot = start + width * l
            here = jnp.logical_and(lane >= spot, lane < spot + width)
            lay_t = jnp.where(here, rolled(lay[kind, l, :cells, hi:rows], spot + width, 1), lay_t)
            lay_b = jnp.where(here, rolled(lay[kind, l, :cells, :LANES], spot, 1), lay_b)
    r2 = lax.broadcasted_iota(jnp.int32, (LANES, LANES), 0)
    c2 = lax.broadcasted_iota(jnp.int32, (LANES, LANES), 1)
    perm_b = jnp.where(r2 == (c2 ^ (STRIP - 1)), 1.0, 0.0).astype(F32)
    perm_l = jnp.where(r2 == jnp.where(c2 < 4 * layers, c2 ^ 1, c2), 1.0, 0.0).astype(F32)
    r1 = lax.broadcasted_iota(jnp.int32, (cells, cells), 0)
    c1 = lax.broadcasted_iota(jnp.int32, (cells, cells), 1)
    mirror = jnp.where(r1 + c1 == cells - 1, 1.0, 0.0).astype(F32)
    dot = functools.partial(
        jnp.dot, preferred_element_type=F32, precision=lax.Precision.HIGHEST
    )
    north_edge = c == 1
    base_t = jnp.where(north_edge, dot(mirror, dot(base_t, perm_b)), base_t)
    lay_t = jnp.where(north_edge, dot(mirror, dot(lay_t, perm_l)), lay_t)
    sub = lax.broadcasted_iota(jnp.int32, (8, LANES), 0)
    for whole, side, fields, columns in ((top, top_side, base_t, lay_t), (bottom, bottom_side, base_b, lay_b)):
        whole[:, :LANES] = fields
        whole[:, LANES:] = columns
        side[0, 0:8] = jnp.where(sub < 2, pltpu.roll(columns[8:], 2, 0), fields[:8])
        side[0, 8:16] = fields[8:]
        side[1, 0:8] = fields[:8]
        side[1, 8:16] = jnp.where(sub >= 6, pltpu.roll(columns[:8], 6, 0), fields[8:])

    def strips(whole, side, into, into_side, k, own, to_west_slot, to_east_slot, merid):
        return [
            copy(whole, into, k, own, merid),
            copy(side.at[0], into_side.at[0], k + 1, to_west_slot, merid),
            copy(side.at[1], into_side.at[1], k + 2, to_east_slot, merid),
        ]

    far_targets = (far[0], far[2], far[1])
    far_copies = strips(top, top_side, north_ref, north_side, 4, *far_targets, c)
    up_copies = strips(top, top_side, south_ref, south_side, 7, z, e, w, other)
    down_copies = strips(bottom, bottom_side, north_ref, north_side, 10, z, e, w, other)

    @pl.when(c == 0)
    def _():
        up_copies[0].start()
        up_copies[1].start()

    @pl.when(c == 1)
    def _():
        down_copies[0].start()
        down_copies[1].start()

    def send_far():
        @pl.when(c == 0)
        def _():
            pl.semaphore_wait(barrier, 3)
            pl.semaphore_signal(
                far_ok, inc=1, device_id={"zonal": z, "merid": other}, device_id_type=MESH
            )

        @pl.when(c == 1)
        def _():
            pl.semaphore_wait(far_ok, 1)
            for target, cp in zip(far_targets, far_copies):
                @pl.when(target != z)
                def _(cp=cp):
                    cp.start()

    late = 2 * z >= devices

    @pl.when(late)
    def _():
        send_far()

    column_copies[0].start()

    pl.semaphore_wait(west_ok, 1)
    state_copies[1].start()
    side_copies[1].start()

    @pl.when(c == 0)
    def _():
        up_copies[2].start()

    @pl.when(c == 1)
    def _():
        down_copies[2].start()

    column_copies[1].start()

    @pl.when(jnp.logical_not(late))
    def _():
        send_far()

    @pl.when(c == 0)
    def _():
        south_ref[...] = jnp.zeros_like(south_ref)
        south_side[...] = jnp.zeros_like(south_side)

    for target, dst, src in (
        (far_targets[0], north_ref, top),
        (far_targets[1], north_side.at[0], top_side.at[0]),
        (far_targets[2], north_side.at[1], top_side.at[1]),
    ):
        @pl.when(jnp.logical_and(c == 1, target == z))
        def _(dst=dst, src=src):
            dst[...] = src[...]

    for kind in (H, U, V):
        for l in range(layers):
            lay[kind, l, cells:, :rows] = jnp.zeros((8, rows), F32)

    for cp in state_copies + side_copies:
        cp.wait()

    @pl.when(c == 0)
    def _():
        for cp in up_copies:
            cp.wait_send()
        for cp in down_copies:
            cp.wait_recv()

    @pl.when(c == 1)
    def _():
        for cp in down_copies:
            cp.wait_send()
        for cp in up_copies:
            cp.wait_recv()

    for target, cp in zip(far_targets, far_copies):
        @pl.when(jnp.logical_and(c == 1, target != z))
        def _(cp=cp):
            cp.wait()

    first8 = lane_iota((8, LANES)) < LANES // 2
    far_rows = lax.broadcasted_iota(jnp.int32, (8, LANES), 0) < 4
    norths = [north_ref[:, :LANES], north_side[1], north_side[0]]
    souths = [south_ref[:, :LANES], south_side[1], south_side[0]]

    def ring(x):
        return (x[OWN][:8], x[OWN][8:], x[EAST][:8], x[WEST][8:])

    for k, (n, s) in enumerate(zip(ring(norths), ring(souths))):
        for f in range(7):
            base[f, 8 * k: 8 * k + 8, rows:] = jnp.where(
                first8, rolled(n, -STRIP * f, 1), rolled(s, LANES - STRIP - STRIP * f, 1)
            )
    at_east, at_west, at_south, at_north = neighbours(rows)
    near = lax.broadcasted_iota(jnp.int32, (8, wide), 0) < 4

    def trimmed(x):
        return jnp.concatenate([x[:cells], jnp.where(near, x[cells: cells + 8], x[cells + 8:])], 0)

    def move(_):
        bu = base[5]
        bv = base[6]
        eta = base[4] - (bu - at_west(bu) + bv - at_south(bv))
        base[4] = eta
        au = base[0]
        bu = jnp.where(au != 0.0, bu - au * (at_east(eta) - eta) + base[2], 0.0)
        base[5] = bu
        av = base[1]
        bv = jnp.where(av != 0.0, bv - av * (at_north(eta) - eta) + base[3], 0.0)
        base[6] = bv
        return bu, bv

    def substep(k, sums):
        bu, bv = move(k)
        return sums[0] + trimmed(bu), sums[1] + trimmed(bv)

    def substep_own(k):
        bu, bv = move(k)
        return bu[:cells, :rows], bv[:cells, :rows]

    zero = jnp.zeros((ext, wide), F32)
    mean_u, mean_v = lax.fori_loop(0, NSUB, substep, (zero, zero))
    for cp in second_copies:
        cp.start()
    depth[2] = mean_u * (1.0 / NSUB)
    depth[3] = mean_v * (1.0 / NSUB)

    def around(own, sides):
        halo = jnp.where(far_rows, pltpu.roll(sides[1, 8:], 2, 0), pltpu.roll(sides[0, :8], 6, 0))
        return jnp.concatenate([own[:, LANES:], halo], 0)

    north = around(north_ref, north_side)
    south = around(south_ref, south_side)
    first24 = lane_iota(north.shape) < LANES // 2
    for kind, start, width in ((H, 0, 2), (U, 4 * layers, 1), (V, 2 * layers, 2)):
        for l in range(layers):
            spot = start + width * l
            lay[kind, l, :, rows:] = jnp.where(
                first24, rolled(north, -spot, 1), rolled(south, LANES - width - spot, 1)
            )
    for cp in column_copies:
        cp.wait()
    for l in range(layers):
        def column(ref, k):
            return ref[k * layers + l: k * layers + l + 1, :]

        lay[H, l, cells: cells + 1, :rows] = column(least, 0)
        lay[H, l, cells + 1: cells + 2, :rows] = 2.0 - column(least, 0)
        lay[U, l, cells: cells + 1, :rows] = column(least, 1)
        lay[V, l, cells: cells + 1, :rows] = column(least, 2)
        lay[H, l, ext - 1: ext, :rows] = column(lwest, 0)
        lay[H, l, ext - 2: ext - 1, :rows] = 2.0 - column(lwest, 0)
        lay[U, l, ext - 1: ext, :rows] = column(lwest, 1)
        lay[U, l, ext - 2: ext - 1, :rows] = column(lwest, 2)
        lay[V, l, ext - 1: ext, :rows] = column(lwest, 3)
    for outer in range(STEPS):
        final = outer == STEPS - 1
        size_c, size_r = (cells, rows) if final else (ext, wide)
        press_u = press_v = total_u = total_v = jnp.zeros((size_c, size_r), F32)
        deep_u = deep_v = press_u
        for l in range(layers):
            h = lay[H, l]
            u = lay[U, l]
            v = lay[V, l]
            if final:
                diff_u = rolled(h[:, :rows], -1, 0) - h[:, :rows]
                diff_v = rolled(h[:cells], -1, 1) - h[:cells]
                hu = h[:, :rows] + 0.5 * diff_u
                hv = h[:cells] + 0.5 * diff_v
                flux_u = u[:, :rows] * hu
                flux_v = v[:cells] * hv
                out_u = (flux_u - rolled(flux_u, 1, 0))[:cells]
                out_v = (flux_v - rolled(flux_v, 1, 1))[:, :rows]
                h_new[l] = h[:cells, :rows] - FLUX_STEP * (out_u + out_v)
                diff_u, hu = diff_u[:cells], hu[:cells]
                diff_v, hv = diff_v[:, :rows], hv[:, :rows]
                u, v = u[:cells, :rows], v[:cells, :rows]
            else:
                diff_u = at_east(h) - h
                diff_v = at_north(h) - h
                hu = h + 0.5 * diff_u
                hv = h + 0.5 * diff_v
                flux_u = u * hu
                flux_v = v * hv
                lay[H, l] = h - FLUX_STEP * (flux_u - at_west(flux_u) + flux_v - at_south(flux_v))
            press_u = press_u + diff_u
            press_v = press_v + diff_v
            ut = u - PRESS_COEF * press_u
            vt = v - PRESS_COEF * press_v
            stage = trial if final else halo_trial
            stage[0, l] = ut
            stage[1, l] = vt
            total_u = total_u + hu * ut
            total_v = total_v + hv * vt
            if outer == 0:
                deep_u = deep_u + hu
                deep_v = deep_v + hv
        if outer == 0:
            depth[0] = deep_u
            depth[1] = deep_v
        if final:
            break
        for k, total in ((U, total_u), (V, total_v)):
            fix = (depth[k + 1] - total) / depth[k - 1]
            open_face = trimmed(base[k - 1]) != 0.0
            for l in range(layers):
                lay[k, l] = jnp.where(open_face, halo_trial[k - 1, l] + fix, 0.0)
    fixes[0] = total_u
    fixes[1] = total_v
    for cp in second_copies:
        cp.wait()
    base[4:7, cells: cells + 8] = late_east[...]
    base[4:7, cells + 8:] = late_west[...]

    def last_substep(k, sums):
        sum_u, sum_v = substep_own(k)
        return sums[0] + sum_u, sums[1] + sum_v

    own = jnp.zeros((cells, rows), F32)
    sum_u, sum_v = lax.fori_loop(0, NSUB, last_substep, (own, own))
    for k, total in ((0, sum_u), (1, sum_v)):
        fixes[k] = (total * (1.0 / NSUB) - fixes[k]) / depth[k, :cells, :rows]
        faces_out[k] = base[k, :cells, :rows]
    for k in range(3):
        state_out[k] = base[4 + k, :cells, :rows]


def finish(
    h_new, trial, fixes, faces, state, eta_out, bu_out, bv_out, h_out, u_out, v_out, results, done,
):
    layers = h_out.shape[0]
    stores = [
        pltpu.make_async_copy(src, out, done.at[k])
        for k, (src, out) in enumerate((
            (h_new, h_out),
            (state.at[0], eta_out),
            (state.at[1], bu_out),
            (state.at[2], bv_out),
            (results.at[0], u_out),
            (results.at[1], v_out),
        ))
    ]
    for cp in stores[:4]:
        cp.start()
    for k in range(2):
        open_face = faces[k] != 0.0
        fix = fixes[k]
        for l in range(layers):
            results[k, l] = jnp.where(open_face, trial[k, l] + fix, 0.0)
        stores[4 + k].start()
    for cp in stores:
        cp.wait()


def body(
    devices, height, transport_u, transport_v, thickness, velocity_u, velocity_v,
    sea_faces, wind_seeds, wind_scale, wind_base,
):
    layers, cells, rows = thickness.shape
    wide = rows + LANES
    ext = cells + 8
    anywhere = pl.BlockSpec(memory_space=pl.ANY)
    vmem = pl.BlockSpec(memory_space=pltpu.VMEM)

    def shape(*dims):
        return jax.ShapeDtypeStruct(dims, F32)

    def inner(*dims):
        return pltpu.VMEM(dims, F32)

    mid = pl.pallas_call(
        functools.partial(exchange, devices),
        out_shape=[
            inner(layers, cells, rows), inner(2, layers, cells, rows), inner(2, cells, rows),
            inner(2, cells, rows), inner(3, cells, rows),
        ],
        in_specs=[anywhere] * 10,
        out_specs=[vmem] * 5,
        scratch_shapes=[
            inner(7, cells + 16, wide),
            inner(3, layers, ext, wide),
            inner(2, layers, ext, wide),
            inner(4, ext, wide),
            pltpu.VMEM(sea_faces.shape, sea_faces.dtype),
            inner(*wind_base.shape),
            pltpu.SMEM(wind_seeds.shape[::-1], wind_seeds.dtype),
            pltpu.SMEM(wind_scale.shape, F32),
            inner(4 * layers, rows), inner(3 * layers, rows), inner(3 * layers, rows), inner(4 * layers, rows),
            inner(3, 8, wide), inner(3, 8, wide),
            inner(cells, 2 * LANES), inner(cells, 2 * LANES), inner(2, cells, LANES), inner(2, cells, LANES),
            inner(cells, 2 * LANES), inner(cells, 2 * LANES), inner(2, cells, LANES), inner(2, cells, LANES),
            pltpu.SemaphoreType.DMA((10,)),
            pltpu.SemaphoreType.DMA((17,)),
            pltpu.SemaphoreType.DMA((17,)),
            pltpu.SemaphoreType.REGULAR,
            pltpu.SemaphoreType.REGULAR,
            pltpu.SemaphoreType.REGULAR,
        ],
        compiler_params=pltpu.CompilerParams(collective_id=0, has_side_effects=True),
        name="exchange",
    )(
        height, transport_u, transport_v, thickness, velocity_u, velocity_v,
        sea_faces, wind_base, wind_seeds.T, wind_scale,
    )
    return pl.pallas_call(
        finish,
        out_shape=[shape(cells, rows)] * 3 + [shape(layers, cells, rows)] * 3,
        in_specs=[vmem] * 5,
        out_specs=[anywhere] * 6,
        scratch_shapes=[inner(2, layers, cells, rows), pltpu.SemaphoreType.DMA((6,))],
        name="finish",
    )(*[pltpu.with_memory_space_constraint(x, pltpu.VMEM) for x in mid])


def solution(mesh):
    flat = P(("members", "zonal"), "merid")
    deep = P(None, ("members", "zonal"), "merid")
    fixed = P(None, "zonal", "merid")
    return jax.shard_map(
        functools.partial(body, mesh.shape["zonal"]),
        mesh=mesh,
        in_specs=(flat, flat, flat, deep, deep, deep, fixed, P("members", None), P("members"), fixed),
        out_specs=(flat, flat, flat, deep, deep, deep),
        check_vma=False,
    )
```

```python
import functools
import math

import jax
import jax.numpy as jnp
from jax import lax
from jax.experimental import pallas as pl
from jax.experimental.pallas import tpu as pltpu
from jax.sharding import PartitionSpec as P

NSUB = 6
STEPS = 2
WAVE_LIMIT = 0.225
STRESS_SCALE = 0.1
FLUX_STEP = 0.05
PRESS_COEF = 0.05

MESH = pl.DeviceIdType.MESH
F32 = jnp.float32
OWN, EAST, WEST = 0, 1, 2
LANES = 128
STRIP = 16


def lane_iota(shape):
    return lax.broadcasted_iota(jnp.int32, shape, len(shape) - 1)


def modulo(value, size):
    return value & (size - 1) if size & (size - 1) == 0 else lax.rem(value, size)


def rolled(x, shift, axis):
    shift = shift % x.shape[axis]
    return pltpu.roll(x, shift, axis) if shift else x


def neighbours(rows):
    fold1 = jnp.logical_and(lane_iota((8, LANES)) < LANES // 2, lax.axis_index("merid") == 1)

    def merge(main, alt):
        fold = jnp.concatenate([fold1] * (alt.shape[0] // 8), 0)
        halo = jnp.where(fold, alt, main[:, rows:])
        return jnp.concatenate([main[:, :rows], halo], 1)

    def at_west(x):
        return merge(rolled(x, 1, 0), rolled(x[:, rows:], -1, 0))

    def at_east(x):
        return merge(rolled(x, -1, 0), rolled(x[:, rows:], 1, 0))

    def at_south(x):
        return merge(rolled(x, 1, 1), rolled(x[:, rows:], -1, 1))

    def at_north(x):
        return merge(rolled(x, -1, 1), rolled(x[:, rows - LANES:], 1, 1)[:, LANES:])

    return at_east, at_west, at_south, at_north


def exchange(
    devices,
    eta_ref, bu_ref, bv_ref, h_ref, u_ref, v_ref, faces_ref, base_ref, seeds_ref, scale_ref,
    h_new, trial, fixes, faces_out, state_out,
    base, lay, halo_trial, depth, faces, winds, seeds, scale, goeast, gowest, least, lwest, late_east, late_west,
    top, bottom, top_side, bottom_side, north_ref, south_ref, north_side, south_side,
    load, send, recv, near_ok, west_ok, far_ok,
):
    z = lax.axis_index("zonal")
    c = lax.axis_index("merid")
    e = lax.rem(z + 1, devices)
    w = lax.rem(z + devices - 1, devices)
    other = 1 - c
    far = [lax.rem(2 * devices - 1 - z + d, devices) for d in (0, -1, 1)]
    layers, cells, rows = h_ref.shape
    wide = rows + LANES
    ext = cells + 8
    H, U, V = 0, 1, 2

    fetches = [
        pltpu.make_async_copy(src, dst, load.at[k])
        for k, (src, dst) in enumerate((
            (eta_ref, base.at[4, pl.ds(0, cells), pl.ds(0, rows)]),
            (bu_ref, base.at[5, pl.ds(0, cells), pl.ds(0, rows)]),
            (bv_ref, base.at[6, pl.ds(0, cells), pl.ds(0, rows)]),
            (seeds_ref, seeds),
            (scale_ref, scale),
            (faces_ref, faces),
            (base_ref, winds),
            (h_ref, lay.at[H, :, pl.ds(0, cells), pl.ds(0, rows)]),
            (u_ref, lay.at[U, :, pl.ds(0, cells), pl.ds(0, rows)]),
            (v_ref, lay.at[V, :, pl.ds(0, cells), pl.ds(0, rows)]),
        ))
    ]
    for cp in fetches:
        cp.start()
    barrier = pltpu.get_barrier_semaphore()

    def greet(zonal, merid):
        pl.semaphore_signal(
            barrier, inc=1, device_id={"zonal": zonal, "merid": merid}, device_id_type=MESH
        )

    greet(w, 1)

    @pl.when(c == 0)
    def _():
        greet(z, 1)

    @pl.when(c == 1)
    def _():
        for target in far:
            greet(target, 0)

    def copy(src, dst, k, zonal, merid):
        return pltpu.make_async_remote_copy(
            src_ref=src, dst_ref=dst, send_sem=send.at[k], recv_sem=recv.at[k],
            device_id={"zonal": zonal, "merid": merid}, device_id_type=MESH,
        )

    lanes = pl.ds(0, rows)

    def to_sides(fields, k):
        return [
            copy(base.at[fields, pl.ds(8, 8), lanes], base.at[fields, pl.ds(24, 8), lanes], k, e, c),
            copy(base.at[fields, pl.ds(0, 8), lanes], base.at[fields, pl.ds(16, 8), lanes], k + 1, w, c),
        ]

    state_copies = to_sides(pl.ds(4, 3), 15)
    side_copies = to_sides(pl.ds(0, 4), 0)
    second_copies = [
        copy(base.at[pl.ds(4, 3), pl.ds(8, 8)], late_west, 2, e, c),
        copy(base.at[pl.ds(4, 3), pl.ds(0, 8)], late_east, 3, w, c),
    ]
    column_copies = [
        copy(goeast, lwest, 13, e, c),
        copy(gowest, least, 14, w, c),
    ]

    for cp in fetches[:3]:
        cp.wait()

    def tell(semaphore, zonal, merid):
        pl.semaphore_signal(
            semaphore, inc=1, device_id={"zonal": zonal, "merid": merid}, device_id_type=MESH
        )

    @pl.when(c == 1)
    def _():
        pl.semaphore_wait(barrier, 3)
        tell(near_ok, z, other)
        tell(west_ok, e, 1)
        tell(west_ok, e, 0)

    @pl.when(c == 0)
    def _():
        pl.semaphore_wait(near_ok, 1)

    state_copies[0].start()
    for cp in fetches[3:7]:
        cp.wait()
    total_x = cells * devices
    total_y = rows * 2
    cols = lax.broadcasted_iota(jnp.int32, (cells, LANES), 0) + z * cells
    rws = lax.broadcasted_iota(jnp.int32, (8, rows), 1) + c * rows
    sum_cos = jnp.zeros((cells, rows), F32)
    sum_sin = jnp.zeros((cells, rows), F32)
    for m in range(seeds.shape[1]):
        ax = (2.0 * math.pi / total_x) * modulo(seeds[0, m] * cols, total_x).astype(F32)
        ay = (2.0 * math.pi / total_y) * modulo(seeds[1, m] * rws, total_y).astype(F32)
        amp = scale[m]
        cx = jnp.concatenate([amp * jnp.cos(ax)] * (rows // LANES), 1)
        sx = jnp.concatenate([amp * jnp.sin(ax)] * (rows // LANES), 1)
        cy = jnp.concatenate([jnp.cos(ay)] * (cells // 8), 0)
        sy = jnp.concatenate([jnp.sin(ay)] * (cells // 8), 0)
        sum_cos = sum_cos + (cx * cy - sx * sy)
        sum_sin = sum_sin + (sx * cy + cx * sy)
    mask_u = faces[0].astype(F32)
    mask_v = faces[1].astype(F32)
    base[2, :cells, :rows] = mask_u * (STRESS_SCALE * (winds[0] + sum_cos))
    base[3, :cells, :rows] = mask_v * (STRESS_SCALE * (winds[1] + sum_sin))
    fetches[7].wait()
    h_sum = lay[H, 0, :cells, :rows]
    for l in range(1, layers):
        h_sum = h_sum + lay[H, l, :cells, :rows]
    wave = (WAVE_LIMIT / layers) * h_sum
    base[0, :cells, :rows] = mask_u * wave
    base[1, :cells, :rows] = mask_v * wave
    for cp in fetches[8:]:
        cp.wait()
    last = cells - 1
    h_last = lay[H, :, last, :rows]
    v_last = lay[V, :, last, :rows]
    flux_in = lay[U, :, last - 1, :rows] * (0.5 * (lay[H, :, last - 1, :rows] + h_last))
    inside = lane_iota((layers, rows)) < rows - 1
    along = jnp.where(inside, v_last * (0.5 * (h_last + rolled(h_last, -1, 1))), 0.0)
    for k, x in enumerate((h_last, lay[U, :, last, :rows], flux_in - (along - rolled(along, 1, 1)))):
        goeast[k * layers: (k + 1) * layers] = x
    ends = v_last[:, rows - LANES:]
    spare = 48 - 3 * layers
    for k in range(0, layers, spare):
        part = ends[k: k + spare]
        at = k // spare * LANES
        goeast[3 * layers: 3 * layers + part.shape[0], at: at + LANES] = part
    h_first = lay[H, :, 0, :rows]
    flux_out = lay[U, :, 0, :rows] * (0.5 * (h_first + lay[H, :, 1, :rows]))
    for k, x in enumerate((h_first, flux_out, lay[V, :, 0, :rows])):
        gowest[k * layers: (k + 1) * layers] = x

    side_copies[0].start()
    strip_rows = ((H, 0), (H, 1), (V, 0), (V, 1), (U, 0))
    lane = lane_iota((cells, LANES))
    hi = rows - LANES
    base_t = jnp.zeros((cells, LANES), F32)
    base_b = jnp.zeros((cells, LANES), F32)
    for f in range(7):
        here = lane // STRIP == f
        base_t = jnp.where(here, rolled(base[f, :cells, hi:rows], f * STRIP + STRIP, 1), base_t)
        base_b = jnp.where(here, rolled(base[f, :cells, :LANES], f * STRIP, 1), base_b)
    lay_t = jnp.zeros((cells, LANES), F32)
    lay_b = jnp.zeros((cells, LANES), F32)
    for row, (kind, depth_in) in enumerate(strip_rows):
        for l in range(layers):
            spot = row * layers + l
            here = lane == spot
            lay_t = jnp.where(here, rolled(lay[kind, l, :cells, hi:rows], spot + 1 + depth_in, 1), lay_t)
            lay_b = jnp.where(here, rolled(lay[kind, l, :cells, :LANES], spot - depth_in, 1), lay_b)
    r2 = lax.broadcasted_iota(jnp.int32, (LANES, LANES), 0)
    c2 = lax.broadcasted_iota(jnp.int32, (LANES, LANES), 1)
    perm_b = jnp.where(r2 == (c2 ^ (STRIP - 1)), 1.0, 0.0).astype(F32)
    r1 = lax.broadcasted_iota(jnp.int32, (cells, cells), 0)
    c1 = lax.broadcasted_iota(jnp.int32, (cells, cells), 1)
    mirror = jnp.where(r1 + c1 == cells - 1, 1.0, 0.0).astype(F32)
    dot = functools.partial(
        jnp.dot, preferred_element_type=F32, precision=lax.Precision.HIGHEST
    )
    north_edge = c == 1
    base_t = jnp.where(north_edge, dot(mirror, dot(base_t, perm_b)), base_t)
    lay_t = jnp.where(north_edge, dot(mirror, lay_t), lay_t)
    sub = lax.broadcasted_iota(jnp.int32, (8, LANES), 0)
    spare_lane = lane_iota((8, LANES)) >= 7 * STRIP
    for whole, side, fields, columns in ((top, top_side, base_t, lay_t), (bottom, bottom_side, base_b, lay_b)):
        whole[:, :LANES] = fields
        whole[:, LANES:] = columns
        for k, rows8, first_row in ((0, slice(8, 16), 1), (1, slice(0, 8), 0)):
            h8, v8, u8 = (
                rolled(rolled(columns[rows8], 7 * STRIP - row * layers, 1), first_row + j, 0)
                for j, row in enumerate((0, 2, 4))
            )
            spares = jnp.where(sub == 0, h8, jnp.where(sub == 1, v8, u8))
            side[k] = jnp.where(spare_lane, spares, fields[rows8])

    def strips(whole, side, into, into_side, k, own, to_west_slot, to_east_slot, merid):
        return [
            copy(whole, into, k, own, merid),
            copy(side.at[0], into_side.at[0], k + 1, to_west_slot, merid),
            copy(side.at[1], into_side.at[1], k + 2, to_east_slot, merid),
        ]

    far_targets = (far[0], far[2], far[1])
    far_copies = strips(top, top_side, north_ref, north_side, 4, *far_targets, c)
    up_copies = strips(top, top_side, south_ref, south_side, 7, z, e, w, other)
    down_copies = strips(bottom, bottom_side, north_ref, north_side, 10, z, e, w, other)

    @pl.when(c == 0)
    def _():
        up_copies[0].start()
        up_copies[1].start()

    @pl.when(c == 1)
    def _():
        down_copies[0].start()
        down_copies[1].start()

    def send_far():
        @pl.when(c == 0)
        def _():
            pl.semaphore_wait(barrier, 3)
            pl.semaphore_signal(
                far_ok, inc=1, device_id={"zonal": z, "merid": other}, device_id_type=MESH
            )

        @pl.when(c == 1)
        def _():
            pl.semaphore_wait(far_ok, 1)
            for target, cp in zip(far_targets, far_copies):
                @pl.when(target != z)
                def _(cp=cp):
                    cp.start()

    late = 2 * z >= devices

    @pl.when(late)
    def _():
        send_far()

    column_copies[0].start()

    pl.semaphore_wait(west_ok, 1)
    state_copies[1].start()
    side_copies[1].start()

    @pl.when(c == 0)
    def _():
        up_copies[2].start()

    @pl.when(c == 1)
    def _():
        down_copies[2].start()

    @pl.when(jnp.logical_not(late))
    def _():
        send_far()

    column_copies[1].start()

    @pl.when(c == 0)
    def _():
        south_ref[...] = jnp.zeros_like(south_ref)
        south_side[...] = jnp.zeros_like(south_side)

    for target, dst, src in (
        (far_targets[0], north_ref, top),
        (far_targets[1], north_side.at[0], top_side.at[0]),
        (far_targets[2], north_side.at[1], top_side.at[1]),
    ):
        @pl.when(jnp.logical_and(c == 1, target == z))
        def _(dst=dst, src=src):
            dst[...] = src[...]

    for kind in (H, U, V):
        for l in range(layers):
            lay[kind, l, cells:, :rows] = jnp.zeros((8, rows), F32)

    for cp in state_copies + side_copies:
        cp.wait()

    @pl.when(c == 0)
    def _():
        for cp in up_copies:
            cp.wait_send()
        for cp in down_copies:
            cp.wait_recv()

    @pl.when(c == 1)
    def _():
        for cp in down_copies:
            cp.wait_send()
        for cp in up_copies:
            cp.wait_recv()

    for target, cp in zip(far_targets, far_copies):
        @pl.when(jnp.logical_and(c == 1, target != z))
        def _(cp=cp):
            cp.wait()

    first8 = lane_iota((8, LANES)) < LANES // 2
    far_rows = lax.broadcasted_iota(jnp.int32, (8, LANES), 0) < 4
    norths = [north_ref[:, :LANES], north_side[1], north_side[0]]
    souths = [south_ref[:, :LANES], south_side[1], south_side[0]]

    def ring(x):
        return (x[OWN][:8], x[OWN][8:], x[EAST], x[WEST])

    for k, (n, s) in enumerate(zip(ring(norths), ring(souths))):
        for f in range(7):
            base[f, 8 * k: 8 * k + 8, rows:] = jnp.where(
                first8, rolled(n, -STRIP * f, 1), rolled(s, LANES - STRIP - STRIP * f, 1)
            )
    at_east, at_west, at_south, at_north = neighbours(rows)
    near = lax.broadcasted_iota(jnp.int32, (8, wide), 0) < 4

    def trimmed(x):
        return jnp.concatenate([x[:cells], jnp.where(near, x[cells: cells + 8], x[cells + 8:])], 0)

    def move(_):
        bu = base[5]
        bv = base[6]
        eta = base[4] - (bu - at_west(bu) + bv - at_south(bv))
        base[4] = eta
        au = base[0]
        bu = jnp.where(au != 0.0, bu - au * (at_east(eta) - eta) + base[2], 0.0)
        base[5] = bu
        av = base[1]
        bv = jnp.where(av != 0.0, bv - av * (at_north(eta) - eta) + base[3], 0.0)
        base[6] = bv
        return bu, bv

    def substep(k, sums):
        bu, bv = move(k)
        return sums[0] + trimmed(bu), sums[1] + trimmed(bv)

    def substep_own(k):
        bu, bv = move(k)
        return bu[:cells, :rows], bv[:cells, :rows]

    zero = jnp.zeros((ext, wide), F32)
    mean_u, mean_v = lax.fori_loop(0, NSUB, substep, (zero, zero))
    for cp in second_copies:
        cp.start()
    depth[2] = mean_u * (1.0 / NSUB)
    depth[3] = mean_v * (1.0 / NSUB)

    lane8 = lane_iota((8, LANES))

    def around(own, sides):
        def unpacked(x, row):
            h8, v8, u8 = (
                rolled(rolled(x, r * layers - 7 * STRIP, 1), row - j, 0) for j, r in enumerate((0, 2, 4))
            )
            return jnp.where(lane8 < layers, h8, jnp.where(lane8 < 4 * layers, v8, u8))

        halo = jnp.where(far_rows, unpacked(sides[1], 0), unpacked(sides[0], 7))
        return jnp.concatenate([own[:, LANES:], halo], 0)

    north = around(north_ref, north_side)
    south = around(south_ref, south_side)
    lane24 = lane_iota(north.shape)
    first24 = lane24 < LANES // 2
    for kind, row, deep_row in ((H, 0, True), (U, 4, False), (V, 2, True)):
        for l in range(layers):
            spot = row * layers + l
            n = rolled(north, -spot, 1)
            s = rolled(south, LANES - 1 - spot, 1)
            if deep_row:
                n = jnp.where(lane24 == 0, n, rolled(north, 1 - spot - layers, 1))
                s = jnp.where(lane24 == LANES - 1, s, rolled(south, LANES - 2 - spot - layers, 1))
            lay[kind, l, :, rows:] = jnp.where(first24, n, s)
    for cp in column_copies:
        cp.wait()
    end_lane = lane_iota((1, LANES)) == LANES - 1
    for l in range(layers):
        def column(ref, k):
            return ref[k * layers + l: k * layers + l + 1, :]

        lay[H, l, cells: cells + 1, :rows] = column(least, 0)
        lay[H, l, cells + 1: cells + 2, :rows] = 2.0 - column(least, 0)
        lay[U, l, cells: cells + 1, :rows] = column(least, 1)
        lay[V, l, cells: cells + 1, :rows] = column(least, 2)
        lay[H, l, ext - 1: ext, :rows] = column(lwest, 0)
        lay[H, l, ext - 2: ext - 1, :rows] = 2.0 - column(lwest, 0)
        lay[U, l, ext - 1: ext, :rows] = column(lwest, 1)
        lay[U, l, ext - 2: ext - 1, :rows] = column(lwest, 2)
        at = l // spare * LANES
        lay[V, l, ext - 1: ext, rows - LANES: rows] = jnp.where(
            end_lane, lwest[3 * layers + l % spare: 3 * layers + l % spare + 1, at: at + LANES], 0.0
        )
    for outer in range(STEPS):
        final = outer == STEPS - 1
        size_c, size_r = (cells, rows) if final else (ext, wide)
        press_u = press_v = total_u = total_v = jnp.zeros((size_c, size_r), F32)
        deep_u = deep_v = press_u
        for l in range(layers):
            h = lay[H, l]
            u = lay[U, l]
            v = lay[V, l]
            if final:
                diff_u = rolled(h[:, :rows], -1, 0) - h[:, :rows]
                diff_v = rolled(h[:cells], -1, 1) - h[:cells]
                hu = h[:, :rows] + 0.5 * diff_u
                hv = h[:cells] + 0.5 * diff_v
                flux_u = u[:, :rows] * hu
                flux_v = v[:cells] * hv
                out_u = (flux_u - rolled(flux_u, 1, 0))[:cells]
                out_v = (flux_v - rolled(flux_v, 1, 1))[:, :rows]
                h_new[l] = h[:cells, :rows] - FLUX_STEP * (out_u + out_v)
                diff_u, hu = diff_u[:cells], hu[:cells]
                diff_v, hv = diff_v[:, :rows], hv[:, :rows]
                u, v = u[:cells, :rows], v[:cells, :rows]
            else:
                diff_u = at_east(h) - h
                diff_v = at_north(h) - h
                hu = h + 0.5 * diff_u
                hv = h + 0.5 * diff_v
                flux_u = u * hu
                flux_v = v * hv
                lay[H, l] = h - FLUX_STEP * (flux_u - at_west(flux_u) + flux_v - at_south(flux_v))
            press_u = press_u + diff_u
            press_v = press_v + diff_v
            ut = u - PRESS_COEF * press_u
            vt = v - PRESS_COEF * press_v
            stage = trial if final else halo_trial
            stage[0, l] = ut
            stage[1, l] = vt
            total_u = total_u + hu * ut
            total_v = total_v + hv * vt
            if outer == 0:
                deep_u = deep_u + hu
                deep_v = deep_v + hv
        if outer == 0:
            depth[0] = deep_u
            depth[1] = deep_v
        if final:
            break
        for k, total in ((U, total_u), (V, total_v)):
            fix = (depth[k + 1] - total) / depth[k - 1]
            open_face = trimmed(base[k - 1]) != 0.0
            for l in range(layers):
                lay[k, l] = jnp.where(open_face, halo_trial[k - 1, l] + fix, 0.0)
    fixes[0] = total_u
    fixes[1] = total_v
    for cp in second_copies:
        cp.wait()
    base[4:7, cells: cells + 8] = late_east[...]
    base[4:7, cells + 8:] = late_west[...]

    def last_substep(k, sums):
        sum_u, sum_v = substep_own(k)
        return sums[0] + sum_u, sums[1] + sum_v

    own = jnp.zeros((cells, rows), F32)
    sum_u, sum_v = lax.fori_loop(0, NSUB, last_substep, (own, own))
    for k, total in ((0, sum_u), (1, sum_v)):
        fixes[k] = (total * (1.0 / NSUB) - fixes[k]) / depth[k, :cells, :rows]
        faces_out[k] = base[k, :cells, :rows]
    for k in range(3):
        state_out[k] = base[4 + k, :cells, :rows]


def finish(
    h_new, trial, fixes, faces, state, eta_out, bu_out, bv_out, h_out, u_out, v_out, results, done,
):
    layers = h_out.shape[0]
    stores = [
        pltpu.make_async_copy(src, out, done.at[k])
        for k, (src, out) in enumerate((
            (h_new, h_out),
            (state.at[0], eta_out),
            (state.at[1], bu_out),
            (state.at[2], bv_out),
            (results.at[0], u_out),
            (results.at[1], v_out),
        ))
    ]
    for cp in stores[:4]:
        cp.start()
    for k in range(2):
        open_face = faces[k] != 0.0
        fix = fixes[k]
        for l in range(layers):
            results[k, l] = jnp.where(open_face, trial[k, l] + fix, 0.0)
        stores[4 + k].start()
    for cp in stores:
        cp.wait()


def body(
    devices, height, transport_u, transport_v, thickness, velocity_u, velocity_v,
    sea_faces, wind_seeds, wind_scale, wind_base,
):
    layers, cells, rows = thickness.shape
    wide = rows + LANES
    ext = cells + 8
    anywhere = pl.BlockSpec(memory_space=pl.ANY)
    vmem = pl.BlockSpec(memory_space=pltpu.VMEM)

    def shape(*dims):
        return jax.ShapeDtypeStruct(dims, F32)

    def inner(*dims):
        return pltpu.VMEM(dims, F32)

    mid = pl.pallas_call(
        functools.partial(exchange, devices),
        out_shape=[
            inner(layers, cells, rows), inner(2, layers, cells, rows), inner(2, cells, rows),
            inner(2, cells, rows), inner(3, cells, rows),
        ],
        in_specs=[anywhere] * 10,
        out_specs=[vmem] * 5,
        scratch_shapes=[
            inner(7, cells + 16, wide),
            inner(3, layers, ext, wide),
            inner(2, layers, ext, wide),
            inner(4, ext, wide),
            pltpu.VMEM(sea_faces.shape, sea_faces.dtype),
            inner(*wind_base.shape),
            pltpu.SMEM(wind_seeds.shape[::-1], wind_seeds.dtype),
            pltpu.SMEM(wind_scale.shape, F32),
            inner(48, rows), inner(3 * layers, rows), inner(3 * layers, rows), inner(48, rows),
            inner(3, 8, wide), inner(3, 8, wide),
            inner(cells, 2 * LANES), inner(cells, 2 * LANES), inner(2, 8, LANES), inner(2, 8, LANES),
            inner(cells, 2 * LANES), inner(cells, 2 * LANES), inner(2, 8, LANES), inner(2, 8, LANES),
            pltpu.SemaphoreType.DMA((10,)),
            pltpu.SemaphoreType.DMA((17,)),
            pltpu.SemaphoreType.DMA((17,)),
            pltpu.SemaphoreType.REGULAR,
            pltpu.SemaphoreType.REGULAR,
            pltpu.SemaphoreType.REGULAR,
        ],
        compiler_params=pltpu.CompilerParams(collective_id=0, has_side_effects=True),
        name="exchange",
    )(
        height, transport_u, transport_v, thickness, velocity_u, velocity_v,
        sea_faces, wind_base, wind_seeds.T, wind_scale,
    )
    return pl.pallas_call(
        finish,
        out_shape=[shape(cells, rows)] * 3 + [shape(layers, cells, rows)] * 3,
        in_specs=[vmem] * 5,
        out_specs=[anywhere] * 6,
        scratch_shapes=[inner(2, layers, cells, rows), pltpu.SemaphoreType.DMA((6,))],
        name="finish",
    )(*[pltpu.with_memory_space_constraint(x, pltpu.VMEM) for x in mid])


def solution(mesh):
    flat = P(("members", "zonal"), "merid")
    deep = P(None, ("members", "zonal"), "merid")
    fixed = P(None, "zonal", "merid")
    return jax.shard_map(
        functools.partial(body, mesh.shape["zonal"]),
        mesh=mesh,
        in_specs=(flat, flat, flat, deep, deep, deep, fixed, P("members", None), P("members"), fixed),
        out_specs=(flat, flat, flat, deep, deep, deep),
        check_vma=False,
    )
```

```python
import functools
import math

import jax
import jax.numpy as jnp
from jax import lax
from jax.experimental import pallas as pl
from jax.experimental.pallas import tpu as pltpu
from jax.sharding import PartitionSpec as P

NSUB = 6
STEPS = 2
WAVE_LIMIT = 0.225
STRESS_SCALE = 0.1
FLUX_STEP = 0.05
PRESS_COEF = 0.05

MESH = pl.DeviceIdType.MESH
F32 = jnp.float32
OWN, EAST, WEST = 0, 1, 2
LANES = 128
STRIP = 16


def lane_iota(shape):
    return lax.broadcasted_iota(jnp.int32, shape, len(shape) - 1)


def modulo(value, size):
    return value & (size - 1) if size & (size - 1) == 0 else lax.rem(value, size)


def rolled(x, shift, axis):
    shift = shift % x.shape[axis]
    return pltpu.roll(x, shift, axis) if shift else x


def neighbours(rows):
    fold1 = jnp.logical_and(lane_iota((8, LANES)) < LANES // 2, lax.axis_index("merid") == 1)

    def merge(main, alt):
        fold = jnp.concatenate([fold1] * (alt.shape[0] // 8), 0)
        halo = jnp.where(fold, alt, main[:, rows:])
        return jnp.concatenate([main[:, :rows], halo], 1)

    def at_west(x):
        return merge(rolled(x, 1, 0), rolled(x[:, rows:], -1, 0))

    def at_east(x):
        return merge(rolled(x, -1, 0), rolled(x[:, rows:], 1, 0))

    def at_south(x):
        return merge(rolled(x, 1, 1), rolled(x[:, rows:], -1, 1))

    def at_north(x):
        return merge(rolled(x, -1, 1), rolled(x[:, rows - LANES:], 1, 1)[:, LANES:])

    return at_east, at_west, at_south, at_north


def exchange(
    devices,
    eta_ref, bu_ref, bv_ref, h_ref, u_ref, v_ref, faces_ref, base_ref, seeds_ref, scale_ref,
    h_new, trial, fixes, faces_out, state_out,
    base, lay, trial_u, trial_v, leaving, depth, faces, winds, seeds, scale, goeast, gowest, least, lwest, late_east, late_west,
    top, bottom, top_side, bottom_side, north_ref, south_ref, north_side, south_side,
    load, send, recv, near_ok, west_ok, far_ok,
):
    z = lax.axis_index("zonal")
    c = lax.axis_index("merid")
    e = lax.rem(z + 1, devices)
    w = lax.rem(z + devices - 1, devices)
    other = 1 - c
    far = [lax.rem(2 * devices - 1 - z + d, devices) for d in (0, -1, 1)]
    layers, cells, rows = h_ref.shape
    wide = rows + LANES
    ext = cells + 8
    H, U, V = 0, 1, 2

    fetches = [
        pltpu.make_async_copy(src, dst, load.at[k])
        for k, (src, dst) in enumerate((
            (eta_ref, base.at[4, pl.ds(0, cells), pl.ds(0, rows)]),
            (bu_ref, base.at[5, pl.ds(0, cells), pl.ds(0, rows)]),
            (bv_ref, base.at[6, pl.ds(0, cells), pl.ds(0, rows)]),
            (seeds_ref, seeds),
            (scale_ref, scale),
            (faces_ref, faces),
            (base_ref, winds),
            (h_ref, lay.at[H, :, pl.ds(0, cells), pl.ds(0, rows)]),
            (u_ref, lay.at[U, :, pl.ds(0, cells), pl.ds(0, rows)]),
            (v_ref, lay.at[V, :, pl.ds(0, cells), pl.ds(0, rows)]),
        ))
    ]
    for cp in fetches:
        cp.start()
    barrier = pltpu.get_barrier_semaphore()

    def greet(zonal, merid):
        pl.semaphore_signal(
            barrier, inc=1, device_id={"zonal": zonal, "merid": merid}, device_id_type=MESH
        )

    greet(w, 1)

    @pl.when(c == 0)
    def _():
        greet(z, 1)

    @pl.when(c == 1)
    def _():
        for target in far:
            greet(target, 0)

    def copy(src, dst, k, zonal, merid):
        return pltpu.make_async_remote_copy(
            src_ref=src, dst_ref=dst, send_sem=send.at[k], recv_sem=recv.at[k],
            device_id={"zonal": zonal, "merid": merid}, device_id_type=MESH,
        )

    lanes = pl.ds(0, rows)

    def to_sides(fields, k):
        return [
            copy(base.at[fields, pl.ds(8, 8), lanes], base.at[fields, pl.ds(24, 8), lanes], k, e, c),
            copy(base.at[fields, pl.ds(0, 8), lanes], base.at[fields, pl.ds(16, 8), lanes], k + 1, w, c),
        ]

    state_copies = to_sides(pl.ds(4, 3), 15)
    side_copies = to_sides(pl.ds(0, 4), 0)
    second_copies = [
        copy(base.at[pl.ds(4, 3), pl.ds(8, 8)], late_west, 2, e, c),
        copy(base.at[pl.ds(4, 3), pl.ds(0, 8)], late_east, 3, w, c),
    ]
    column_copies = [
        copy(goeast, lwest, 13, e, c),
        copy(gowest, least, 14, w, c),
    ]

    def tell(semaphore, zonal, merid):
        pl.semaphore_signal(
            semaphore, inc=1, device_id={"zonal": zonal, "merid": merid}, device_id_type=MESH
        )

    @pl.when(c == 1)
    def _():
        pl.semaphore_wait(barrier, 3)
        tell(near_ok, z, other)
        tell(west_ok, e, 1)
        tell(west_ok, e, 0)

    @pl.when(c == 0)
    def _():
        pl.semaphore_wait(near_ok, 1)

    for cp in fetches[:3]:
        cp.wait()
    state_copies[0].start()
    for cp in fetches[3:7]:
        cp.wait()
    total_x = cells * devices
    total_y = rows * 2
    cols = lax.broadcasted_iota(jnp.int32, (cells, LANES), 0) + z * cells
    rws = lax.broadcasted_iota(jnp.int32, (8, rows), 1) + c * rows
    sum_cos = jnp.zeros((cells, rows), F32)
    sum_sin = jnp.zeros((cells, rows), F32)
    for m in range(seeds.shape[1]):
        ax = (2.0 * math.pi / total_x) * modulo(seeds[0, m] * cols, total_x).astype(F32)
        ay = (2.0 * math.pi / total_y) * modulo(seeds[1, m] * rws, total_y).astype(F32)
        amp = scale[m]
        cx = jnp.concatenate([amp * jnp.cos(ax)] * (rows // LANES), 1)
        sx = jnp.concatenate([amp * jnp.sin(ax)] * (rows // LANES), 1)
        cy = jnp.concatenate([jnp.cos(ay)] * (cells // 8), 0)
        sy = jnp.concatenate([jnp.sin(ay)] * (cells // 8), 0)
        sum_cos = sum_cos + (cx * cy - sx * sy)
        sum_sin = sum_sin + (sx * cy + cx * sy)
    mask_u = faces[0].astype(F32)
    mask_v = faces[1].astype(F32)
    base[2, :cells, :rows] = mask_u * (STRESS_SCALE * (winds[0] + sum_cos))
    base[3, :cells, :rows] = mask_v * (STRESS_SCALE * (winds[1] + sum_sin))
    fetches[7].wait()
    h_sum = lay[H, 0, :cells, :rows]
    for l in range(1, layers):
        h_sum = h_sum + lay[H, l, :cells, :rows]
    wave = (WAVE_LIMIT / layers) * h_sum
    base[0, :cells, :rows] = mask_u * wave
    base[1, :cells, :rows] = mask_v * wave
    for cp in fetches[8:]:
        cp.wait()
    side_copies[0].start()
    strip_rows = ((H, 0), (H, 1), (V, 0), (V, 1), (U, 0))
    lane = lane_iota((cells, LANES))
    hi = rows - LANES
    base_t = jnp.zeros((cells, LANES), F32)
    base_b = jnp.zeros((cells, LANES), F32)
    for f in range(7):
        here = lane // STRIP == f
        base_t = jnp.where(here, rolled(base[f, :cells, hi:rows], f * STRIP + STRIP, 1), base_t)
        base_b = jnp.where(here, rolled(base[f, :cells, :LANES], f * STRIP, 1), base_b)
    lay_t = jnp.zeros((cells, LANES), F32)
    lay_b = jnp.zeros((cells, LANES), F32)
    for row, (kind, depth_in) in enumerate(strip_rows):
        for l in range(layers):
            spot = row * layers + l
            here = lane == spot
            lay_t = jnp.where(here, rolled(lay[kind, l, :cells, hi:rows], spot + 1 + depth_in, 1), lay_t)
            lay_b = jnp.where(here, rolled(lay[kind, l, :cells, :LANES], spot - depth_in, 1), lay_b)
    r2 = lax.broadcasted_iota(jnp.int32, (LANES, LANES), 0)
    c2 = lax.broadcasted_iota(jnp.int32, (LANES, LANES), 1)
    perm_b = jnp.where(r2 == (c2 ^ (STRIP - 1)), 1.0, 0.0).astype(F32)
    r1 = lax.broadcasted_iota(jnp.int32, (cells, cells), 0)
    c1 = lax.broadcasted_iota(jnp.int32, (cells, cells), 1)
    mirror = jnp.where(r1 + c1 == cells - 1, 1.0, 0.0).astype(F32)
    dot = functools.partial(
        jnp.dot, preferred_element_type=F32, precision=lax.Precision.HIGHEST
    )
    north_edge = c == 1
    base_t = jnp.where(north_edge, dot(mirror, dot(base_t, perm_b)), base_t)
    lay_t = jnp.where(north_edge, dot(mirror, lay_t), lay_t)
    sub = lax.broadcasted_iota(jnp.int32, (8, LANES), 0)
    spare_lane = lane_iota((8, LANES)) >= 7 * STRIP
    for whole, side, fields, columns in ((top, top_side, base_t, lay_t), (bottom, bottom_side, base_b, lay_b)):
        whole[:, :LANES] = fields
        whole[:, LANES:] = columns
        for k, rows8, first_row in ((0, slice(8, 16), 1), (1, slice(0, 8), 0)):
            h8, v8, u8 = (
                rolled(rolled(columns[rows8], 7 * STRIP - row * layers, 1), first_row + j, 0)
                for j, row in enumerate((0, 2, 4))
            )
            spares = jnp.where(sub == 0, h8, jnp.where(sub == 1, v8, u8))
            side[k] = jnp.where(spare_lane, spares, fields[rows8])

    def strips(whole, side, into, into_side, k, own, to_west_slot, to_east_slot, merid):
        return [
            copy(whole, into, k, own, merid),
            copy(side.at[0], into_side.at[0], k + 1, to_west_slot, merid),
            copy(side.at[1], into_side.at[1], k + 2, to_east_slot, merid),
        ]

    far_targets = (far[0], far[2], far[1])
    far_copies = strips(top, top_side, north_ref, north_side, 4, *far_targets, c)
    up_copies = strips(top, top_side, south_ref, south_side, 7, z, e, w, other)
    down_copies = strips(bottom, bottom_side, north_ref, north_side, 10, z, e, w, other)

    @pl.when(c == 0)
    def _():
        up_copies[0].start()
        up_copies[1].start()

    @pl.when(c == 1)
    def _():
        down_copies[0].start()
        down_copies[1].start()

    def send_far():
        @pl.when(c == 0)
        def _():
            pl.semaphore_wait(barrier, 3)
            pl.semaphore_signal(
                far_ok, inc=1, device_id={"zonal": z, "merid": other}, device_id_type=MESH
            )

        @pl.when(c == 1)
        def _():
            pl.semaphore_wait(far_ok, 1)
            for target, cp in zip(far_targets, far_copies):
                @pl.when(target != z)
                def _(cp=cp):
                    cp.start()

    late = 2 * z >= devices

    @pl.when(late)
    def _():
        send_far()

    last = cells - 1
    h_last = lay[H, :, last, :rows]
    v_last = lay[V, :, last, :rows]
    flux_in = lay[U, :, last - 1, :rows] * (0.5 * (lay[H, :, last - 1, :rows] + h_last))
    inside = lane_iota((layers, rows)) < rows - 1
    along = jnp.where(inside, v_last * (0.5 * (h_last + rolled(h_last, -1, 1))), 0.0)
    for k, x in enumerate((h_last, lay[U, :, last, :rows], flux_in - (along - rolled(along, 1, 1)))):
        goeast[k * layers: (k + 1) * layers] = x
    ends = v_last[:, rows - LANES:]
    spare = 48 - 3 * layers
    for k in range(0, layers, spare):
        part = ends[k: k + spare]
        at = k // spare * LANES
        goeast[3 * layers: 3 * layers + part.shape[0], at: at + LANES] = part
    h_first = lay[H, :, 0, :rows]
    flux_out = lay[U, :, 0, :rows] * (0.5 * (h_first + lay[H, :, 1, :rows]))
    for k, x in enumerate((h_first, flux_out, lay[V, :, 0, :rows])):
        gowest[k * layers: (k + 1) * layers] = x

    column_copies[0].start()

    pl.semaphore_wait(west_ok, 1)
    state_copies[1].start()
    side_copies[1].start()

    @pl.when(c == 0)
    def _():
        up_copies[2].start()

    @pl.when(c == 1)
    def _():
        down_copies[2].start()

    @pl.when(jnp.logical_not(late))
    def _():
        send_far()

    column_copies[1].start()

    @pl.when(c == 0)
    def _():
        south_ref[...] = jnp.zeros_like(south_ref)
        south_side[...] = jnp.zeros_like(south_side)

    for target, dst, src in (
        (far_targets[0], north_ref, top),
        (far_targets[1], north_side.at[0], top_side.at[0]),
        (far_targets[2], north_side.at[1], top_side.at[1]),
    ):
        @pl.when(jnp.logical_and(c == 1, target == z))
        def _(dst=dst, src=src):
            dst[...] = src[...]

    for kind in (H, U, V):
        for l in range(layers):
            lay[kind, l, cells:, :rows] = jnp.zeros((8, rows), F32)

    for cp in state_copies + side_copies:
        cp.wait()

    @pl.when(c == 0)
    def _():
        for cp in up_copies:
            cp.wait_send()
        for cp in down_copies:
            cp.wait_recv()

    @pl.when(c == 1)
    def _():
        for cp in down_copies:
            cp.wait_send()
        for cp in up_copies:
            cp.wait_recv()

    for target, cp in zip(far_targets, far_copies):
        @pl.when(jnp.logical_and(c == 1, target != z))
        def _(cp=cp):
            cp.wait()

    first8 = lane_iota((8, LANES)) < LANES // 2
    far_rows = lax.broadcasted_iota(jnp.int32, (8, LANES), 0) < 4
    norths = [north_ref[:, :LANES], north_side[1], north_side[0]]
    souths = [south_ref[:, :LANES], south_side[1], south_side[0]]

    def ring(x):
        return (x[OWN][:8], x[OWN][8:], x[EAST], x[WEST])

    for k, (n, s) in enumerate(zip(ring(norths), ring(souths))):
        for f in range(7):
            base[f, 8 * k: 8 * k + 8, rows:] = jnp.where(
                first8, rolled(n, -STRIP * f, 1), rolled(s, LANES - STRIP - STRIP * f, 1)
            )
    at_east, at_west, at_south, at_north = neighbours(rows)
    near = lax.broadcasted_iota(jnp.int32, (8, wide), 0) < 4

    def trimmed(x):
        return jnp.concatenate([x[:cells], jnp.where(near, x[cells: cells + 8], x[cells + 8:])], 0)

    def move(first=False):
        bu = base[5]
        bv = base[6]
        eta = base[4] - (bu - at_west(bu) + bv - at_south(bv))
        base[4] = eta
        au = base[0]
        bu = bu - au * (at_east(eta) - eta) + base[2]
        if first:
            bu = jnp.where(au != 0.0, bu, 0.0)
        base[5] = bu
        av = base[1]
        bv = bv - av * (at_north(eta) - eta) + base[3]
        if first:
            bv = jnp.where(av != 0.0, bv, 0.0)
        base[6] = bv
        return bu, bv

    def substep(_, sums):
        bu, bv = move()
        return sums[0] + trimmed(bu), sums[1] + trimmed(bv)

    def substep_own():
        bu, bv = move()
        return bu[:cells, :rows], bv[:cells, :rows]

    first_u, first_v = move(first=True)
    mean_u, mean_v = lax.fori_loop(1, NSUB, substep, (trimmed(first_u), trimmed(first_v)))
    for cp in second_copies:
        cp.start()
    depth[2] = mean_u * (1.0 / NSUB)
    depth[3] = mean_v * (1.0 / NSUB)

    lane8 = lane_iota((8, LANES))

    def around(own, sides):
        def unpacked(x, row):
            h8, v8, u8 = (
                rolled(rolled(x, r * layers - 7 * STRIP, 1), row - j, 0) for j, r in enumerate((0, 2, 4))
            )
            return jnp.where(lane8 < layers, h8, jnp.where(lane8 < 4 * layers, v8, u8))

        halo = jnp.where(far_rows, unpacked(sides[1], 0), unpacked(sides[0], 7))
        return jnp.concatenate([own[:, LANES:], halo], 0)

    north = around(north_ref, north_side)
    south = around(south_ref, south_side)
    lane24 = lane_iota(north.shape)
    first24 = lane24 < LANES // 2
    for kind, row, deep_row in ((H, 0, True), (U, 4, False), (V, 2, True)):
        for l in range(layers):
            spot = row * layers + l
            n = rolled(north, -spot, 1)
            s = rolled(south, LANES - 1 - spot, 1)
            if deep_row:
                n = jnp.where(lane24 == 0, n, rolled(north, 1 - spot - layers, 1))
                s = jnp.where(lane24 == LANES - 1, s, rolled(south, LANES - 2 - spot - layers, 1))
            lay[kind, l, :, rows:] = jnp.where(first24, n, s)
    press = total = deep = jnp.zeros((cells, wide), F32)
    for l in range(layers):
        h = lay[H, l, :cells]
        v = lay[V, l, :cells]
        diff = at_north(h) - h
        press = press + diff
        half = h + 0.5 * diff
        flux = v * half
        leaving[l] = flux - at_south(flux)
        vt = v - PRESS_COEF * press
        trial_v[l] = vt
        total = total + half * vt
        deep = deep + half
    depth[1, :cells] = deep
    fix = (depth[3, :cells] - total) / deep
    open_face = base[1, :cells] != 0.0
    for l in range(layers):
        lay[V, l, :cells] = jnp.where(open_face, trial_v[l] + fix, 0.0)
    for cp in column_copies:
        cp.wait()
    end_lane = lane_iota((1, LANES)) == LANES - 1
    for l in range(layers):
        def column(ref, k):
            return ref[k * layers + l: k * layers + l + 1, :]

        lay[H, l, cells: cells + 1, :rows] = column(least, 0)
        lay[H, l, cells + 1: cells + 2, :rows] = 2.0 - column(least, 0)
        lay[U, l, cells: cells + 1, :rows] = column(least, 1)
        lay[V, l, cells: cells + 1, :rows] = column(least, 2)
        lay[H, l, ext - 1: ext, :rows] = column(lwest, 0)
        lay[H, l, ext - 2: ext - 1, :rows] = 2.0 - column(lwest, 0)
        lay[U, l, ext - 1: ext, :rows] = column(lwest, 1)
        lay[U, l, ext - 2: ext - 1, :rows] = column(lwest, 2)
        at = l // spare * LANES
        lay[V, l, ext - 1: ext, rows - LANES: rows] = jnp.where(
            end_lane, lwest[3 * layers + l % spare: 3 * layers + l % spare + 1, at: at + LANES], 0.0
        )
    press = total = deep = jnp.zeros((ext, wide), F32)
    for l in range(layers):
        h = lay[H, l]
        u = lay[U, l]
        diff = at_east(h) - h
        press = press + diff
        half = h + 0.5 * diff
        flux = u * half
        side_h = h[cells:]
        side_flux = lay[V, l, cells:] * (side_h + 0.5 * (at_north(side_h) - side_h))
        out_v = jnp.concatenate([leaving[l], side_flux - at_south(side_flux)], 0)
        lay[H, l] = h - FLUX_STEP * (flux - at_west(flux) + out_v)
        ut = u - PRESS_COEF * press
        trial_u[l] = ut[:, :rows]
        total = total + half * ut
        deep = deep + half
    depth[0] = deep
    fix = ((depth[2] - total) / deep)[:, :rows]
    open_face = trimmed(base[0])[:, :rows] != 0.0
    for l in range(layers):
        lay[U, l, :, :rows] = jnp.where(open_face, trial_u[l] + fix, 0.0)
    press_u = press_v = total_u = total_v = jnp.zeros((cells, rows), F32)
    for l in range(layers):
        h_u = lay[H, l, :, :rows]
        h_v = lay[H, l, :cells]
        diff_u = rolled(h_u, -1, 0) - h_u
        diff_v = rolled(h_v, -1, 1) - h_v
        hu = h_u + 0.5 * diff_u
        hv = h_v + 0.5 * diff_v
        u = lay[U, l, :, :rows]
        v = lay[V, l, :cells]
        flux_u = u * hu
        flux_v = v * hv
        out_u = (flux_u - rolled(flux_u, 1, 0))[:cells]
        out_v = (flux_v - rolled(flux_v, 1, 1))[:, :rows]
        h_new[l] = h_u[:cells] - FLUX_STEP * (out_u + out_v)
        press_u = press_u + diff_u[:cells]
        press_v = press_v + diff_v[:, :rows]
        ut = u[:cells] - PRESS_COEF * press_u
        vt = v[:, :rows] - PRESS_COEF * press_v
        trial[0, l] = ut
        trial[1, l] = vt
        total_u = total_u + hu[:cells] * ut
        total_v = total_v + hv[:, :rows] * vt
    fixes[0] = total_u
    fixes[1] = total_v
    for cp in second_copies:
        cp.wait()
    base[4:7, cells: cells + 8] = late_east[...]
    base[4:7, cells + 8:] = late_west[...]

    def last_substep(k, sums):
        sum_u, sum_v = substep_own()
        return sums[0] + sum_u, sums[1] + sum_v

    own = jnp.zeros((cells, rows), F32)
    sum_u, sum_v = lax.fori_loop(0, NSUB, last_substep, (own, own))
    for k, total in ((0, sum_u), (1, sum_v)):
        fixes[k] = (total * (1.0 / NSUB) - fixes[k]) / depth[k, :cells, :rows]
        faces_out[k] = base[k, :cells, :rows]
    for k in range(3):
        state_out[k] = base[4 + k, :cells, :rows]


def finish(
    h_new, trial, fixes, faces, state, eta_out, bu_out, bv_out, h_out, u_out, v_out, results, done,
):
    layers = h_out.shape[0]
    stores = [
        pltpu.make_async_copy(src, out, done.at[k])
        for k, (src, out) in enumerate((
            (h_new, h_out),
            (state.at[0], eta_out),
            (state.at[1], bu_out),
            (state.at[2], bv_out),
        ))
    ]
    half = layers // 2
    parts = (pl.ds(0, half), pl.ds(half, layers - half))
    stores += [
        pltpu.make_async_copy(results.at[k, part], out.at[part], done.at[4 + 2 * k + j])
        for k, out in enumerate((u_out, v_out))
        for j, part in enumerate(parts)
    ]
    for cp in stores[:4]:
        cp.start()
    for k in range(2):
        open_face = faces[k] != 0.0
        fix = fixes[k]
        for l in range(layers):
            results[k, l] = jnp.where(open_face, trial[k, l] + fix, 0.0)
            if l == half - 1:
                stores[4 + 2 * k].start()
        stores[5 + 2 * k].start()
    for cp in stores:
        cp.wait()


def body(
    devices, height, transport_u, transport_v, thickness, velocity_u, velocity_v,
    sea_faces, wind_seeds, wind_scale, wind_base,
):
    layers, cells, rows = thickness.shape
    wide = rows + LANES
    ext = cells + 8
    anywhere = pl.BlockSpec(memory_space=pl.ANY)
    vmem = pl.BlockSpec(memory_space=pltpu.VMEM)

    def shape(*dims):
        return jax.ShapeDtypeStruct(dims, F32)

    def inner(*dims):
        return pltpu.VMEM(dims, F32)

    mid = pl.pallas_call(
        functools.partial(exchange, devices),
        out_shape=[
            inner(layers, cells, rows), inner(2, layers, cells, rows), inner(2, cells, rows),
            inner(2, cells, rows), inner(3, cells, rows),
        ],
        in_specs=[anywhere] * 10,
        out_specs=[vmem] * 5,
        scratch_shapes=[
            inner(7, cells + 16, wide),
            inner(3, layers, ext, wide),
            inner(layers, ext, rows),
            inner(layers, cells, wide),
            inner(layers, cells, wide),
            inner(4, ext, wide),
            pltpu.VMEM(sea_faces.shape, sea_faces.dtype),
            inner(*wind_base.shape),
            pltpu.SMEM(wind_seeds.shape[::-1], wind_seeds.dtype),
            pltpu.SMEM(wind_scale.shape, F32),
            inner(48, rows), inner(3 * layers, rows), inner(3 * layers, rows), inner(48, rows),
            inner(3, 8, wide), inner(3, 8, wide),
            inner(cells, 2 * LANES), inner(cells, 2 * LANES), inner(2, 8, LANES), inner(2, 8, LANES),
            inner(cells, 2 * LANES), inner(cells, 2 * LANES), inner(2, 8, LANES), inner(2, 8, LANES),
            pltpu.SemaphoreType.DMA((10,)),
            pltpu.SemaphoreType.DMA((17,)),
            pltpu.SemaphoreType.DMA((17,)),
            pltpu.SemaphoreType.REGULAR,
            pltpu.SemaphoreType.REGULAR,
            pltpu.SemaphoreType.REGULAR,
        ],
        compiler_params=pltpu.CompilerParams(collective_id=0, has_side_effects=True),
        name="exchange",
    )(
        height, transport_u, transport_v, thickness, velocity_u, velocity_v,
        sea_faces, wind_base, wind_seeds.T, wind_scale,
    )
    return pl.pallas_call(
        finish,
        out_shape=[shape(cells, rows)] * 3 + [shape(layers, cells, rows)] * 3,
        in_specs=[vmem] * 5,
        out_specs=[anywhere] * 6,
        scratch_shapes=[inner(2, layers, cells, rows), pltpu.SemaphoreType.DMA((8,))],
        name="finish",
    )(*[pltpu.with_memory_space_constraint(x, pltpu.VMEM) for x in mid])


def solution(mesh):
    flat = P(("members", "zonal"), "merid")
    deep = P(None, ("members", "zonal"), "merid")
    fixed = P(None, "zonal", "merid")
    return jax.shard_map(
        functools.partial(body, mesh.shape["zonal"]),
        mesh=mesh,
        in_specs=(flat, flat, flat, deep, deep, deep, fixed, P("members", None), P("members"), fixed),
        out_specs=(flat, flat, flat, deep, deep, deep),
        check_vma=False,
    )
```

```python
import functools
import math

import jax
import jax.numpy as jnp
from jax import lax
from jax.experimental import pallas as pl
from jax.experimental.pallas import tpu as pltpu
from jax.sharding import PartitionSpec as P

NSUB = 6
STEPS = 2
WAVE_LIMIT = 0.225
STRESS_SCALE = 0.1
FLUX_STEP = 0.05
PRESS_COEF = 0.05

MESH = pl.DeviceIdType.MESH
F32 = jnp.float32
OWN, EAST, WEST = 0, 1, 2
LANES = 128
STRIP = 16


def lane_iota(shape):
    return lax.broadcasted_iota(jnp.int32, shape, len(shape) - 1)


def modulo(value, size):
    return value & (size - 1) if size & (size - 1) == 0 else lax.rem(value, size)


def rolled(x, shift, axis):
    shift = shift % x.shape[axis]
    return pltpu.roll(x, shift, axis) if shift else x


def neighbours(rows):
    fold1 = jnp.logical_and(lane_iota((8, LANES)) < LANES // 2, lax.axis_index("merid") == 1)

    def merge(main, alt):
        fold = jnp.concatenate([fold1] * (alt.shape[0] // 8), 0)
        halo = jnp.where(fold, alt, main[:, rows:])
        return jnp.concatenate([main[:, :rows], halo], 1)

    def at_west(x):
        return merge(rolled(x, 1, 0), rolled(x[:, rows:], -1, 0))

    def at_east(x):
        return merge(rolled(x, -1, 0), rolled(x[:, rows:], 1, 0))

    def at_south(x):
        return merge(rolled(x, 1, 1), rolled(x[:, rows:], -1, 1))

    def at_north(x):
        return merge(rolled(x, -1, 1), rolled(x[:, rows - LANES:], 1, 1)[:, LANES:])

    return at_east, at_west, at_south, at_north


def exchange(
    devices,
    eta_ref, bu_ref, bv_ref, h_ref, u_ref, v_ref, faces_ref, base_ref, seeds_ref, scale_ref,
    h_new, trial, fixes, faces_out, state_out,
    base, lay, trial_u, trial_v, leaving, depth, faces, winds, seeds, scale, goeast, gowest, least, lwest, late_east, late_west, late_strips, strips_east, strips_west,
    top, bottom, top_side, bottom_side, north_ref, south_ref, north_side, south_side,
    load, send, recv, near_ok, west_ok, far_ok,
):
    z = lax.axis_index("zonal")
    c = lax.axis_index("merid")
    e = lax.rem(z + 1, devices)
    w = lax.rem(z + devices - 1, devices)
    other = 1 - c
    far = [lax.rem(2 * devices - 1 - z + d, devices) for d in (0, -1, 1)]
    layers, cells, rows = h_ref.shape
    wide = rows + LANES
    ext = cells + 8
    H, U, V = 0, 1, 2

    fetches = [
        pltpu.make_async_copy(src, dst, load.at[k])
        for k, (src, dst) in enumerate((
            (eta_ref, base.at[4, pl.ds(0, cells), pl.ds(0, rows)]),
            (bu_ref, base.at[5, pl.ds(0, cells), pl.ds(0, rows)]),
            (bv_ref, base.at[6, pl.ds(0, cells), pl.ds(0, rows)]),
            (seeds_ref, seeds),
            (scale_ref, scale),
            (faces_ref, faces),
            (base_ref, winds),
            (h_ref, lay.at[H, :, pl.ds(0, cells), pl.ds(0, rows)]),
            (u_ref, lay.at[U, :, pl.ds(0, cells), pl.ds(0, rows)]),
            (v_ref, lay.at[V, :, pl.ds(0, cells), pl.ds(0, rows)]),
        ))
    ]
    for cp in fetches:
        cp.start()
    barrier = pltpu.get_barrier_semaphore()

    def greet(zonal, merid):
        pl.semaphore_signal(
            barrier, inc=1, device_id={"zonal": zonal, "merid": merid}, device_id_type=MESH
        )

    greet(w, 1)

    @pl.when(c == 0)
    def _():
        greet(z, 1)

    @pl.when(c == 1)
    def _():
        for target in far:
            greet(target, 0)

    def copy(src, dst, k, zonal, merid):
        return pltpu.make_async_remote_copy(
            src_ref=src, dst_ref=dst, send_sem=send.at[k], recv_sem=recv.at[k],
            device_id={"zonal": zonal, "merid": merid}, device_id_type=MESH,
        )

    lanes = pl.ds(0, rows)

    def to_sides(fields, k):
        return [
            copy(base.at[fields, pl.ds(8, 8), lanes], base.at[fields, pl.ds(24, 8), lanes], k, e, c),
            copy(base.at[fields, pl.ds(0, 8), lanes], base.at[fields, pl.ds(16, 8), lanes], k + 1, w, c),
        ]

    state_copies = to_sides(pl.ds(4, 3), 15)
    side_copies = to_sides(pl.ds(0, 4), 0)
    second_copies = [
        copy(base.at[pl.ds(4, 3), pl.ds(8, 8), lanes], late_west, 2, e, c),
        copy(base.at[pl.ds(4, 3), pl.ds(0, 8), lanes], late_east, 3, w, c),
        copy(late_strips.at[1], strips_west, 17, e, c),
        copy(late_strips.at[0], strips_east, 18, w, c),
    ]
    column_copies = [
        copy(goeast, lwest, 13, e, c),
        copy(gowest, least, 14, w, c),
    ]

    def tell(semaphore, zonal, merid):
        pl.semaphore_signal(
            semaphore, inc=1, device_id={"zonal": zonal, "merid": merid}, device_id_type=MESH
        )

    @pl.when(c == 1)
    def _():
        pl.semaphore_wait(barrier, 3)
        tell(near_ok, z, other)
        tell(west_ok, e, 1)
        tell(west_ok, e, 0)

    @pl.when(c == 0)
    def _():
        pl.semaphore_wait(near_ok, 1)

    for cp in fetches[:3]:
        cp.wait()
    state_copies[0].start()
    for cp in fetches[3:7]:
        cp.wait()
    total_x = cells * devices
    total_y = rows * 2
    cols = lax.broadcasted_iota(jnp.int32, (cells, LANES), 0) + z * cells
    rws = lax.broadcasted_iota(jnp.int32, (8, rows), 1) + c * rows
    sum_cos = jnp.zeros((cells, rows), F32)
    sum_sin = jnp.zeros((cells, rows), F32)
    for m in range(seeds.shape[1]):
        ax = (2.0 * math.pi / total_x) * modulo(seeds[0, m] * cols, total_x).astype(F32)
        ay = (2.0 * math.pi / total_y) * modulo(seeds[1, m] * rws, total_y).astype(F32)
        amp = scale[m]
        cx = jnp.concatenate([amp * jnp.cos(ax)] * (rows // LANES), 1)
        sx = jnp.concatenate([amp * jnp.sin(ax)] * (rows // LANES), 1)
        cy = jnp.concatenate([jnp.cos(ay)] * (cells // 8), 0)
        sy = jnp.concatenate([jnp.sin(ay)] * (cells // 8), 0)
        sum_cos = sum_cos + (cx * cy - sx * sy)
        sum_sin = sum_sin + (sx * cy + cx * sy)
    mask_u = faces[0].astype(F32)
    mask_v = faces[1].astype(F32)
    base[2, :cells, :rows] = mask_u * (STRESS_SCALE * (winds[0] + sum_cos))
    base[3, :cells, :rows] = mask_v * (STRESS_SCALE * (winds[1] + sum_sin))
    fetches[7].wait()
    h_sum = lay[H, 0, :cells, :rows]
    for l in range(1, layers):
        h_sum = h_sum + lay[H, l, :cells, :rows]
    wave = (WAVE_LIMIT / layers) * h_sum
    base[0, :cells, :rows] = mask_u * wave
    base[1, :cells, :rows] = mask_v * wave
    for cp in fetches[8:]:
        cp.wait()
    side_copies[0].start()
    strip_rows = ((H, 0), (H, 1), (V, 0), (V, 1), (U, 0))
    lane = lane_iota((cells, LANES))
    hi = rows - LANES
    base_t = jnp.zeros((cells, LANES), F32)
    base_b = jnp.zeros((cells, LANES), F32)
    for f in range(7):
        here = lane // STRIP == f
        base_t = jnp.where(here, rolled(base[f, :cells, hi:rows], f * STRIP + STRIP, 1), base_t)
        base_b = jnp.where(here, rolled(base[f, :cells, :LANES], f * STRIP, 1), base_b)
    lay_t = jnp.zeros((cells, LANES), F32)
    lay_b = jnp.zeros((cells, LANES), F32)
    for row, (kind, depth_in) in enumerate(strip_rows):
        for l in range(layers):
            spot = row * layers + l
            here = lane == spot
            lay_t = jnp.where(here, rolled(lay[kind, l, :cells, hi:rows], spot + 1 + depth_in, 1), lay_t)
            lay_b = jnp.where(here, rolled(lay[kind, l, :cells, :LANES], spot - depth_in, 1), lay_b)
    r2 = lax.broadcasted_iota(jnp.int32, (LANES, LANES), 0)
    c2 = lax.broadcasted_iota(jnp.int32, (LANES, LANES), 1)
    perm_b = jnp.where(r2 == (c2 ^ (STRIP - 1)), 1.0, 0.0).astype(F32)
    r1 = lax.broadcasted_iota(jnp.int32, (cells, cells), 0)
    c1 = lax.broadcasted_iota(jnp.int32, (cells, cells), 1)
    mirror = jnp.where(r1 + c1 == cells - 1, 1.0, 0.0).astype(F32)
    dot = functools.partial(
        jnp.dot, preferred_element_type=F32, precision=lax.Precision.HIGHEST
    )
    north_edge = c == 1
    base_t = jnp.where(north_edge, dot(mirror, dot(base_t, perm_b)), base_t)
    lay_t = jnp.where(north_edge, dot(mirror, lay_t), lay_t)
    sub = lax.broadcasted_iota(jnp.int32, (8, LANES), 0)
    spare_lane = lane_iota((8, LANES)) >= 7 * STRIP
    for whole, side, fields, columns in ((top, top_side, base_t, lay_t), (bottom, bottom_side, base_b, lay_b)):
        whole[:, :LANES] = fields
        whole[:, LANES:] = columns
        for k, rows8, first_row in ((0, slice(8, 16), 1), (1, slice(0, 8), 0)):
            h8, v8, u8 = (
                rolled(rolled(columns[rows8], 7 * STRIP - row * layers, 1), first_row + j, 0)
                for j, row in enumerate((0, 2, 4))
            )
            spares = jnp.where(sub == 0, h8, jnp.where(sub == 1, v8, u8))
            side[k] = jnp.where(spare_lane, spares, fields[rows8])

    def strips(whole, side, into, into_side, k, own, to_west_slot, to_east_slot, merid):
        return [
            copy(whole, into, k, own, merid),
            copy(side.at[0], into_side.at[0], k + 1, to_west_slot, merid),
            copy(side.at[1], into_side.at[1], k + 2, to_east_slot, merid),
        ]

    far_targets = (far[0], far[2], far[1])
    far_copies = strips(top, top_side, north_ref, north_side, 4, *far_targets, c)
    up_copies = strips(top, top_side, south_ref, south_side, 7, z, e, w, other)
    down_copies = strips(bottom, bottom_side, north_ref, north_side, 10, z, e, w, other)

    @pl.when(c == 0)
    def _():
        up_copies[0].start()
        up_copies[1].start()

    @pl.when(c == 1)
    def _():
        down_copies[0].start()
        down_copies[1].start()

    def send_far():
        @pl.when(c == 0)
        def _():
            pl.semaphore_wait(barrier, 3)
            pl.semaphore_signal(
                far_ok, inc=1, device_id={"zonal": z, "merid": other}, device_id_type=MESH
            )

        @pl.when(c == 1)
        def _():
            pl.semaphore_wait(far_ok, 1)
            for target, cp in zip(far_targets, far_copies):
                @pl.when(target != z)
                def _(cp=cp):
                    cp.start()

    late = 2 * z >= devices

    @pl.when(late)
    def _():
        send_far()

    last = cells - 1
    h_last = lay[H, :, last, :rows]
    v_last = lay[V, :, last, :rows]
    flux_in = lay[U, :, last - 1, :rows] * (0.5 * (lay[H, :, last - 1, :rows] + h_last))
    inside = lane_iota((layers, rows)) < rows - 1
    along = jnp.where(inside, v_last * (0.5 * (h_last + rolled(h_last, -1, 1))), 0.0)
    for k, x in enumerate((h_last, lay[U, :, last, :rows], flux_in - (along - rolled(along, 1, 1)))):
        goeast[k * layers: (k + 1) * layers] = x
    ends = v_last[:, rows - LANES:]
    spare = 48 - 3 * layers
    for k in range(0, layers, spare):
        part = ends[k: k + spare]
        at = k // spare * LANES
        goeast[3 * layers: 3 * layers + part.shape[0], at: at + LANES] = part
    h_first = lay[H, :, 0, :rows]
    flux_out = lay[U, :, 0, :rows] * (0.5 * (h_first + lay[H, :, 1, :rows]))
    for k, x in enumerate((h_first, flux_out, lay[V, :, 0, :rows])):
        gowest[k * layers: (k + 1) * layers] = x

    column_copies[0].start()

    pl.semaphore_wait(west_ok, 1)
    state_copies[1].start()
    side_copies[1].start()

    @pl.when(c == 0)
    def _():
        up_copies[2].start()

    @pl.when(c == 1)
    def _():
        down_copies[2].start()

    @pl.when(jnp.logical_not(late))
    def _():
        send_far()

    column_copies[1].start()

    @pl.when(c == 0)
    def _():
        south_ref[...] = jnp.zeros_like(south_ref)
        south_side[...] = jnp.zeros_like(south_side)

    for target, dst, src in (
        (far_targets[0], north_ref, top),
        (far_targets[1], north_side.at[0], top_side.at[0]),
        (far_targets[2], north_side.at[1], top_side.at[1]),
    ):
        @pl.when(jnp.logical_and(c == 1, target == z))
        def _(dst=dst, src=src):
            dst[...] = src[...]

    for kind in (H, U, V):
        for l in range(layers):
            lay[kind, l, cells:, :rows] = jnp.zeros((8, rows), F32)

    for cp in state_copies + side_copies:
        cp.wait()

    @pl.when(c == 0)
    def _():
        for cp in up_copies:
            cp.wait_send()
        for cp in down_copies:
            cp.wait_recv()

    @pl.when(c == 1)
    def _():
        for cp in down_copies:
            cp.wait_send()
        for cp in up_copies:
            cp.wait_recv()

    for target, cp in zip(far_targets, far_copies):
        @pl.when(jnp.logical_and(c == 1, target != z))
        def _(cp=cp):
            cp.wait()

    first8 = lane_iota((8, LANES)) < LANES // 2
    far_rows = lax.broadcasted_iota(jnp.int32, (8, LANES), 0) < 4
    norths = [north_ref[:, :LANES], north_side[1], north_side[0]]
    souths = [south_ref[:, :LANES], south_side[1], south_side[0]]

    def ring(x):
        return (x[OWN][:8], x[OWN][8:], x[EAST], x[WEST])

    for k, (n, s) in enumerate(zip(ring(norths), ring(souths))):
        for f in range(7):
            base[f, 8 * k: 8 * k + 8, rows:] = jnp.where(
                first8, rolled(n, -STRIP * f, 1), rolled(s, LANES - STRIP - STRIP * f, 1)
            )
    at_east, at_west, at_south, at_north = neighbours(rows)
    near = lax.broadcasted_iota(jnp.int32, (8, wide), 0) < 4

    def trimmed(x):
        return jnp.concatenate([x[:cells], jnp.where(near, x[cells: cells + 8], x[cells + 8:])], 0)

    def move(first=False):
        bu = base[5]
        bv = base[6]
        eta = base[4] - (bu - at_west(bu) + bv - at_south(bv))
        base[4] = eta
        au = base[0]
        bu = bu - au * (at_east(eta) - eta) + base[2]
        if first:
            bu = jnp.where(au != 0.0, bu, 0.0)
        base[5] = bu
        av = base[1]
        bv = bv - av * (at_north(eta) - eta) + base[3]
        if first:
            bv = jnp.where(av != 0.0, bv, 0.0)
        base[6] = bv
        return bu, bv

    def substep(_, sums):
        bu, bv = move()
        return sums[0] + trimmed(bu), sums[1] + trimmed(bv)

    def substep_own():
        bu, bv = move()
        return bu[:cells, :rows], bv[:cells, :rows]

    first_u, first_v = move(first=True)
    mean_u, mean_v = lax.fori_loop(1, NSUB, substep, (trimmed(first_u), trimmed(first_v)))
    for cp in second_copies[:2]:
        cp.start()
    for k in range(2):
        packed = jnp.zeros((8, LANES), F32)
        for j in range(3):
            strip = rolled(base[4 + j, 8 * k: 8 * k + 8, rows:], STRIP + 2 * STRIP * j, 1)
            packed = jnp.where(lane_iota((8, LANES)) // (2 * STRIP) == j, strip, packed)
        late_strips[k] = packed
    for cp in second_copies[2:]:
        cp.start()
    depth[2] = mean_u * (1.0 / NSUB)
    depth[3] = mean_v * (1.0 / NSUB)

    lane8 = lane_iota((8, LANES))

    def around(own, sides):
        def unpacked(x, row):
            h8, v8, u8 = (
                rolled(rolled(x, r * layers - 7 * STRIP, 1), row - j, 0) for j, r in enumerate((0, 2, 4))
            )
            return jnp.where(lane8 < layers, h8, jnp.where(lane8 < 4 * layers, v8, u8))

        halo = jnp.where(far_rows, unpacked(sides[1], 0), unpacked(sides[0], 7))
        return jnp.concatenate([own[:, LANES:], halo], 0)

    north = around(north_ref, north_side)
    south = around(south_ref, south_side)
    lane24 = lane_iota(north.shape)
    first24 = lane24 < LANES // 2
    for kind, row, deep_row in ((H, 0, True), (U, 4, False), (V, 2, True)):
        for l in range(layers):
            spot = row * layers + l
            n = rolled(north, -spot, 1)
            s = rolled(south, LANES - 1 - spot, 1)
            if deep_row:
                n = jnp.where(lane24 == 0, n, rolled(north, 1 - spot - layers, 1))
                s = jnp.where(lane24 == LANES - 1, s, rolled(south, LANES - 2 - spot - layers, 1))
            lay[kind, l, :, rows:] = jnp.where(first24, n, s)
    press = total = deep = jnp.zeros((cells, wide), F32)
    for l in range(layers):
        h = lay[H, l, :cells]
        v = lay[V, l, :cells]
        diff = at_north(h) - h
        press = press + diff
        half = h + 0.5 * diff
        flux = v * half
        leaving[l] = flux - at_south(flux)
        vt = v - PRESS_COEF * press
        trial_v[l] = vt
        total = total + half * vt
        deep = deep + half
    depth[1, :cells] = deep
    fix = (depth[3, :cells] - total) / deep
    open_face = base[1, :cells] != 0.0
    for l in range(layers):
        lay[V, l, :cells] = jnp.where(open_face, trial_v[l] + fix, 0.0)
    for cp in column_copies:
        cp.wait()
    end_lane = lane_iota((1, LANES)) == LANES - 1
    for l in range(layers):
        def column(ref, k):
            return ref[k * layers + l: k * layers + l + 1, :]

        lay[H, l, cells: cells + 1, :rows] = column(least, 0)
        lay[H, l, cells + 1: cells + 2, :rows] = 2.0 - column(least, 0)
        lay[U, l, cells: cells + 1, :rows] = column(least, 1)
        lay[V, l, cells: cells + 1, :rows] = column(least, 2)
        lay[H, l, ext - 1: ext, :rows] = column(lwest, 0)
        lay[H, l, ext - 2: ext - 1, :rows] = 2.0 - column(lwest, 0)
        lay[U, l, ext - 1: ext, :rows] = column(lwest, 1)
        lay[U, l, ext - 2: ext - 1, :rows] = column(lwest, 2)
        at = l // spare * LANES
        lay[V, l, ext - 1: ext, rows - LANES: rows] = jnp.where(
            end_lane, lwest[3 * layers + l % spare: 3 * layers + l % spare + 1, at: at + LANES], 0.0
        )
    press = total = deep = jnp.zeros((ext, wide), F32)
    for l in range(layers):
        h = lay[H, l]
        u = lay[U, l]
        diff = at_east(h) - h
        press = press + diff
        half = h + 0.5 * diff
        flux = u * half
        side_h = h[cells:]
        side_flux = lay[V, l, cells:] * (side_h + 0.5 * (at_north(side_h) - side_h))
        out_v = jnp.concatenate([leaving[l], side_flux - at_south(side_flux)], 0)
        lay[H, l] = h - FLUX_STEP * (flux - at_west(flux) + out_v)
        ut = u - PRESS_COEF * press
        trial_u[l] = ut[:, :rows]
        total = total + half * ut
        deep = deep + half
    depth[0] = deep
    fix = ((depth[2] - total) / deep)[:, :rows]
    open_face = trimmed(base[0])[:, :rows] != 0.0
    for l in range(layers):
        lay[U, l, :, :rows] = jnp.where(open_face, trial_u[l] + fix, 0.0)
    press_u = press_v = total_u = total_v = jnp.zeros((cells, rows), F32)
    for l in range(layers):
        h_u = lay[H, l, :, :rows]
        h_v = lay[H, l, :cells]
        diff_u = rolled(h_u, -1, 0) - h_u
        diff_v = rolled(h_v, -1, 1) - h_v
        hu = h_u + 0.5 * diff_u
        hv = h_v + 0.5 * diff_v
        u = lay[U, l, :, :rows]
        v = lay[V, l, :cells]
        flux_u = u * hu
        flux_v = v * hv
        out_u = (flux_u - rolled(flux_u, 1, 0))[:cells]
        out_v = (flux_v - rolled(flux_v, 1, 1))[:, :rows]
        h_new[l] = h_u[:cells] - FLUX_STEP * (out_u + out_v)
        press_u = press_u + diff_u[:cells]
        press_v = press_v + diff_v[:, :rows]
        ut = u[:cells] - PRESS_COEF * press_u
        vt = v[:, :rows] - PRESS_COEF * press_v
        trial[0, l] = ut
        trial[1, l] = vt
        total_u = total_u + hu[:cells] * ut
        total_v = total_v + hv[:, :rows] * vt
    fixes[0] = total_u
    fixes[1] = total_v
    for cp in second_copies:
        cp.wait()
    base[4:7, cells: cells + 8, :rows] = late_east[...]
    base[4:7, cells + 8:, :rows] = late_west[...]
    for j in range(3):
        base[4 + j, cells: cells + 8, rows:] = rolled(strips_east[...], -STRIP - 2 * STRIP * j, 1)
        base[4 + j, cells + 8:, rows:] = rolled(strips_west[...], -STRIP - 2 * STRIP * j, 1)

    def last_substep(k, sums):
        sum_u, sum_v = substep_own()
        return sums[0] + sum_u, sums[1] + sum_v

    own = jnp.zeros((cells, rows), F32)
    sum_u, sum_v = lax.fori_loop(0, NSUB, last_substep, (own, own))
    for k, total in ((0, sum_u), (1, sum_v)):
        fixes[k] = (total * (1.0 / NSUB) - fixes[k]) / depth[k, :cells, :rows]
        faces_out[k] = base[k, :cells, :rows]
    for k in range(3):
        state_out[k] = base[4 + k, :cells, :rows]


def finish(
    h_new, trial, fixes, faces, state, eta_out, bu_out, bv_out, h_out, u_out, v_out, results, done,
):
    layers = h_out.shape[0]
    stores = [
        pltpu.make_async_copy(src, out, done.at[k])
        for k, (src, out) in enumerate((
            (h_new, h_out),
            (state.at[0], eta_out),
            (state.at[1], bu_out),
            (state.at[2], bv_out),
        ))
    ]
    half = layers // 2
    parts = (pl.ds(0, half), pl.ds(half, layers - half))
    stores += [
        pltpu.make_async_copy(results.at[k, part], out.at[part], done.at[4 + 2 * k + j])
        for k, out in enumerate((u_out, v_out))
        for j, part in enumerate(parts)
    ]
    for cp in stores[:4]:
        cp.start()
    for k in range(2):
        open_face = faces[k] != 0.0
        fix = fixes[k]
        for l in range(layers):
            results[k, l] = jnp.where(open_face, trial[k, l] + fix, 0.0)
            if l == half - 1:
                stores[4 + 2 * k].start()
        stores[5 + 2 * k].start()
    for cp in stores:
        cp.wait()


def body(
    devices, height, transport_u, transport_v, thickness, velocity_u, velocity_v,
    sea_faces, wind_seeds, wind_scale, wind_base,
):
    layers, cells, rows = thickness.shape
    wide = rows + LANES
    ext = cells + 8
    anywhere = pl.BlockSpec(memory_space=pl.ANY)
    vmem = pl.BlockSpec(memory_space=pltpu.VMEM)

    def shape(*dims):
        return jax.ShapeDtypeStruct(dims, F32)

    def inner(*dims):
        return pltpu.VMEM(dims, F32)

    mid = pl.pallas_call(
        functools.partial(exchange, devices),
        out_shape=[
            inner(layers, cells, rows), inner(2, layers, cells, rows), inner(2, cells, rows),
            inner(2, cells, rows), inner(3, cells, rows),
        ],
        in_specs=[anywhere] * 10,
        out_specs=[vmem] * 5,
        scratch_shapes=[
            inner(7, cells + 16, wide),
            inner(3, layers, ext, wide),
            inner(layers, ext, rows),
            inner(layers, cells, wide),
            inner(layers, cells, wide),
            inner(4, ext, wide),
            pltpu.VMEM(sea_faces.shape, sea_faces.dtype),
            inner(*wind_base.shape),
            pltpu.SMEM(wind_seeds.shape[::-1], wind_seeds.dtype),
            pltpu.SMEM(wind_scale.shape, F32),
            inner(48, rows), inner(3 * layers, rows), inner(3 * layers, rows), inner(48, rows),
            inner(3, 8, rows), inner(3, 8, rows), inner(2, 8, LANES), inner(8, LANES), inner(8, LANES),
            inner(cells, 2 * LANES), inner(cells, 2 * LANES), inner(2, 8, LANES), inner(2, 8, LANES),
            inner(cells, 2 * LANES), inner(cells, 2 * LANES), inner(2, 8, LANES), inner(2, 8, LANES),
            pltpu.SemaphoreType.DMA((10,)),
            pltpu.SemaphoreType.DMA((19,)),
            pltpu.SemaphoreType.DMA((19,)),
            pltpu.SemaphoreType.REGULAR,
            pltpu.SemaphoreType.REGULAR,
            pltpu.SemaphoreType.REGULAR,
        ],
        compiler_params=pltpu.CompilerParams(collective_id=0, has_side_effects=True),
        name="exchange",
    )(
        height, transport_u, transport_v, thickness, velocity_u, velocity_v,
        sea_faces, wind_base, wind_seeds.T, wind_scale,
    )
    return pl.pallas_call(
        finish,
        out_shape=[shape(cells, rows)] * 3 + [shape(layers, cells, rows)] * 3,
        in_specs=[vmem] * 5,
        out_specs=[anywhere] * 6,
        scratch_shapes=[inner(2, layers, cells, rows), pltpu.SemaphoreType.DMA((8,))],
        name="finish",
    )(*[pltpu.with_memory_space_constraint(x, pltpu.VMEM) for x in mid])


def solution(mesh):
    flat = P(("members", "zonal"), "merid")
    deep = P(None, ("members", "zonal"), "merid")
    fixed = P(None, "zonal", "merid")
    return jax.shard_map(
        functools.partial(body, mesh.shape["zonal"]),
        mesh=mesh,
        in_specs=(flat, flat, flat, deep, deep, deep, fixed, P("members", None), P("members"), fixed),
        out_specs=(flat, flat, flat, deep, deep, deep),
        check_vma=False,
    )
```

```python
import functools
import math

import jax
import jax.numpy as jnp
from jax import lax
from jax.experimental import pallas as pl
from jax.experimental.pallas import tpu as pltpu
from jax.sharding import PartitionSpec as P

NSUB = 6
STEPS = 2
WAVE_LIMIT = 0.225
STRESS_SCALE = 0.1
FLUX_STEP = 0.05
PRESS_COEF = 0.05

MESH = pl.DeviceIdType.MESH
F32 = jnp.float32
OWN, EAST, WEST = 0, 1, 2
LANES = 128
STRIP = 16


def lane_iota(shape):
    return lax.broadcasted_iota(jnp.int32, shape, len(shape) - 1)


def modulo(value, size):
    return value & (size - 1) if size & (size - 1) == 0 else lax.rem(value, size)


def rolled(x, shift, axis):
    shift = shift % x.shape[axis]
    return pltpu.roll(x, shift, axis) if shift else x


def neighbours(rows):
    fold1 = jnp.logical_and(lane_iota((8, LANES)) < LANES // 2, lax.axis_index("merid") == 1)

    def merge(main, alt):
        fold = jnp.concatenate([fold1] * (alt.shape[0] // 8), 0)
        halo = jnp.where(fold, alt, main[:, rows:])
        return jnp.concatenate([main[:, :rows], halo], 1)

    def at_west(x):
        return merge(rolled(x, 1, 0), rolled(x[:, rows:], -1, 0))

    def at_east(x):
        return merge(rolled(x, -1, 0), rolled(x[:, rows:], 1, 0))

    def at_south(x):
        return merge(rolled(x, 1, 1), rolled(x[:, rows:], -1, 1))

    def at_north(x):
        return merge(rolled(x, -1, 1), rolled(x[:, rows - LANES:], 1, 1)[:, LANES:])

    return at_east, at_west, at_south, at_north


def exchange(
    devices,
    eta_ref, bu_ref, bv_ref, h_ref, u_ref, v_ref, faces_ref, base_ref, seeds_ref, scale_ref,
    h_new, trial, fixes, faces_out, state_out,
    base, lay, trial_u, trial_v, leaving, depth, faces, winds, seeds, scale, goeast, gowest, least, lwest, late_east, late_west, late_strips, strips_east, strips_west,
    top, bottom, top_side, bottom_side, north_ref, south_ref, north_side, south_side,
    load, send, recv, near_ok, west_ok, far_ok,
):
    z = lax.axis_index("zonal")
    c = lax.axis_index("merid")
    e = lax.rem(z + 1, devices)
    w = lax.rem(z + devices - 1, devices)
    other = 1 - c
    far = [lax.rem(2 * devices - 1 - z + d, devices) for d in (0, -1, 1)]
    layers, cells, rows = h_ref.shape
    wide = rows + LANES
    ext = cells + 8
    H, U, V = 0, 1, 2

    fetches = [
        pltpu.make_async_copy(src, dst, load.at[k])
        for k, (src, dst) in enumerate((
            (eta_ref, base.at[4, pl.ds(0, cells), pl.ds(0, rows)]),
            (bu_ref, base.at[5, pl.ds(0, cells), pl.ds(0, rows)]),
            (bv_ref, base.at[6, pl.ds(0, cells), pl.ds(0, rows)]),
            (seeds_ref, seeds),
            (scale_ref, scale),
            (faces_ref, faces),
            (base_ref, winds),
            (h_ref, lay.at[H, :, pl.ds(0, cells), pl.ds(0, rows)]),
            (u_ref, lay.at[U, :, pl.ds(0, cells), pl.ds(0, rows)]),
            (v_ref, lay.at[V, :, pl.ds(0, cells), pl.ds(0, rows)]),
        ))
    ]
    for cp in fetches:
        cp.start()
    barrier = pltpu.get_barrier_semaphore()

    def greet(zonal, merid):
        pl.semaphore_signal(
            barrier, inc=1, device_id={"zonal": zonal, "merid": merid}, device_id_type=MESH
        )

    greet(w, 1)

    @pl.when(c == 0)
    def _():
        greet(z, 1)

    @pl.when(c == 1)
    def _():
        for target in far:
            greet(target, 0)

    def copy(src, dst, k, zonal, merid):
        return pltpu.make_async_remote_copy(
            src_ref=src, dst_ref=dst, send_sem=send.at[k], recv_sem=recv.at[k],
            device_id={"zonal": zonal, "merid": merid}, device_id_type=MESH,
        )

    lanes = pl.ds(0, rows)

    def to_sides(fields, k):
        return [
            copy(base.at[fields, pl.ds(8, 8), lanes], base.at[fields, pl.ds(24, 8), lanes], k, e, c),
            copy(base.at[fields, pl.ds(0, 8), lanes], base.at[fields, pl.ds(16, 8), lanes], k + 1, w, c),
        ]

    state_copies = to_sides(pl.ds(4, 3), 15)
    side_copies = to_sides(pl.ds(0, 4), 0)
    second_copies = [
        copy(base.at[pl.ds(4, 3), pl.ds(8, 8), lanes], late_west, 2, e, c),
        copy(base.at[pl.ds(4, 3), pl.ds(0, 8), lanes], late_east, 3, w, c),
        copy(late_strips.at[1], strips_west, 17, e, c),
        copy(late_strips.at[0], strips_east, 18, w, c),
    ]
    column_copies = [
        copy(goeast, lwest, 13, e, c),
        copy(gowest, least, 14, w, c),
    ]

    def tell(semaphore, zonal, merid):
        pl.semaphore_signal(
            semaphore, inc=1, device_id={"zonal": zonal, "merid": merid}, device_id_type=MESH
        )

    @pl.when(c == 1)
    def _():
        pl.semaphore_wait(barrier, 3)
        tell(near_ok, z, other)
        tell(west_ok, e, 1)
        tell(west_ok, e, 0)

    @pl.when(c == 0)
    def _():
        pl.semaphore_wait(near_ok, 1)

    for cp in fetches[:3]:
        cp.wait()
    state_copies[0].start()
    for cp in fetches[3:7]:
        cp.wait()
    total_x = cells * devices
    total_y = rows * 2
    cols = lax.broadcasted_iota(jnp.int32, (cells, LANES), 0) + z * cells
    rws = lax.broadcasted_iota(jnp.int32, (8, rows), 1) + c * rows
    sum_cos = jnp.zeros((cells, rows), F32)
    sum_sin = jnp.zeros((cells, rows), F32)
    for m in range(seeds.shape[1]):
        ax = (2.0 * math.pi / total_x) * modulo(seeds[0, m] * cols, total_x).astype(F32)
        ay = (2.0 * math.pi / total_y) * modulo(seeds[1, m] * rws, total_y).astype(F32)
        amp = scale[m]
        cx = jnp.concatenate([amp * jnp.cos(ax)] * (rows // LANES), 1)
        sx = jnp.concatenate([amp * jnp.sin(ax)] * (rows // LANES), 1)
        cy = jnp.concatenate([jnp.cos(ay)] * (cells // 8), 0)
        sy = jnp.concatenate([jnp.sin(ay)] * (cells // 8), 0)
        sum_cos = sum_cos + (cx * cy - sx * sy)
        sum_sin = sum_sin + (sx * cy + cx * sy)
    mask_u = faces[0].astype(F32)
    mask_v = faces[1].astype(F32)
    base[2, :cells, :rows] = mask_u * (STRESS_SCALE * (winds[0] + sum_cos))
    base[3, :cells, :rows] = mask_v * (STRESS_SCALE * (winds[1] + sum_sin))
    fetches[7].wait()
    h_sum = lay[H, 0, :cells, :rows]
    for l in range(1, layers):
        h_sum = h_sum + lay[H, l, :cells, :rows]
    wave = (WAVE_LIMIT / layers) * h_sum
    base[0, :cells, :rows] = mask_u * wave
    base[1, :cells, :rows] = mask_v * wave
    for cp in fetches[8:]:
        cp.wait()
    side_copies[0].start()
    strip_rows = ((H, 0), (H, 1), (V, 0), (V, 1), (U, 0))
    lane = lane_iota((cells, LANES))
    hi = rows - LANES
    base_t = jnp.zeros((cells, LANES), F32)
    base_b = jnp.zeros((cells, LANES), F32)
    for f in range(7):
        here = lane // STRIP == f
        base_t = jnp.where(here, rolled(base[f, :cells, hi:rows], f * STRIP + STRIP, 1), base_t)
        base_b = jnp.where(here, rolled(base[f, :cells, :LANES], f * STRIP, 1), base_b)
    lay_t = jnp.zeros((cells, LANES), F32)
    lay_b = jnp.zeros((cells, LANES), F32)
    for row, (kind, depth_in) in enumerate(strip_rows):
        for l in range(layers):
            spot = row * layers + l
            here = lane == spot
            lay_t = jnp.where(here, rolled(lay[kind, l, :cells, hi:rows], spot + 1 + depth_in, 1), lay_t)
            lay_b = jnp.where(here, rolled(lay[kind, l, :cells, :LANES], spot - depth_in, 1), lay_b)
    r2 = lax.broadcasted_iota(jnp.int32, (LANES, LANES), 0)
    c2 = lax.broadcasted_iota(jnp.int32, (LANES, LANES), 1)
    perm_b = jnp.where(r2 == (c2 ^ (STRIP - 1)), 1.0, 0.0).astype(F32)
    r1 = lax.broadcasted_iota(jnp.int32, (cells, cells), 0)
    c1 = lax.broadcasted_iota(jnp.int32, (cells, cells), 1)
    mirror = jnp.where(r1 + c1 == cells - 1, 1.0, 0.0).astype(F32)
    dot = functools.partial(
        jnp.dot, preferred_element_type=F32, precision=lax.Precision.HIGHEST
    )
    north_edge = c == 1
    base_t = jnp.where(north_edge, dot(mirror, dot(base_t, perm_b)), base_t)
    lay_t = jnp.where(north_edge, dot(mirror, lay_t), lay_t)
    sub = lax.broadcasted_iota(jnp.int32, (8, LANES), 0)
    spare_lane = lane_iota((8, LANES)) >= 7 * STRIP
    for whole, side, fields, columns in ((top, top_side, base_t, lay_t), (bottom, bottom_side, base_b, lay_b)):
        whole[:, :LANES] = fields
        whole[:, LANES:] = columns
        for k, rows8, first_row in ((0, slice(8, 16), 1), (1, slice(0, 8), 0)):
            h8, v8, u8 = (
                rolled(rolled(columns[rows8], 7 * STRIP - row * layers, 1), first_row + j, 0)
                for j, row in enumerate((0, 2, 4))
            )
            spares = jnp.where(sub == 0, h8, jnp.where(sub == 1, v8, u8))
            side[k] = jnp.where(spare_lane, spares, fields[rows8])

    def strips(whole, side, into, into_side, k, own, to_west_slot, to_east_slot, merid):
        return [
            copy(whole, into, k, own, merid),
            copy(side.at[0], into_side.at[0], k + 1, to_west_slot, merid),
            copy(side.at[1], into_side.at[1], k + 2, to_east_slot, merid),
        ]

    far_targets = (far[0], far[2], far[1])
    far_copies = strips(top, top_side, north_ref, north_side, 4, *far_targets, c)
    up_copies = strips(top, top_side, south_ref, south_side, 7, z, e, w, other)
    down_copies = strips(bottom, bottom_side, north_ref, north_side, 10, z, e, w, other)

    @pl.when(c == 0)
    def _():
        up_copies[0].start()
        up_copies[1].start()

    @pl.when(c == 1)
    def _():
        down_copies[0].start()
        down_copies[1].start()

    def send_far():
        @pl.when(c == 0)
        def _():
            pl.semaphore_wait(barrier, 3)
            pl.semaphore_signal(
                far_ok, inc=1, device_id={"zonal": z, "merid": other}, device_id_type=MESH
            )

        @pl.when(c == 1)
        def _():
            pl.semaphore_wait(far_ok, 1)
            for target, cp in zip(far_targets, far_copies):
                @pl.when(target != z)
                def _(cp=cp):
                    cp.start()

    late = 2 * z >= devices

    @pl.when(late)
    def _():
        send_far()

    last = cells - 1
    h_last = lay[H, :, last, :rows]
    v_last = lay[V, :, last, :rows]
    flux_in = lay[U, :, last - 1, :rows] * (0.5 * (lay[H, :, last - 1, :rows] + h_last))
    inside = lane_iota((layers, rows)) < rows - 1
    along = jnp.where(inside, v_last * (0.5 * (h_last + rolled(h_last, -1, 1))), 0.0)
    for k, x in enumerate((h_last, lay[U, :, last, :rows], flux_in - (along - rolled(along, 1, 1)))):
        goeast[k * layers: (k + 1) * layers] = x
    ends = v_last[:, rows - LANES:]
    spare = 48 - 3 * layers
    for k in range(0, layers, spare):
        part = ends[k: k + spare]
        at = k // spare * LANES
        goeast[3 * layers: 3 * layers + part.shape[0], at: at + LANES] = part
    h_first = lay[H, :, 0, :rows]
    flux_out = lay[U, :, 0, :rows] * (0.5 * (h_first + lay[H, :, 1, :rows]))
    for k, x in enumerate((h_first, flux_out, lay[V, :, 0, :rows])):
        gowest[k * layers: (k + 1) * layers] = x

    column_copies[0].start()

    pl.semaphore_wait(west_ok, 1)
    state_copies[1].start()
    side_copies[1].start()

    @pl.when(c == 0)
    def _():
        up_copies[2].start()

    @pl.when(c == 1)
    def _():
        down_copies[2].start()

    @pl.when(jnp.logical_not(late))
    def _():
        send_far()

    column_copies[1].start()

    @pl.when(c == 0)
    def _():
        south_ref[...] = jnp.zeros_like(south_ref)
        south_side[...] = jnp.zeros_like(south_side)

    for target, dst, src in (
        (far_targets[0], north_ref, top),
        (far_targets[1], north_side.at[0], top_side.at[0]),
        (far_targets[2], north_side.at[1], top_side.at[1]),
    ):
        @pl.when(jnp.logical_and(c == 1, target == z))
        def _(dst=dst, src=src):
            dst[...] = src[...]

    for kind in (H, U, V):
        for l in range(layers):
            lay[kind, l, cells:, :rows] = jnp.zeros((8, rows), F32)

    for cp in state_copies + side_copies:
        cp.wait()

    @pl.when(c == 0)
    def _():
        for cp in up_copies:
            cp.wait_send()
        for cp in down_copies:
            cp.wait_recv()

    @pl.when(c == 1)
    def _():
        for cp in down_copies:
            cp.wait_send()
        for cp in up_copies:
            cp.wait_recv()

    for target, cp in zip(far_targets, far_copies):
        @pl.when(jnp.logical_and(c == 1, target != z))
        def _(cp=cp):
            cp.wait()

    first8 = lane_iota((8, LANES)) < LANES // 2
    far_rows = lax.broadcasted_iota(jnp.int32, (8, LANES), 0) < 4
    norths = [north_ref[:, :LANES], north_side[1], north_side[0]]
    souths = [south_ref[:, :LANES], south_side[1], south_side[0]]

    def ring(x):
        return (x[OWN][:8], x[OWN][8:], x[EAST], x[WEST])

    for k, (n, s) in enumerate(zip(ring(norths), ring(souths))):
        for f in range(7):
            base[f, 8 * k: 8 * k + 8, rows:] = jnp.where(
                first8, rolled(n, -STRIP * f, 1), rolled(s, LANES - STRIP - STRIP * f, 1)
            )
    at_east, at_west, at_south, at_north = neighbours(rows)
    near = lax.broadcasted_iota(jnp.int32, (8, wide), 0) < 4

    def trimmed(x):
        return jnp.concatenate([x[:cells], jnp.where(near, x[cells: cells + 8], x[cells + 8:])], 0)

    def move(first=False):
        bu = base[5]
        bv = base[6]
        eta = base[4] - (bu - at_west(bu) + bv - at_south(bv))
        base[4] = eta
        au = base[0]
        bu = bu - au * (at_east(eta) - eta) + base[2]
        if first:
            bu = jnp.where(au != 0.0, bu, 0.0)
        base[5] = bu
        av = base[1]
        bv = bv - av * (at_north(eta) - eta) + base[3]
        if first:
            bv = jnp.where(av != 0.0, bv, 0.0)
        base[6] = bv
        return bu, bv

    def substep(_, sums):
        bu, bv = move()
        return sums[0] + trimmed(bu), sums[1] + trimmed(bv)

    def substep_own():
        bu, bv = move()
        return bu[:cells, :rows], bv[:cells, :rows]

    first_u, first_v = move(first=True)
    mean_u, mean_v = lax.fori_loop(1, NSUB, substep, (trimmed(first_u), trimmed(first_v)))
    for cp in second_copies[:2]:
        cp.start()
    for k in range(2):
        packed = jnp.zeros((8, LANES), F32)
        for j in range(3):
            strip = rolled(base[4 + j, 8 * k: 8 * k + 8, rows:], STRIP + 2 * STRIP * j, 1)
            packed = jnp.where(lane_iota((8, LANES)) // (2 * STRIP) == j, strip, packed)
        late_strips[k] = packed
    for cp in second_copies[2:]:
        cp.start()
    depth[2] = mean_u * (1.0 / NSUB)
    depth[3] = mean_v * (1.0 / NSUB)

    lane8 = lane_iota((8, LANES))

    def around(own, sides):
        def unpacked(x, row):
            h8, v8, u8 = (
                rolled(rolled(x, r * layers - 7 * STRIP, 1), row - j, 0) for j, r in enumerate((0, 2, 4))
            )
            return jnp.where(lane8 < layers, h8, jnp.where(lane8 < 4 * layers, v8, u8))

        halo = jnp.where(far_rows, unpacked(sides[1], 0), unpacked(sides[0], 7))
        return jnp.concatenate([own[:, LANES:], halo], 0)

    north = around(north_ref, north_side)
    south = around(south_ref, south_side)
    lane24 = lane_iota(north.shape)
    first24 = lane24 < LANES // 2
    for kind, row, deep_row in ((H, 0, True), (U, 4, False), (V, 2, True)):
        for l in range(layers):
            spot = row * layers + l
            n = rolled(north, -spot, 1)
            s = rolled(south, LANES - 1 - spot, 1)
            if deep_row:
                n = jnp.where(lane24 == 0, n, rolled(north, 1 - spot - layers, 1))
                s = jnp.where(lane24 == LANES - 1, s, rolled(south, LANES - 2 - spot - layers, 1))
            lay[kind, l, :, rows:] = jnp.where(first24, n, s)
    column_copies[1].wait_recv()
    for l in range(layers):
        def column(ref, k):
            return ref[k * layers + l: k * layers + l + 1, :]

        lay[H, l, cells: cells + 1, :rows] = column(least, 0)
        lay[H, l, cells + 1: cells + 2, :rows] = 2.0 - column(least, 0)
        lay[U, l, cells: cells + 1, :rows] = column(least, 1)
        lay[V, l, cells: cells + 1, :rows] = column(least, 2)

    press = total = deep = jnp.zeros((cells, wide), F32)
    for l in range(layers):
        h = lay[H, l, :cells]
        v = lay[V, l, :cells]
        diff = at_north(h) - h
        press = press + diff
        half = h + 0.5 * diff
        flux = v * half
        leaving[l] = flux - at_south(flux)
        vt = v - PRESS_COEF * press
        trial_v[l] = vt
        total = total + half * vt
        deep = deep + half
    depth[1, :cells] = deep
    fix = (depth[3, :cells] - total) / deep
    open_face = base[1, :cells] != 0.0
    for l in range(layers):
        lay[V, l, :cells] = jnp.where(open_face, trial_v[l] + fix, 0.0)
    for cp in column_copies:
        cp.wait_send()
    column_copies[0].wait_recv()
    end_lane = lane_iota((1, LANES)) == LANES - 1
    for l in range(layers):
        def column(ref, k):
            return ref[k * layers + l: k * layers + l + 1, :]

        lay[H, l, ext - 1: ext, :rows] = column(lwest, 0)
        lay[H, l, ext - 2: ext - 1, :rows] = 2.0 - column(lwest, 0)
        lay[U, l, ext - 1: ext, :rows] = column(lwest, 1)
        lay[U, l, ext - 2: ext - 1, :rows] = column(lwest, 2)
        at = l // spare * LANES
        lay[V, l, ext - 1: ext, rows - LANES: rows] = jnp.where(
            end_lane, lwest[3 * layers + l % spare: 3 * layers + l % spare + 1, at: at + LANES], 0.0
        )
    press = total = deep = jnp.zeros((ext, wide), F32)
    for l in range(layers):
        h = lay[H, l]
        u = lay[U, l]
        diff = at_east(h) - h
        press = press + diff
        half = h + 0.5 * diff
        flux = u * half
        side_h = h[cells:]
        side_flux = lay[V, l, cells:] * (side_h + 0.5 * (at_north(side_h) - side_h))
        out_v = jnp.concatenate([leaving[l], side_flux - at_south(side_flux)], 0)
        lay[H, l] = h - FLUX_STEP * (flux - at_west(flux) + out_v)
        ut = u - PRESS_COEF * press
        trial_u[l] = ut[:, :rows]
        total = total + half * ut
        deep = deep + half
    depth[0] = deep
    fix = ((depth[2] - total) / deep)[:, :rows]
    open_face = trimmed(base[0])[:, :rows] != 0.0
    for l in range(layers):
        lay[U, l, :, :rows] = jnp.where(open_face, trial_u[l] + fix, 0.0)
    press_u = press_v = total_u = total_v = jnp.zeros((cells, rows), F32)
    for l in range(layers):
        h_u = lay[H, l, :, :rows]
        h_v = lay[H, l, :cells]
        diff_u = rolled(h_u, -1, 0) - h_u
        diff_v = rolled(h_v, -1, 1) - h_v
        hu = h_u + 0.5 * diff_u
        hv = h_v + 0.5 * diff_v
        u = lay[U, l, :, :rows]
        v = lay[V, l, :cells]
        flux_u = u * hu
        flux_v = v * hv
        out_u = (flux_u - rolled(flux_u, 1, 0))[:cells]
        out_v = (flux_v - rolled(flux_v, 1, 1))[:, :rows]
        h_new[l] = h_u[:cells] - FLUX_STEP * (out_u + out_v)
        press_u = press_u + diff_u[:cells]
        press_v = press_v + diff_v[:, :rows]
        ut = u[:cells] - PRESS_COEF * press_u
        vt = v[:, :rows] - PRESS_COEF * press_v
        trial[0, l] = ut
        trial[1, l] = vt
        total_u = total_u + hu[:cells] * ut
        total_v = total_v + hv[:, :rows] * vt
    fixes[0] = total_u
    fixes[1] = total_v
    for cp in second_copies:
        cp.wait()
    base[4:7, cells: cells + 8, :rows] = late_east[...]
    base[4:7, cells + 8:, :rows] = late_west[...]
    for j in range(3):
        base[4 + j, cells: cells + 8, rows:] = rolled(strips_east[...], -STRIP - 2 * STRIP * j, 1)
        base[4 + j, cells + 8:, rows:] = rolled(strips_west[...], -STRIP - 2 * STRIP * j, 1)

    def last_substep(k, sums):
        sum_u, sum_v = substep_own()
        return sums[0] + sum_u, sums[1] + sum_v

    own = jnp.zeros((cells, rows), F32)
    sum_u, sum_v = lax.fori_loop(0, NSUB, last_substep, (own, own))
    for k, total in ((0, sum_u), (1, sum_v)):
        fixes[k] = (total * (1.0 / NSUB) - fixes[k]) / depth[k, :cells, :rows]
        faces_out[k] = base[k, :cells, :rows]
    for k in range(3):
        state_out[k] = base[4 + k, :cells, :rows]


def finish(
    h_new, trial, fixes, faces, state, eta_out, bu_out, bv_out, h_out, u_out, v_out, results, done,
):
    layers = h_out.shape[0]
    stores = [
        pltpu.make_async_copy(src, out, done.at[k])
        for k, (src, out) in enumerate((
            (h_new, h_out),
            (state.at[0], eta_out),
            (state.at[1], bu_out),
            (state.at[2], bv_out),
        ))
    ]
    half = layers // 2
    parts = (pl.ds(0, half), pl.ds(half, layers - half))
    stores += [
        pltpu.make_async_copy(results.at[k, part], out.at[part], done.at[4 + 2 * k + j])
        for k, out in enumerate((u_out, v_out))
        for j, part in enumerate(parts)
    ]
    for cp in stores[:4]:
        cp.start()
    for k in range(2):
        open_face = faces[k] != 0.0
        fix = fixes[k]
        for l in range(layers):
            results[k, l] = jnp.where(open_face, trial[k, l] + fix, 0.0)
            if l == half - 1:
                stores[4 + 2 * k].start()
        stores[5 + 2 * k].start()
    for cp in stores:
        cp.wait()


def body(
    devices, height, transport_u, transport_v, thickness, velocity_u, velocity_v,
    sea_faces, wind_seeds, wind_scale, wind_base,
):
    layers, cells, rows = thickness.shape
    wide = rows + LANES
    ext = cells + 8
    anywhere = pl.BlockSpec(memory_space=pl.ANY)
    vmem = pl.BlockSpec(memory_space=pltpu.VMEM)

    def shape(*dims):
        return jax.ShapeDtypeStruct(dims, F32)

    def inner(*dims):
        return pltpu.VMEM(dims, F32)

    mid = pl.pallas_call(
        functools.partial(exchange, devices),
        out_shape=[
            inner(layers, cells, rows), inner(2, layers, cells, rows), inner(2, cells, rows),
            inner(2, cells, rows), inner(3, cells, rows),
        ],
        in_specs=[anywhere] * 10,
        out_specs=[vmem] * 5,
        scratch_shapes=[
            inner(7, cells + 16, wide),
            inner(3, layers, ext, wide),
            inner(layers, ext, rows),
            inner(layers, cells, wide),
            inner(layers, cells, wide),
            inner(4, ext, wide),
            pltpu.VMEM(sea_faces.shape, sea_faces.dtype),
            inner(*wind_base.shape),
            pltpu.SMEM(wind_seeds.shape[::-1], wind_seeds.dtype),
            pltpu.SMEM(wind_scale.shape, F32),
            inner(48, rows), inner(3 * layers, rows), inner(3 * layers, rows), inner(48, rows),
            inner(3, 8, rows), inner(3, 8, rows), inner(2, 8, LANES), inner(8, LANES), inner(8, LANES),
            inner(cells, 2 * LANES), inner(cells, 2 * LANES), inner(2, 8, LANES), inner(2, 8, LANES),
            inner(cells, 2 * LANES), inner(cells, 2 * LANES), inner(2, 8, LANES), inner(2, 8, LANES),
            pltpu.SemaphoreType.DMA((10,)),
            pltpu.SemaphoreType.DMA((19,)),
            pltpu.SemaphoreType.DMA((19,)),
            pltpu.SemaphoreType.REGULAR,
            pltpu.SemaphoreType.REGULAR,
            pltpu.SemaphoreType.REGULAR,
        ],
        compiler_params=pltpu.CompilerParams(collective_id=0, has_side_effects=True),
        name="exchange",
    )(
        height, transport_u, transport_v, thickness, velocity_u, velocity_v,
        sea_faces, wind_base, wind_seeds.T, wind_scale,
    )
    return pl.pallas_call(
        finish,
        out_shape=[shape(cells, rows)] * 3 + [shape(layers, cells, rows)] * 3,
        in_specs=[vmem] * 5,
        out_specs=[anywhere] * 6,
        scratch_shapes=[inner(2, layers, cells, rows), pltpu.SemaphoreType.DMA((8,))],
        name="finish",
    )(*[pltpu.with_memory_space_constraint(x, pltpu.VMEM) for x in mid])


def solution(mesh):
    flat = P(("members", "zonal"), "merid")
    deep = P(None, ("members", "zonal"), "merid")
    fixed = P(None, "zonal", "merid")
    return jax.shard_map(
        functools.partial(body, mesh.shape["zonal"]),
        mesh=mesh,
        in_specs=(flat, flat, flat, deep, deep, deep, fixed, P("members", None), P("members"), fixed),
        out_specs=(flat, flat, flat, deep, deep, deep),
        check_vma=False,
    )
```
